32 devices in a mesh: cp: 16 (over z, y, core), tp: 2 (over x).
Axes of the slice: x: 2, y: 2, z: 4, core: 2. Of those that a mesh axis runs over, the one named last changes fastest.
Arguments:
- block_input: bfloat16 [2, 2048, 1536], P(None, ('cp', 'tp')), may hold values from -6 to 6
- segments: int32 [2, 2048], replicated, may hold values from 0 to 2, as said below
- positions: int32 [2, 2048], replicated, may hold values from 0 to 1023, as said below
- query_weight: bfloat16 [1536, 1536], P('cp', 'tp'), may hold values from -0.15625 to 0.15625
- key_matrix: bfloat16 [1536, 768], P('cp', 'tp'), may hold values from -0.15625 to 0.15625
- value_matrix: bfloat16 [1536, 768], P('cp', 'tp'), may hold values from -0.15625 to 0.15625
- out_weight: bfloat16 [1536, 1536], P('tp', 'cp'), may hold values from -0.875 to 0.875
- gate_weight: bfloat16 [1536, 4096], P('cp', 'tp'), may hold values from -0.15625 to 0.15625
- up_weight: bfloat16 [1536, 4096], P('cp', 'tp'), may hold values from -0.15625 to 0.15625
- down_weight: bfloat16 [4096, 1536], P('tp', 'cp'), may hold values from -0.09375 to 0.09375
- gain_first: float32 [1536], replicated, may hold values from 0.5 to 1.5
- gain_second: float32 [1536], replicated, may hold values from 0.5 to 1.5
- cotangent: bfloat16 [2, 2048, 1536], P(None, ('cp', 'tp')), may hold values from -6 to 6
Outputs:
- block_output: bfloat16 [2, 2048, 1536], P(None, ('cp', 'tp'))
- grad_input: bfloat16 [2, 2048, 1536], P(None, ('cp', 'tp'))
- grad_query: float32 [1536, 1536], P('cp', 'tp')
- grad_key: float32 [1536, 768], P('cp', 'tp')
- grad_value: float32 [1536, 768], P('cp', 'tp')
- grad_out: float32 [1536, 1536], P('tp', 'cp')
- grad_gate: float32 [1536, 4096], P('cp', 'tp')
- grad_up: float32 [1536, 4096], P('cp', 'tp')
- grad_down: float32 [4096, 1536], P('tp', 'cp')
- grad_first: float32 [1536], replicated
- grad_second: float32 [1536], replicated
The draws below stay inside these ranges and needn't reach their ends.
Inputs may be any that keep to these rules, and one draw needn't show every extreme that they name: `segments`: in packed order (see the row layout) segment ids count the documents of a micro-batch from 0 and never fall; a document is at most 1024 tokens and never crosses a multiple of 1024 packed tokens; each micro-batch holds 3 documents, one of exactly 1024 tokens. `positions`: the position of each token within its document, counting from 0 in packed order.
All inputs are finite; a program needn't handle non-finite values.
Results may differ from the reference program's by a relative error of at most 0.024.
Values may be sent and summed in bfloat16 or wider, within the bound.
A program may use at most 192 MiB of HBM per device.

```python
import math
import jax
import jax.numpy as jnp
from jax import lax

MODEL_WIDTH = 1536
QUERY_HEADS = 16
KEY_VALUE_HEADS = 8
HEAD_SIZE = 96
FF = 4096
MICRO = 2
DOCUMENT_LIMIT = 1024
BLOCK = 64
PACK = 2048


def layout_rows(packed_rows):
    count = PACK // (2 * BLOCK)
    blocks = packed_rows.reshape(MICRO, 2 * count, BLOCK)
    paired = jnp.stack([blocks[:, :count], blocks[:, count:][:, ::-1]], axis=2)
    return paired.reshape(MICRO, PACK)


def document_layout(key):
    key_cut = jax.random.fold_in(key, 11)
    key_whole = jax.random.fold_in(key, 13)
    regions = PACK // DOCUMENT_LIMIT
    spots = jnp.arange(PACK, dtype=jnp.int32)
    region_of = spots // DOCUMENT_LIMIT
    inner = spots % DOCUMENT_LIMIT
    cut_at = jax.random.randint(key_cut, (MICRO, regions), 1, DOCUMENT_LIMIT)
    whole_block = jax.random.randint(key_whole, (MICRO, 1), 0, regions)
    region_match = (region_of[:, None] == jnp.arange(regions, dtype=jnp.int32)[None, :]).astype(jnp.int32)
    cut_spot = jnp.sum(region_match[None, :, :] * cut_at[:, None, :], axis=2)
    free_block = region_of[None, :] != whole_block
    starts = (inner == 0)[None, :] | (inner[None, :] == cut_spot) & free_block
    seg_packed = jnp.cumsum(starts.astype(jnp.int32), axis=1) - 1
    start_spot = lax.cummax(jnp.where(starts, spots[None, :], 0), axis=1)
    pos_packed = spots[None, :] - start_spot
    return (layout_rows(seg_packed).astype(jnp.int32), layout_rows(pos_packed).astype(jnp.int32))


def draw_segments(key, part):
    return document_layout(jax.random.fold_in(key, 7))[0]


def draw_positions(key, part):
    return document_layout(jax.random.fold_in(key, 7))[1]


def block_scale(rng, dims, pieces, smallest, largest):
    def one(position, parts):
        steps = jax.random.uniform(jax.random.fold_in(jax.random.fold_in(rng, 6), position), (parts,), jnp.float32, smallest / len(pieces), largest / len(pieces))
        return jnp.repeat(jnp.exp(steps), dims[position] // parts).reshape((-1,) + (1,) * (len(dims) - position - 1))

    level = one(*pieces[0])
    for cut in pieces[1:]:
        level = level * one(*cut)
    return level


def gaussian(key, shape, scale, bound, split=(), held_as=jnp.bfloat16):
    level = block_scale(key, shape, split, -0.22, 0.18) if split else 1.0
    drawn = jax.random.normal(key, shape, jnp.float32) * scale * level
    return jnp.minimum(jnp.maximum(drawn, -bound), bound).astype(held_as)


def setup_inputs(seed: int = 0) -> dict:
    key_list = jax.random.split(jax.random.key(seed), 14)
    block_input = gaussian(key_list[0], (MICRO, PACK, MODEL_WIDTH), 1.0, 6.0, ((1, 32),))
    segments = draw_segments(jax.random.fold_in(key_list[13], 71), 0)
    positions = draw_positions(jax.random.fold_in(key_list[13], 71), 0)
    query_weight = gaussian(key_list[3], (MODEL_WIDTH, QUERY_HEADS * HEAD_SIZE), MODEL_WIDTH ** -0.5, 0.15625, ((0, 16), (1, 2)))
    key_matrix = gaussian(key_list[4], (MODEL_WIDTH, KEY_VALUE_HEADS * HEAD_SIZE), MODEL_WIDTH ** -0.5, 0.15625, ((0, 16), (1, 2)))
    value_matrix = gaussian(key_list[5], (MODEL_WIDTH, KEY_VALUE_HEADS * HEAD_SIZE), MODEL_WIDTH ** -0.5, 0.15625, ((0, 16), (1, 2)))
    out_weight = gaussian(key_list[6], (QUERY_HEADS * HEAD_SIZE, MODEL_WIDTH), (QUERY_HEADS * HEAD_SIZE // 32) ** -0.5, 0.875, ((0, 2), (1, 16)))
    gate_weight = gaussian(key_list[7], (MODEL_WIDTH, FF), MODEL_WIDTH ** -0.5, 0.15625, ((0, 16), (1, 2)))
    up_weight = gaussian(key_list[8], (MODEL_WIDTH, FF), MODEL_WIDTH ** -0.5, 0.15625, ((0, 16), (1, 2)))
    down_weight = gaussian(key_list[9], (FF, MODEL_WIDTH), FF ** -0.5, 0.09375, ((0, 2), (1, 16)))
    gain_first = jnp.clip(1.0 + 0.1 * jax.random.normal(key_list[10], (MODEL_WIDTH,), jnp.float32), 0.5, 1.5)
    gain_second = jnp.clip(1.0 + 0.1 * jax.random.normal(key_list[11], (MODEL_WIDTH,), jnp.float32), 0.5, 1.5)
    cotangent = gaussian(key_list[12], (MICRO, PACK, MODEL_WIDTH), 1.0, 6.0, ((1, 32),))
    return dict(block_input=block_input, segments=segments, positions=positions, query_weight=query_weight, key_matrix=key_matrix, value_matrix=value_matrix, out_weight=out_weight, gate_weight=gate_weight, up_weight=up_weight, down_weight=down_weight, gain_first=gain_first, gain_second=gain_second, cotangent=cotangent)


@jax.custom_vjp
def reduced_input(v):
    return lax.optimization_barrier(v.astype(jnp.bfloat16)).astype(jnp.float32)

@jax.custom_vjp
def reduced_backward(v):
    return v

def low_keep(v):
    return (reduced_input(v), None)

def low_pass(kept, grad):
    return (grad,)

def back_keep(v):
    return (v, None)

def back_low(kept, grad):
    return (reduced_input(grad),)
reduced_input.defvjp(low_keep, low_pass)
reduced_backward.defvjp(back_keep, back_low)
eps_norm = 1e-05
rope_base = 100000.0
masked_score = -1e+30
TOP_PRECISION = lax.Precision.HIGHEST

def to_packed(row_data):
    count = row_data.shape[0] // (2 * BLOCK)
    blocks = row_data.reshape((count, 2, BLOCK) + row_data.shape[1:])
    joined = jnp.concatenate([blocks[:, 0], blocks[::-1, 1]], axis=0)
    return joined.reshape(row_data.shape)

def to_layout(row_data):
    count = row_data.shape[0] // (2 * BLOCK)
    blocks = row_data.reshape((2 * count, BLOCK) + row_data.shape[1:])
    paired = jnp.stack([blocks[:count], blocks[count:][::-1]], axis=1)
    return paired.reshape(row_data.shape)

def rms_scale(values, gain):
    return values * lax.rsqrt(lax.optimization_barrier(jnp.mean(values * values, axis=-1, keepdims=True)) + eps_norm) * gain

def rotation(spots):
    half_dim = HEAD_SIZE // 2
    frequency = jnp.exp(jnp.arange(half_dim, dtype=jnp.float32) * (-2.0 * math.log(rope_base) / HEAD_SIZE))
    angles = spots.astype(jnp.float32)[:, None] * frequency[None, :]
    return (jnp.cos(angles)[:, None, :], jnp.sin(angles)[:, None, :])

def rotate(values, cosine, sine_part):
    half_dim = values.shape[-1] // 2
    front_half = values[..., :half_dim]
    back_half = values[..., half_dim:]
    return jnp.concatenate([front_half * cosine - back_half * sine_part, back_half * cosine + front_half * sine_part], axis=-1)

def attend(query_set, key_row_set, value_row_set, seg_line, pos_line):
    length_total = query_set.shape[0]
    block_length = min(512, DOCUMENT_LIMIT)
    window_len = DOCUMENT_LIMIT + block_length
    group_width = QUERY_HEADS // KEY_VALUE_HEADS
    score_scale = HEAD_SIZE ** (-0.5)
    key_padded = jnp.concatenate([jnp.zeros((DOCUMENT_LIMIT, KEY_VALUE_HEADS, HEAD_SIZE), jnp.float32), key_row_set], axis=0)
    value_padded = jnp.concatenate([jnp.zeros((DOCUMENT_LIMIT, KEY_VALUE_HEADS, HEAD_SIZE), jnp.float32), value_row_set], axis=0)
    seg_pad = jnp.concatenate([jnp.full((DOCUMENT_LIMIT,), -1, jnp.int32), seg_line.astype(jnp.int32)])
    pos_pad = jnp.concatenate([jnp.zeros((DOCUMENT_LIMIT,), jnp.int32), pos_line.astype(jnp.int32)])
    query_block_list = query_set.reshape(length_total // block_length, block_length, KEY_VALUE_HEADS, group_width, HEAD_SIZE)
    block_starts = jnp.arange(length_total // block_length, dtype=jnp.int32) * block_length

    def one_block(packed_pair):
        query_block, start = packed_pair
        key_window = lax.dynamic_slice_in_dim(key_padded, start, window_len, 0)
        value_window = lax.dynamic_slice_in_dim(value_padded, start, window_len, 0)
        seg_window = lax.dynamic_slice_in_dim(seg_pad, start, window_len, 0)
        pos_window = lax.dynamic_slice_in_dim(pos_pad, start, window_len, 0)
        seg_query = lax.dynamic_slice_in_dim(seg_line.astype(jnp.int32), start, block_length, 0)
        pos_query = lax.dynamic_slice_in_dim(pos_line.astype(jnp.int32), start, block_length, 0)
        scores = reduced_backward(jnp.einsum('qkge,wke->kgqw', query_block, key_window, precision=TOP_PRECISION) * score_scale)
        allowed = (seg_window[None, :] == seg_query[:, None]) & (pos_window[None, :] <= pos_query[:, None])
        scores = jnp.where(allowed, scores, masked_score)
        probs = reduced_input(jax.nn.softmax(scores, axis=-1))
        return jnp.einsum('kgqw,wke->qkge', probs, value_window, precision=TOP_PRECISION)
    outcome = lax.map(jax.checkpoint(one_block), (query_block_list, block_starts))
    return outcome.reshape(length_total, QUERY_HEADS * HEAD_SIZE)

def layer(inputs, query_weight, key_matrix, value_matrix, out_weight, gate_weight, up_weight, down_weight, gain_first, gain_second, seg_line, pos_line):
    length_total = inputs.shape[0]
    cosine, sine_part = rotation(pos_line)
    normalized_rows = reduced_input(rms_scale(inputs, gain_first))
    query_lin = reduced_backward(jnp.dot(normalized_rows, query_weight, precision=TOP_PRECISION)).reshape(length_total, QUERY_HEADS, HEAD_SIZE)
    key_linear = reduced_backward(jnp.dot(normalized_rows, key_matrix, precision=TOP_PRECISION)).reshape(length_total, KEY_VALUE_HEADS, HEAD_SIZE)
    value_row_set = reduced_input(reduced_backward(jnp.dot(normalized_rows, value_matrix, precision=TOP_PRECISION))).reshape(length_total, KEY_VALUE_HEADS, HEAD_SIZE)
    query_set = reduced_input(rotate(query_lin, cosine, sine_part))
    key_row_set = reduced_input(rotate(key_linear, cosine, sine_part))
    attended = reduced_input(reduced_backward(attend(query_set, key_row_set, value_row_set, seg_line, pos_line)))
    residual = inputs + reduced_backward(jnp.dot(attended, out_weight, precision=TOP_PRECISION))
    normed_mlp = reduced_input(rms_scale(residual, gain_second))
    gate_value = reduced_backward(jnp.dot(normed_mlp, gate_weight, precision=TOP_PRECISION))
    upward = reduced_backward(jnp.dot(normed_mlp, up_weight, precision=TOP_PRECISION))
    hidden = reduced_input(jax.nn.silu(gate_value) * upward)
    return residual + reduced_backward(jnp.dot(hidden, down_weight, precision=TOP_PRECISION))

def reference(block_input, segments, positions, query_weight, key_matrix, value_matrix, out_weight, gate_weight, up_weight, down_weight, gain_first, gain_second, cotangent):
    weight_list = tuple((weight_item.astype(jnp.float32) for weight_item in (query_weight, key_matrix, value_matrix, out_weight, gate_weight, up_weight, down_weight, gain_first, gain_second)))
    totals = tuple((jnp.zeros(weight_item.shape, jnp.float32) for weight_item in weight_list))
    outputs = []
    input_grads = []
    for batch_index in range(MICRO):
        seg_line = to_packed(segments[batch_index])
        pos_line = to_packed(positions[batch_index])
        packed_input = to_packed(block_input[batch_index].astype(jnp.float32))

        def forward(inputs, *params):
            return layer(inputs, *params, seg_line, pos_line)
        result, pullback = jax.vjp(forward, packed_input, *weight_list)
        gradients = pullback(to_packed(cotangent[batch_index].astype(jnp.float32)))
        outputs.append(to_layout(result).astype(jnp.bfloat16))
        input_grads.append(to_layout(gradients[0]).astype(jnp.bfloat16))
        totals = jax.tree.map(jnp.add, totals, tuple(gradients[1:]))
    return (jnp.stack(outputs), jnp.stack(input_grads), totals[0], totals[1], totals[2], totals[3], totals[4], totals[5], totals[6], totals[7], totals[8])
```

```python
import functools
import math

import jax
import jax.numpy as jnp
from jax import lax
from jax.experimental import pallas as pl
from jax.experimental.pallas import tpu as pltpu
from jax.sharding import Mesh
from jax.sharding import PartitionSpec as P

HEAD_SIZE = 96
DOCUMENT_LIMIT = 1024
CORES = 2

eps_norm = 1e-05
rope_base = 100000.0
masked_score = -1e30


f32 = jnp.float32
low = jnp.bfloat16


def mm(left, right, dims):
    return lax.dot_general(left, right, (dims, ((), ())), preferred_element_type=f32)


def pair_swap(values, axis):
    return lax.ppermute(values, axis, [(0, 1), (1, 0)])


def both(values, axis):
    other = pair_swap(values, axis)
    first = lax.axis_index(axis) == 0
    return jnp.stack([jnp.where(first, values, other), jnp.where(first, other, values)])


def split_pair(low_part, high_part, axis):
    first = lax.axis_index(axis) == 0
    return jnp.where(first, low_part, high_part), jnp.where(first, high_part, low_part)


def ring_of(count):
    order = list(range(0, count, 2)) + list(range(count - 1, 0, -2))
    place = [order.index(chip) for chip in range(count)]
    ahead = [(order[i], order[(i + 1) % count]) for i in range(count)]
    back = [(order[i], order[(i - 1) % count]) for i in range(count)]
    return order, place, ahead, back


def ring_gather(block):
    count = lax.axis_size("chip")
    order, place, ahead, back = ring_of(count)
    spot = jnp.array(place)[lax.axis_index("chip")]
    half_way, half_rows = count // 2, block.shape[0] // 2

    def put(whole, piece, step):
        owner = jnp.array(order)[(spot + step) % count]
        return lax.dynamic_update_index_in_dim(whole, piece, owner, 0)

    whole = put(jnp.zeros((count,) + block.shape, block.dtype), block, 0)
    up = down = block
    for step in range(1, half_way):
        up, down = lax.ppermute(up, "chip", ahead), lax.ppermute(down, "chip", back)
        whole = put(put(whole, up, count - step), down, step)
    up = lax.ppermute(up[:half_rows], "chip", ahead)
    down = lax.ppermute(down[half_rows:], "chip", back)
    whole = put(whole, jnp.concatenate([up, down], axis=0), half_way)
    return whole.reshape((count * block.shape[0],) + block.shape[1:])


def ring_scatter(terms):
    count = lax.axis_size("chip")
    order, place, ahead, back = ring_of(count)
    spot = jnp.array(place)[lax.axis_index("chip")]
    rows = terms.shape[0] // count
    half_way, half_rows = count // 2, rows // 2
    terms = terms.reshape((count, rows) + terms.shape[1:])

    def own(step):
        owner = jnp.array(order)[(spot + step) % count]
        return lax.dynamic_index_in_dim(terms, owner, 0, keepdims=False).astype(f32)

    far = own(half_way).astype(low)
    up = lax.ppermute(far[:half_rows], "chip", ahead)
    down = lax.ppermute(far[half_rows:], "chip", back)
    for step in range(half_way - 1, 0, -1):
        own_up, own_down = own(step), own(count - step)
        if step == half_way - 1:
            up = jnp.concatenate([own_up[:half_rows] + up.astype(f32), own_up[half_rows:]], axis=0)
            down = jnp.concatenate([own_down[:half_rows], own_down[half_rows:] + down.astype(f32)], axis=0)
        else:
            up, down = own_up + up.astype(f32), own_down + down.astype(f32)
        up = lax.ppermute(up.astype(low), "chip", ahead)
        down = lax.ppermute(down.astype(low), "chip", back)
    return own(0) + up.astype(f32) + down.astype(f32)


def core_split(low_part, high_part):
    kept, sent = split_pair(low_part, high_part, "core")
    other = pair_swap(sent, "core")
    first = lax.axis_index("core") == 0
    return jnp.concatenate([jnp.where(first, kept, other), jnp.where(first, other, kept)], axis=0)


def core_merge(rows):
    half = rows.shape[0] // 2
    kept, sent = split_pair(rows[:half], rows[half:], "core")
    other = pair_swap(sent.astype(low), "core").astype(f32)
    first = lax.axis_index("core") == 0
    return jnp.where(first, kept, other), jnp.where(first, other, kept)


def all_sum(values):
    for axis in ("tp", "core", "chip"):
        step = 1
        while step < lax.axis_size(axis):
            pairs = [(i, i ^ step) for i in range(lax.axis_size(axis))]
            values = values + lax.ppermute(values, axis, pairs)
            step *= 2
    return values


def gather_rows(rows, micro_count, cores):
    width = rows.shape[-1]
    tp_count = lax.axis_size("tp")
    joined = both(rows, "tp") if tp_count == 2 else lax.all_gather(rows, "tp", axis=0)
    joined = both(joined, "core") if cores == 2 else joined
    joined = joined.reshape((cores, 2, tp_count // 2, micro_count, -1, width))
    return joined.transpose((3, 1, 0, 2, 4, 5)).reshape((-1, width))


def scatter_rows(parts, micro_count, cores):
    width = parts.shape[-1]
    tp_count = lax.axis_size("tp")
    parts = parts.reshape((micro_count, 2, cores, tp_count // 2, -1, width)).transpose((2, 1, 3, 0, 4, 5))
    parts = parts.reshape((cores, tp_count, -1, width))
    if cores == 2:
        kept, sent = split_pair(parts[0], parts[1], "core")
        parts = (kept.astype(f32) + pair_swap(sent, "core").astype(f32)).astype(low)
    else:
        parts = parts[0]
    if tp_count == 2:
        kept, sent = split_pair(parts[0], parts[1], "tp")
        return kept.astype(f32) + pair_swap(sent, "tp").astype(f32)
    return lax.psum_scatter(parts, "tp", scatter_dimension=0, tiled=False).astype(f32)


def norm_scale(values):
    return lax.rsqrt(jnp.mean(values * values, axis=-1, keepdims=True) + eps_norm)


def norm_back(values, gain, grads):
    rho = norm_scale(values)
    scaled = grads * gain
    inner = jnp.mean(scaled * values, axis=-1, keepdims=True)
    return rho * scaled - values * (rho * rho * rho * inner), jnp.sum(grads * values * rho, axis=0)


def angles_of(spots):
    half_dim = HEAD_SIZE // 2
    frequency = jnp.exp(jnp.arange(half_dim, dtype=f32) * (-2.0 * math.log(rope_base) / HEAD_SIZE))
    angles = frequency[:, None] * spots.astype(f32)[None, :]
    return jnp.cos(angles), jnp.sin(angles)


def unit_chunks(tokens):
    width = min(256, tokens)
    return [slice(start, start + width) for start in range(0, tokens, width)]


def lay_out(pieces_ref, flat):
    count, _, width = pieces_ref.shape
    for piece in range(count):
        flat[:, piece * width : (piece + 1) * width] = pieces_ref[piece]


def allowed_keys(code_column, last_row, first_row):
    return (code_column <= last_row) & (code_column >= first_row)


def attend_kernel(group, pieces_ref, code_ref, last_ref, first_ref, out_ref, stat_ref, flat):
    dim = HEAD_SIZE
    count, _, width = pieces_ref.shape
    tokens = count * width
    score_scale = dim ** (-0.5)
    lay_out(pieces_ref, flat)
    key_rows = flat[group * dim : (group + 1) * dim, :].astype(f32).T.astype(low)
    value_t = flat[(group + 1) * dim :, :]
    for cols in unit_chunks(tokens):
        keep = allowed_keys(code_ref[...], last_ref[:, cols], first_ref[:, cols])
        for head in range(group):
            query_t = flat[head * dim : (head + 1) * dim, cols]
            scores = mm(key_rows, query_t, ((1,), (0,))) * score_scale
            scores = jnp.where(keep, scores, masked_score)
            maximum = jnp.max(scores, axis=0, keepdims=True)
            weights = jnp.exp(scores - maximum)
            totals = jnp.sum(weights, axis=0, keepdims=True)
            probs = (weights * (1.0 / totals)).astype(low)
            stat_ref[head : head + 1, cols] = maximum + jnp.log(totals)
            result = mm(value_t, probs, ((1,), (0,))).astype(low)
            for piece in range(cols.start // width, cols.stop // width):
                start = piece * width - cols.start
                out_ref[piece, head * dim : (head + 1) * dim, :] = result[:, start : start + width]


def attend_back_kernel(
    group, pieces_ref, grads_ref, code_ref, last_ref, first_ref, stat_ref, cos_ref, sin_ref, out_ref, flat, grad_flat, key_sum, value_sum
):
    dim = HEAD_SIZE
    half = dim // 2
    count, _, width = pieces_ref.shape
    tokens = count * width
    score_scale = dim ** (-0.5)
    lay_out(pieces_ref, flat)
    lay_out(grads_ref, grad_flat)
    key_t = flat[group * dim : (group + 1) * dim, :]
    key_rows = key_t.astype(f32).T.astype(low)
    value_rows = flat[(group + 1) * dim :, :].astype(f32).T.astype(low)

    def store(values, base, cols):
        for piece in range(cols.start // width, cols.stop // width):
            start = piece * width - cols.start
            out_ref[piece, base : base + values.shape[0], :] = values[:, start : start + width]

    def unturn(values, base, cols):
        front, back = values[:half] * score_scale, values[half:] * score_scale
        cosine, sine = cos_ref[:, cols], sin_ref[:, cols]
        store((front * cosine + back * sine).astype(low), base, cols)
        store((back * cosine - front * sine).astype(low), base + half, cols)

    for index, cols in enumerate(unit_chunks(tokens)):
        keep = allowed_keys(code_ref[...], last_ref[:, cols], first_ref[:, cols])
        for head in range(group):
            rows = slice(head * dim, (head + 1) * dim)
            query_t, grad_t = flat[rows, cols], grad_flat[rows, cols]
            scores = mm(key_rows, query_t, ((1,), (0,))) * score_scale
            probs = jnp.where(keep, jnp.exp(scores - stat_ref[head : head + 1, cols]), 0.0)
            grad_probs = mm(value_rows, grad_t, ((1,), (0,)))
            delta = jnp.sum(probs * grad_probs, axis=0, keepdims=True)
            grad_scores = (probs * (grad_probs - delta)).astype(low)
            unturn(mm(key_t, grad_scores, ((1,), (0,))), head * dim, cols)
            key_part = mm(query_t, grad_scores, ((1,), (1,)))
            value_part = mm(grad_t, probs.astype(low), ((1,), (1,)))
            if index == 0 and head == 0:
                key_sum[...] = key_part
                value_sum[...] = value_part
            else:
                key_sum[...] += key_part
                value_sum[...] += value_part
    everything = slice(0, tokens)
    unturn(key_sum[...], group * dim, everything)
    store(value_sum[...].astype(low), (group + 1) * dim, everything)


def vmem_call(kernel, outs, scratch, flops, *operands):
    spec = pl.BlockSpec(memory_space=pltpu.VMEM)
    moved = sum(math.prod(a.shape) * a.dtype.itemsize for a in operands + tuple(outs))
    return pl.pallas_call(
        kernel,
        out_shape=tuple(outs),
        in_specs=[spec] * len(operands),
        out_specs=tuple([spec] * len(outs)),
        scratch_shapes=scratch,
        cost_estimate=pl.CostEstimate(flops=flops, bytes_accessed=moved, transcendentals=2 * DOCUMENT_LIMIT**2),
        compiler_params=pltpu.CompilerParams(vmem_limit_bytes=48 << 20),
    )(*operands)


def on_device(
    block_input,
    segments,
    positions,
    query_weight,
    key_matrix,
    value_matrix,
    out_weight,
    gate_weight,
    up_weight,
    down_weight,
    gain_first,
    gain_second,
    cotangent,
):
    chips, tp_count = lax.axis_size("chip"), lax.axis_size("tp")
    chip, core = lax.axis_index("chip"), lax.axis_index("core")
    cp_count, cp_index = chips * CORES, chip * CORES + core
    micro, tok_dev, width = block_input.shape
    dim = HEAD_SIZE
    block_rows = tok_dev * tp_count // 2
    query_heads, value_heads = query_weight.shape[1] // dim, key_matrix.shape[1] // dim
    group = query_heads // value_heads
    unit_rows = (group + 2) * dim
    head_cores = CORES if value_heads % CORES == 0 else 1
    heads = value_heads // head_cores
    toks = head_cores * block_rows
    pieces = DOCUMENT_LIMIT // toks
    assert pieces == micro * 2 * heads and cp_count % (pieces * head_cores) == 0

    by_head = jnp.concatenate(
        [
            query_weight.reshape(-1, value_heads, group * dim),
            key_matrix.reshape(-1, value_heads, dim),
            value_matrix.reshape(-1, value_heads, dim),
        ],
        axis=2,
    ).reshape(query_weight.shape[0], -1)
    out_t, down_t = out_weight.T, down_weight.T

    def halves(matrix):
        half = matrix.shape[1] // 2
        return matrix[:, :half], matrix[:, half:]

    def gather_head_weight(matrix):
        if head_cores == 2:
            return ring_gather(core_split(*halves(matrix)))
        return lax.all_gather(matrix, ("chip", "core"), axis=0, tiled=True)

    def scatter_head_weight(grads):
        if head_cores == 2:
            return jnp.concatenate(core_merge(ring_scatter(grads)), axis=1)
        return lax.psum_scatter(grads, ("chip", "core"), scatter_dimension=0, tiled=True).astype(f32)

    head_full = gather_head_weight(by_head)
    out_full = gather_head_weight(out_t)
    gate_full = ring_gather(core_split(*halves(gate_weight)))
    up_full = ring_gather(core_split(*halves(up_weight)))
    down_full = ring_gather(core_split(*halves(down_t)))

    by_block = lambda line: line.reshape(micro, cp_count, 2, block_rows)
    group_cp = pieces * head_cores
    first_cp = cp_index // head_cores * head_cores
    row_pos = lax.dynamic_slice_in_dim(by_block(positions), first_cp, head_cores, 1)
    row_pos = row_pos.transpose(0, 2, 1, 3).reshape(-1)
    unit_index = cp_index // head_cores % pieces
    unit_micro, unit_half = unit_index // (2 * heads), unit_index // heads % 2

    def unit_line(line):
        mine = lax.dynamic_slice(
            by_block(line),
            (unit_micro, cp_index // group_cp * group_cp, unit_half, 0),
            (1, group_cp, 1, block_rows),
        )
        return mine.reshape(1, DOCUMENT_LIMIT)

    unit_pos, unit_seg = unit_line(positions), unit_line(segments)
    first_code = unit_seg * DOCUMENT_LIMIT
    last_code = first_code + unit_pos
    code_column = last_code.reshape(DOCUMENT_LIMIT, 1)
    cosine, sine = angles_of(row_pos)
    unit_cosine, unit_sine = angles_of(unit_pos.reshape(-1))

    if head_cores == 2:
        exchange_axis = "chip"
        groups = [[g + i for i in range(pieces)] for g in range(0, chips, pieces)]
    else:
        exchange_axis = ("chip", "core")
        groups = [[g + i for i in range(pieces)] for g in range(0, cp_count, pieces)]
    groups = None if len(groups) == 1 else groups

    def exchange(values):
        return lax.all_to_all(values, exchange_axis, 0, 0, axis_index_groups=groups)

    def to_units(values):
        rows = values.shape[0] // heads
        return values.reshape(heads, rows, micro * 2, toks).transpose(2, 0, 1, 3).reshape(pieces, rows, toks)

    def from_units(values):
        rows = values.shape[1]
        return values.reshape(micro * 2, heads, rows, toks).transpose(1, 2, 0, 3).reshape(heads * rows, -1)

    gather_head_rows = functools.partial(gather_rows, micro_count=micro, cores=head_cores)
    scatter_head_rows = functools.partial(scatter_rows, micro_count=micro, cores=head_cores)
    gather_all_rows = functools.partial(gather_rows, micro_count=micro, cores=CORES)
    scatter_all_rows = functools.partial(scatter_rows, micro_count=micro, cores=CORES)

    own_input = block_input.reshape(-1, width).astype(f32)
    cot_own = cotangent.reshape(-1, width)
    first_rows = gather_head_rows((own_input * norm_scale(own_input) * gain_first).astype(low))
    projected = mm(head_full, first_rows, ((0,), (1,))).reshape(heads, unit_rows, -1)
    turned = projected[:, : (group + 1) * dim].reshape(heads, group + 1, 2, dim // 2, -1)
    front, back = turned[:, :, 0], turned[:, :, 1]
    turned = jnp.stack([front * cosine - back * sine, back * cosine + front * sine], axis=2)
    projected = jnp.concatenate(
        [turned.reshape(heads, (group + 1) * dim, -1).astype(low), projected[:, (group + 1) * dim :].astype(low)], axis=1
    )
    unit = exchange(to_units(projected.reshape(heads * unit_rows, -1)))
    square = DOCUMENT_LIMIT * DOCUMENT_LIMIT * dim * 2 * group
    unit_out, unit_stat = vmem_call(
        functools.partial(attend_kernel, group),
        (
            jax.ShapeDtypeStruct((pieces, group * dim, toks), low),
            jax.ShapeDtypeStruct((group, DOCUMENT_LIMIT), f32),
        ),
        [pltpu.VMEM((unit_rows, DOCUMENT_LIMIT), low)],
        2 * square,
        unit,
        code_column,
        last_code,
        first_code,
    )
    attended = from_units(exchange(unit_out))
    residual = own_input + scatter_head_rows(mm(attended, out_full, ((0,), (1,))).astype(low))

    second_rows = gather_all_rows((residual * norm_scale(residual) * gain_second).astype(low))
    cot_rows = gather_all_rows(cot_own)
    gate_value = mm(second_rows, gate_full, ((1,), (0,)))
    upward = mm(second_rows, up_full, ((1,), (0,)))
    sigma = jax.nn.sigmoid(gate_value)
    active = gate_value * sigma
    hidden = (active * upward).astype(low)
    grad_hidden = mm(cot_rows, down_full, ((1,), (0,)))
    gate_back = (grad_hidden * upward * (sigma * (1.0 + gate_value * (1.0 - sigma)))).astype(low)
    up_back = (grad_hidden * active).astype(low)
    second_parts = (mm(gate_back, gate_full, ((1,), (1,))) + mm(up_back, up_full, ((1,), (1,)))).astype(low)
    grad_second_rows = scatter_all_rows(second_parts)
    down_grad = ring_scatter(mm(cot_rows, hidden, ((0,), (0,))).astype(low))
    gate_grad = ring_scatter(mm(second_rows, gate_back, ((0,), (0,))).astype(low))
    up_grad = ring_scatter(mm(second_rows, up_back, ((0,), (0,))).astype(low))
    output_rows = residual + scatter_all_rows(mm(hidden, down_full, ((1,), (1,))).astype(low))

    residual_part, gain_two = norm_back(residual, gain_second, grad_second_rows)
    grad_residual = cot_own.astype(f32) + residual_part
    grad_rows = gather_head_rows(grad_residual.astype(low))
    grad_attended = mm(out_full, grad_rows, ((0,), (1,))).astype(low)
    unit_grad = exchange(to_units(grad_attended))
    (unit_back,) = vmem_call(
        functools.partial(attend_back_kernel, group),
        (jax.ShapeDtypeStruct((pieces, unit_rows, toks), low),),
        [
            pltpu.VMEM((unit_rows, DOCUMENT_LIMIT), low),
            pltpu.VMEM((group * dim, DOCUMENT_LIMIT), low),
            pltpu.VMEM((dim, DOCUMENT_LIMIT), f32),
            pltpu.VMEM((dim, DOCUMENT_LIMIT), f32),
        ],
        5 * square,
        unit,
        unit_grad,
        code_column,
        last_code,
        first_code,
        unit_stat,
        unit_cosine,
        unit_sine,
    )
    back_rows = from_units(exchange(unit_back))
    grad_first_rows = scatter_head_rows(mm(back_rows, head_full, ((0,), (1,))).astype(low))
    head_grad = scatter_head_weight(mm(first_rows, back_rows, ((0,), (1,))).astype(low))
    out_grad = scatter_head_weight(mm(grad_rows, attended, ((0,), (1,))).astype(low))
    input_part, gain_one = norm_back(own_input, gain_first, grad_first_rows)
    input_grad = (grad_residual + input_part).astype(low)
    gain_sums = all_sum(jnp.stack([gain_one, gain_two]))

    head_grad = head_grad.reshape(-1, value_heads, unit_rows)
    columns = query_weight.shape[0]
    return (
        output_rows.astype(low).reshape(block_input.shape),
        input_grad.reshape(block_input.shape),
        head_grad[:, :, : group * dim].reshape(columns, -1),
        head_grad[:, :, group * dim : (group + 1) * dim].reshape(columns, -1),
        head_grad[:, :, (group + 1) * dim :].reshape(columns, -1),
        out_grad.T,
        jnp.concatenate(core_merge(gate_grad), axis=1),
        jnp.concatenate(core_merge(up_grad), axis=1),
        jnp.concatenate(core_merge(down_grad), axis=1).T,
        gain_sums[0],
        gain_sums[1],
    )


def solution(mesh):
    cp_count, tp_count = mesh.shape["cp"], mesh.shape["tp"]
    fine = Mesh(mesh.devices.reshape(cp_count // CORES, CORES, tp_count), ("chip", "core", "tp"))
    cp = ("chip", "core")
    rows = P(None, cp + ("tp",), None)
    wide, tall = P(cp, "tp"), P("tp", cp)
    return jax.shard_map(
        on_device,
        mesh=fine,
        in_specs=(rows, P(), P(), wide, wide, wide, tall, wide, wide, tall, P(), P(), rows),
        out_specs=(rows, rows, wide, wide, wide, tall, wide, wide, tall, P(), P()),
        check_vma=False,
    )
```

```python
import functools
import math

import jax
import jax.numpy as jnp
from jax import lax
from jax.experimental import pallas as pl
from jax.experimental.pallas import tpu as pltpu
from jax.sharding import Mesh
from jax.sharding import PartitionSpec as P

HEAD_SIZE = 96
DOCUMENT_LIMIT = 1024
CORES = 2

eps_norm = 1e-05
rope_base = 100000.0
masked_score = -1e30


f32 = jnp.float32
low = jnp.bfloat16


def mm(left, right, dims):
    return lax.dot_general(left, right, (dims, ((), ())), preferred_element_type=f32)


def pair_swap(values, axis):
    return lax.ppermute(values, axis, [(0, 1), (1, 0)])


def both(values, axis):
    other = pair_swap(values, axis)
    first = lax.axis_index(axis) == 0
    return jnp.stack([jnp.where(first, values, other), jnp.where(first, other, values)])


def split_pair(low_part, high_part, axis):
    first = lax.axis_index(axis) == 0
    return jnp.where(first, low_part, high_part), jnp.where(first, high_part, low_part)


def ring_of(count):
    order = list(range(0, count, 2)) + list(range(count - 1, 0, -2))
    place = [order.index(chip) for chip in range(count)]
    ahead = [(order[i], order[(i + 1) % count]) for i in range(count)]
    back = [(order[i], order[(i - 1) % count]) for i in range(count)]
    return order, place, ahead, back


def ring_gather(block):
    count = lax.axis_size("chip")
    order, place, ahead, back = ring_of(count)
    spot = jnp.array(place)[lax.axis_index("chip")]
    half_way, half_rows = count // 2, block.shape[0] // 2

    def put(whole, piece, step):
        owner = jnp.array(order)[(spot + step) % count]
        return lax.dynamic_update_index_in_dim(whole, piece, owner, 0)

    whole = put(jnp.zeros((count,) + block.shape, block.dtype), block, 0)
    up = down = block
    for step in range(1, half_way):
        up, down = lax.ppermute(up, "chip", ahead), lax.ppermute(down, "chip", back)
        whole = put(put(whole, up, count - step), down, step)
    up = lax.ppermute(up[:half_rows], "chip", ahead)
    down = lax.ppermute(down[half_rows:], "chip", back)
    whole = put(whole, jnp.concatenate([up, down], axis=0), half_way)
    return whole.reshape((count * block.shape[0],) + block.shape[1:])


def ring_scatter(terms):
    count = lax.axis_size("chip")
    order, place, ahead, back = ring_of(count)
    spot = jnp.array(place)[lax.axis_index("chip")]
    rows = terms.shape[0] // count
    half_way, half_rows = count // 2, rows // 2
    terms = terms.reshape((count, rows) + terms.shape[1:])

    def own(step):
        owner = jnp.array(order)[(spot + step) % count]
        return lax.dynamic_index_in_dim(terms, owner, 0, keepdims=False).astype(f32)

    far = own(half_way).astype(low)
    up = lax.ppermute(far[:half_rows], "chip", ahead)
    down = lax.ppermute(far[half_rows:], "chip", back)
    for step in range(half_way - 1, 0, -1):
        own_up, own_down = own(step), own(count - step)
        if step == half_way - 1:
            up = jnp.concatenate([own_up[:half_rows] + up.astype(f32), own_up[half_rows:]], axis=0)
            down = jnp.concatenate([own_down[:half_rows], own_down[half_rows:] + down.astype(f32)], axis=0)
        else:
            up, down = own_up + up.astype(f32), own_down + down.astype(f32)
        up = lax.ppermute(up.astype(low), "chip", ahead)
        down = lax.ppermute(down.astype(low), "chip", back)
    return own(0) + up.astype(f32) + down.astype(f32)


def core_split(low_part, high_part):
    kept, sent = split_pair(low_part, high_part, "core")
    other = pair_swap(sent, "core")
    first = lax.axis_index("core") == 0
    return jnp.concatenate([jnp.where(first, kept, other), jnp.where(first, other, kept)], axis=0)


def core_merge(rows):
    half = rows.shape[0] // 2
    kept, sent = split_pair(rows[:half], rows[half:], "core")
    other = pair_swap(sent.astype(low), "core").astype(f32)
    first = lax.axis_index("core") == 0
    return jnp.where(first, kept, other), jnp.where(first, other, kept)


def all_sum(values):
    for axis in ("tp", "core", "chip"):
        step = 1
        while step < lax.axis_size(axis):
            pairs = [(i, i ^ step) for i in range(lax.axis_size(axis))]
            values = values + lax.ppermute(values, axis, pairs)
            step *= 2
    return values


def gather_rows(rows, micro_count, cores):
    width = rows.shape[-1]
    tp_count = lax.axis_size("tp")
    joined = both(rows, "tp") if tp_count == 2 else lax.all_gather(rows, "tp", axis=0)
    joined = both(joined, "core") if cores == 2 else joined
    joined = joined.reshape((cores, 2, tp_count // 2, micro_count, -1, width))
    return joined.transpose((3, 1, 0, 2, 4, 5)).reshape((-1, width))


def scatter_rows(parts, micro_count, cores):
    width = parts.shape[-1]
    tp_count = lax.axis_size("tp")
    parts = parts.reshape((micro_count, 2, cores, tp_count // 2, -1, width)).transpose((2, 1, 3, 0, 4, 5))
    parts = parts.reshape((cores, tp_count, -1, width))
    if cores == 2:
        kept, sent = split_pair(parts[0], parts[1], "core")
        parts = (kept.astype(f32) + pair_swap(sent, "core").astype(f32)).astype(low)
    else:
        parts = parts[0]
    if tp_count == 2:
        kept, sent = split_pair(parts[0], parts[1], "tp")
        return kept.astype(f32) + pair_swap(sent, "tp").astype(f32)
    return lax.psum_scatter(parts, "tp", scatter_dimension=0, tiled=False).astype(f32)


def norm_scale(values):
    return lax.rsqrt(jnp.mean(values * values, axis=-1, keepdims=True) + eps_norm)


def norm_back(values, gain, grads):
    rho = norm_scale(values)
    scaled = grads * gain
    inner = jnp.mean(scaled * values, axis=-1, keepdims=True)
    return rho * scaled - values * (rho * rho * rho * inner), jnp.sum(grads * values * rho, axis=0)


def angles_of(spots):
    half_dim = HEAD_SIZE // 2
    frequency = jnp.exp(jnp.arange(half_dim, dtype=f32) * (-2.0 * math.log(rope_base) / HEAD_SIZE))
    angles = frequency[:, None] * spots.astype(f32)[None, :]
    return jnp.cos(angles), jnp.sin(angles)


def unit_chunks(tokens):
    width = min(256, tokens)
    return [slice(start, start + width) for start in range(0, tokens, width)]


def lay_out(pieces_ref, flat):
    count, _, width = pieces_ref.shape
    for piece in range(count):
        flat[:, piece * width : (piece + 1) * width] = pieces_ref[piece]


def allowed_keys(code_column, last_row, first_row):
    return (code_column <= last_row) & (code_column >= first_row)


def attend_kernel(group, pieces_ref, code_ref, last_ref, first_ref, out_ref, stat_ref, flat):
    dim = HEAD_SIZE
    count, _, width = pieces_ref.shape
    tokens = count * width
    score_scale = dim ** (-0.5)
    lay_out(pieces_ref, flat)
    key_rows = flat[group * dim : (group + 1) * dim, :].astype(f32).T.astype(low)
    value_t = flat[(group + 1) * dim :, :]
    for cols in unit_chunks(tokens):
        keep = allowed_keys(code_ref[...], last_ref[:, cols], first_ref[:, cols])
        for head in range(group):
            query_t = flat[head * dim : (head + 1) * dim, cols]
            scores = mm(key_rows, query_t, ((1,), (0,))) * score_scale
            scores = jnp.where(keep, scores, masked_score)
            maximum = jnp.max(scores, axis=0, keepdims=True)
            weights = jnp.exp(scores - maximum)
            totals = jnp.sum(weights, axis=0, keepdims=True)
            probs = (weights * (1.0 / totals)).astype(low)
            stat_ref[head : head + 1, cols] = maximum + jnp.log(totals)
            result = mm(value_t, probs, ((1,), (0,))).astype(low)
            for piece in range(cols.start // width, cols.stop // width):
                start = piece * width - cols.start
                out_ref[piece, head * dim : (head + 1) * dim, :] = result[:, start : start + width]


def attend_back_kernel(
    group, pieces_ref, grads_ref, code_ref, last_ref, first_ref, stat_ref, cos_ref, sin_ref, out_ref, flat, grad_flat, key_sum, value_sum
):
    dim = HEAD_SIZE
    half = dim // 2
    count, _, width = pieces_ref.shape
    tokens = count * width
    score_scale = dim ** (-0.5)
    lay_out(pieces_ref, flat)
    lay_out(grads_ref, grad_flat)
    key_t = flat[group * dim : (group + 1) * dim, :]
    key_rows = key_t.astype(f32).T.astype(low)
    value_rows = flat[(group + 1) * dim :, :].astype(f32).T.astype(low)

    def store(values, base, cols):
        for piece in range(cols.start // width, cols.stop // width):
            start = piece * width - cols.start
            out_ref[piece, base : base + values.shape[0], :] = values[:, start : start + width]

    def unturn(values, base, cols):
        front, back = values[:half] * score_scale, values[half:] * score_scale
        cosine, sine = cos_ref[:, cols], sin_ref[:, cols]
        store((front * cosine + back * sine).astype(low), base, cols)
        store((back * cosine - front * sine).astype(low), base + half, cols)

    for index, cols in enumerate(unit_chunks(tokens)):
        keep = allowed_keys(code_ref[...], last_ref[:, cols], first_ref[:, cols])
        for head in range(group):
            rows = slice(head * dim, (head + 1) * dim)
            query_t, grad_t = flat[rows, cols], grad_flat[rows, cols]
            scores = mm(key_rows, query_t, ((1,), (0,))) * score_scale
            probs = jnp.where(keep, jnp.exp(scores - stat_ref[head : head + 1, cols]), 0.0)
            grad_probs = mm(value_rows, grad_t, ((1,), (0,)))
            delta = jnp.sum(probs * grad_probs, axis=0, keepdims=True)
            grad_scores = (probs * (grad_probs - delta)).astype(low)
            unturn(mm(key_t, grad_scores, ((1,), (0,))), head * dim, cols)
            key_part = mm(query_t, grad_scores, ((1,), (1,)))
            value_part = mm(grad_t, probs.astype(low), ((1,), (1,)))
            if index == 0 and head == 0:
                key_sum[...] = key_part
                value_sum[...] = value_part
            else:
                key_sum[...] += key_part
                value_sum[...] += value_part
    everything = slice(0, tokens)
    unturn(key_sum[...], group * dim, everything)
    store(value_sum[...].astype(low), (group + 1) * dim, everything)


MESH_ID = pl.DeviceIdType.MESH


class Sems:
    def __init__(self, send, recv):
        self.send, self.recv, self.used = send, recv, 0

    def take(self, count=1):
        base = self.used
        self.used += count
        return base


def remote(sems, index, source, target, there, arrive=None):
    return pltpu.make_async_remote_copy(
        src_ref=source,
        dst_ref=target,
        send_sem=sems.send.at[index],
        recv_sem=sems.recv.at[index if arrive is None else arrive],
        device_id=there,
        device_id_type=MESH_ID,
    )


def greet(chips, chip, core, tp):
    barrier = pltpu.get_barrier_semaphore()

    @pl.loop(1, chips)
    def _(step):
        pl.semaphore_signal(barrier, inc=1, device_id={"chip": (chip + step) % chips}, device_id_type=MESH_ID)

    pl.semaphore_signal(barrier, inc=1, device_id={"core": 1 - core}, device_id_type=MESH_ID)
    pl.semaphore_signal(barrier, inc=1, device_id={"tp": 1 - tp}, device_id_type=MESH_ID)
    pl.semaphore_wait(barrier, chips + 1)


def spot_of(chip, count):
    odd = chip % 2
    return (1 - odd) * (chip // 2) + odd * (count - 1 - chip // 2)


def chip_at(spot, count):
    spot = (spot + count) % count
    far = spot // (count // 2)
    return (1 - far) * 2 * spot + far * (2 * (count - 1 - spot) + 1)


class Ring:
    def __init__(self, sems, whole, rows, count, chip):
        self.sems, self.whole, self.rows, self.count = sems, whole, rows, count
        self.spot = spot_of(chip, count)
        self.half = count // 2
        self.base = sems.take(2 * self.half)
        self.ways = (1, -1)

    def copy(self, side, hop, behind):
        way = self.ways[side]
        start = chip_at(self.spot - way * behind, self.count) * self.rows
        size = self.rows
        if hop == self.half:
            size = self.rows // 2
            start = start + side * size
        piece = self.whole.at[pl.ds(pl.multiple_of(start, 16), size), :]
        there = {"chip": chip_at(self.spot + way, self.count)}
        return remote(self.sems, self.base + side * self.half + hop - 1, piece, piece, there)

    def start(self, hop):
        for side in (0, 1):
            self.copy(side, hop, hop - 1).start()

    def arrive(self, hop):
        for side in (0, 1):
            self.copy(side, hop, hop).wait_recv()

    def relay(self, hop):
        for side in (0, 1):
            if hop > 1:
                self.copy(side, hop - 1, hop - 1).wait_recv()
            self.copy(side, hop, hop - 1).start()

    def drain(self):
        for side in (0, 1):
            for hop in range(1, self.half + 1):
                self.copy(side, hop, hop - 1).wait_send()


class Spread:
    def __init__(self, sems, source, whole, micro, chip_core_tp):
        self.sems, self.source, self.whole, self.micro = sems, source, whole, micro
        _, self.core, self.tp = chip_core_tp
        self.rows = source.shape[0] // micro
        self.base = sems.take(3 * micro)

    def place(self, m, half, core):
        start = ((m * 2 + half) * 2 + core) * self.rows
        return self.whole.at[pl.ds(pl.multiple_of(start, 16), self.rows), :]

    def own(self, m):
        return self.source.at[m * self.rows : (m + 1) * self.rows, :]

    def over_tp(self, m, half):
        target = self.place(m, half, self.core)
        return remote(self.sems, self.base + m, self.own(m), target, {"tp": 1 - self.tp})

    def over_core(self, m, core):
        target = self.place(m, self.tp, core)
        return remote(self.sems, self.base + self.micro + m, self.own(m), target, {"core": 1 - self.core})

    def passed_on(self, m, core):
        piece = self.place(m, 1 - self.tp, core)
        return remote(self.sems, self.base + 2 * self.micro + m, piece, piece, {"core": 1 - self.core})

    def start(self):
        for m in range(self.micro):
            self.over_tp(m, self.tp).start()
            self.over_core(m, self.core).start()

    def keep(self):
        for m in range(self.micro):
            start = ((m * 2 + self.tp) * 2 + self.core) * self.rows
            self.whole[pl.ds(pl.multiple_of(start, 16), self.rows), :] = self.source[m * self.rows : (m + 1) * self.rows, :]

    def pass_on(self):
        for m in range(self.micro):
            self.over_tp(m, 1 - self.tp).wait_recv()
            self.passed_on(m, self.core).start()

    def finish(self):
        for m in range(self.micro):
            self.over_core(m, 1 - self.core).wait_recv()
            self.passed_on(m, 1 - self.core).wait_recv()

    def drain(self):
        for m in range(self.micro):
            self.over_tp(m, self.tp).wait_send()
            self.over_core(m, self.core).wait_send()
            self.passed_on(m, self.core).wait_send()


class Fold:
    def __init__(self, sems, parts, from_core, to_tp, from_tp, micro, chip_core_tp):
        self.sems, self.parts, self.from_core, self.to_tp, self.from_tp = sems, parts, from_core, to_tp, from_tp
        self.micro = micro
        _, self.core, self.tp = chip_core_tp
        self.rows = from_tp.shape[0] // micro
        self.base = sems.take(3 * micro)

    def piece(self, m, half, core):
        start = ((m * 2 + half) * 2 + core) * self.rows
        return pl.ds(pl.multiple_of(start, 16), self.rows)

    def landing(self, m, half):
        return pl.ds(pl.multiple_of((m * 2 + half) * self.rows, 16), self.rows)

    def over_core(self, m, half):
        source = self.parts.at[self.piece(m, half, 1 - self.core), :]
        index = self.base + m * 2 + half
        return remote(self.sems, index, source, self.from_core.at[self.landing(m, half), :], {"core": 1 - self.core})

    def over_tp(self, m):
        rows = pl.ds(m * self.rows, self.rows)
        index = self.base + 2 * self.micro + m
        return remote(self.sems, index, self.to_tp.at[rows, :], self.from_tp.at[rows, :], {"tp": 1 - self.tp})

    def start(self, m, half):
        self.over_core(m, half).start()

    def summed(self, m, half):
        mine = self.parts[self.piece(m, half, self.core), :].astype(f32)
        return mine + self.from_core[self.landing(m, half), :].astype(f32)

    def send(self, m):
        for half in (0, 1):
            self.over_core(m, half).wait_recv()
        self.to_tp[m * self.rows : (m + 1) * self.rows, :] = self.summed(m, 1 - self.tp).astype(low)
        self.over_tp(m).start()

    def result(self, m):
        kept = self.summed(m, self.tp)
        self.over_tp(m).wait_recv()
        return kept + self.from_tp[m * self.rows : (m + 1) * self.rows, :].astype(f32)

    def drain(self):
        for m in range(self.micro):
            for half in (0, 1):
                self.over_core(m, half).wait_send()
            self.over_tp(m).wait_send()


class Exchange:
    def __init__(self, sems, outgoing, incoming, chips, chip):
        self.sems, self.outgoing, self.incoming, self.chips, self.chip = sems, outgoing, incoming, chips, chip
        self.base = sems.take(chips)

    def copy(self, to):
        return remote(
            self.sems, self.base + to, self.outgoing.at[to], self.incoming.at[self.chip], {"chip": to}, self.base + self.chip
        )

    def send(self, to):
        @pl.when(to != self.chip)
        def _():
            self.copy(to).start()

        @pl.when(to == self.chip)
        def _():
            self.incoming[to] = self.outgoing[to]

    def finish(self):
        @pl.loop(1, self.chips)
        def _(step):
            source = (self.chip + step) % self.chips
            remote(
                self.sems, self.base + source, self.outgoing.at[source], self.incoming.at[source], {"chip": source}
            ).wait_recv()

    def drain(self):
        @pl.loop(1, self.chips)
        def _(step):
            self.copy((self.chip + step) % self.chips).wait_send()


class Actions:
    def __init__(self, steps):
        self.steps = list(steps)

    def run(self, count=None):
        count = len(self.steps) if count is None else count
        for step in self.steps[:count]:
            step()
        self.steps = self.steps[count:]


def forward_kernel(
    micro, group, chips,
    x_ref, first_ref, cot_ref, head_ref, out_ref, gate_ref, up_ref, down_ref, gain_ref, cos_ref, sin_ref, code_ref, last_ref, start_ref,
    head_o, out_o, gate_o, up_o, down_o, first_o, second_o, cot_o, unit_o, att_o, stat_ref, residual_ref,
    head_w, out_w, gate_w, up_w, down_w, first_all, second_own, second_all, cot_all, unit_send, unit_in, flat, att_send, att_in,
    parts, from_core, to_tp, from_tp, send_sem, recv_sem, local_sem, save_sem,
):
    dim = HEAD_SIZE
    half = dim // 2
    chip, core, tp = lax.axis_index("chip"), lax.axis_index("core"), lax.axis_index("tp")
    where = (chip, core, tp)
    sems = Sems(send_sem, recv_sem)
    rows = x_ref.shape[0] // micro
    toks = 2 * rows
    heads = head_w.shape[1] // ((group + 2) * dim)
    unit_rows = (group + 2) * dim
    greet(chips, chip, core, tp)

    depth = head_ref.shape[0]
    weights = ((head_ref, head_w, head_o), (out_ref, out_w, out_o), (down_ref, down_w, down_o), (gate_ref, gate_w, gate_o), (up_ref, up_w, up_o))
    rings, swaps, keeps = [], [], []
    for index, (shard, whole, _) in enumerate(weights):
        columns = whole.shape[1]
        mine = whole.at[pl.ds(pl.multiple_of((chip * 2 + core) * depth, 16), depth), :]
        theirs = whole.at[pl.ds(pl.multiple_of((chip * 2 + 1 - core) * depth, 16), depth), :]
        at = sems.take()
        give = shard.at[:, pl.ds(pl.multiple_of((1 - core) * columns, 128), columns)]
        hold = shard.at[:, pl.ds(pl.multiple_of(core * columns, 128), columns)]
        swaps.append((remote(sems, at, give, mine, {"core": 1 - core}), remote(sems, at, give, theirs, {"core": 1 - core})))
        keeps.append(pltpu.make_async_copy(hold, mine, local_sem.at[index]))
        rings.append(Ring(sems, whole, 2 * depth, chips, chip))
    first, second, cot = (
        Spread(sems, first_ref, first_all, micro, where),
        Spread(sems, second_own, second_all, micro, where),
        Spread(sems, cot_ref, cot_all, micro, where),
    )
    to_unit = Exchange(sems, unit_send, unit_in, chips, chip)
    from_unit = Exchange(sems, att_send, att_in, chips, chip)
    fold = Fold(sems, parts, from_core, to_tp, from_tp, micro, where)

    for index in (0, 1):
        swaps[index][0].start()
        keeps[index].start()
    first.start()
    for index in (2, 3, 4):
        swaps[index][0].start()
        keeps[index].start()
    first.keep()
    head_ring, out_ring, down_ring, gate_ring, up_ring = rings
    for index in (0, 1):
        keeps[index].wait()
        swaps[index][1].wait_recv()
        rings[index].start(1)
    first.pass_on()
    for hop in range(2, chips // 2 + 1):
        head_ring.relay(hop)
        out_ring.relay(hop)
    for index in (2, 3, 4):
        keeps[index].wait()
        swaps[index][1].wait_recv()
    down_ring.start(1)
    first.finish()
    head_ring.arrive(chips // 2)
    later = Actions(
        [lambda ring=ring: ring.start(1) for ring in (gate_ring, up_ring)]
        + [lambda ring=ring, hop=hop: ring.relay(hop) for hop in range(2, chips // 2 + 1) for ring in (down_ring, gate_ring, up_ring)]
    )

    @pl.loop(0, micro * 2 * heads)
    def _(u):
        block, head = u // heads, u % heads
        tokens = pl.ds(pl.multiple_of(block * toks, 128), toks)
        columns = pl.ds(pl.multiple_of(head * unit_rows, 128), unit_rows)
        lines = mm(first_all[tokens, :], head_w[:, columns], ((1,), (0,))).T
        cosine, sine = cos_ref[:, tokens], sin_ref[:, tokens]
        for turn in range(group + 1):
            front = lines[turn * dim : turn * dim + half]
            back = lines[turn * dim + half : (turn + 1) * dim]
            unit_send[u, turn * dim : turn * dim + half, :] = (front * cosine - back * sine).astype(low)
            unit_send[u, turn * dim + half : (turn + 1) * dim, :] = (back * cosine + front * sine).astype(low)
        unit_send[u, (group + 1) * dim :, :] = lines[(group + 1) * dim :].astype(low)
        to_unit.send(u)

    later.run(1)
    cot.start()
    cot.keep()
    out_ring.arrive(chips // 2)
    saves = [
        pltpu.make_async_copy(head_w, head_o, save_sem.at[0]),
        pltpu.make_async_copy(out_w, out_o, save_sem.at[1]),
        pltpu.make_async_copy(first_all, first_o, save_sem.at[2]),
    ]
    for save in saves:
        save.start()
    later.run(2)
    cot.pass_on()
    to_unit.finish()

    score_scale = dim ** (-0.5)
    lay_out(unit_in, flat)
    saves.append(pltpu.make_async_copy(unit_in, unit_o, save_sem.at[3]))
    saves[-1].start()
    tokens = chips * toks
    key_rows = flat[group * dim : (group + 1) * dim, :].astype(f32).T.astype(low)
    for number, cols in enumerate(unit_chunks(tokens)):
        keep = allowed_keys(code_ref[...], last_ref[:, cols], start_ref[:, cols])
        for head in range(group):
            query_t = flat[head * dim : (head + 1) * dim, cols]
            scores = mm(key_rows, query_t, ((1,), (0,))) * score_scale
            scores = jnp.where(keep, scores, masked_score)
            maximum = jnp.max(scores, axis=0, keepdims=True)
            exponents = jnp.exp(scores - maximum)
            totals = jnp.sum(exponents, axis=0, keepdims=True)
            probs = (exponents * (1.0 / totals)).astype(low)
            stat_ref[head : head + 1, cols] = maximum + jnp.log(totals)
            result = mm(flat[(group + 1) * dim :, :], probs, ((1,), (0,))).astype(low)
            for piece in range(cols.start // toks, cols.stop // toks):
                start = piece * toks - cols.start
                att_send[piece, head * dim : (head + 1) * dim, :] = result[:, start : start + toks]
        for piece in range(cols.start // toks, cols.stop // toks):
            from_unit.send(piece)
        if number == 1:
            later.run(1)
    later.run(1)
    cot.finish()
    saves.append(pltpu.make_async_copy(cot_all, cot_o, save_sem.at[4]))
    saves[-1].start()
    from_unit.finish()
    saves.append(pltpu.make_async_copy(att_in, att_o, save_sem.at[5]))
    saves[-1].start()

    @pl.loop(0, micro * 2)
    def _(block):
        lines = jnp.concatenate([att_in[block * heads + head] for head in range(heads)], axis=0)
        lines = lines.astype(f32).T.astype(low)
        sums = mm(lines, out_w[...], ((1,), (1,)))
        parts[pl.ds(pl.multiple_of(block * toks, 128), toks), :] = sums.astype(low)
        fold.start(block // 2, block % 2)

    for m in range(micro):
        fold.send(m)
    later.run(1)
    for m in range(micro):
        own = slice(m * rows, (m + 1) * rows)
        residual = x_ref[own, :] + fold.result(m)
        residual_ref[own, :] = residual
        second_own[own, :] = (residual * norm_scale(residual) * gain_ref[...]).astype(low)
    second.start()
    second.keep()
    later.run(2)
    second.pass_on()
    second.finish()
    saves.append(pltpu.make_async_copy(second_all, second_o, save_sem.at[6]))
    saves[-1].start()
    later.run()
    for index, ring in enumerate((down_ring, gate_ring, up_ring)):
        ring.arrive(chips // 2)
        saves.append(pltpu.make_async_copy(weights[2 + index][1], weights[2 + index][2], save_sem.at[7 + index]))
        saves[-1].start()
    for save in saves:
        save.wait()
    for swap, _ in swaps:
        swap.wait_send()
    for part in rings + [first, second, cot, to_unit, from_unit, fold]:
        part.drain()


def forward_call(micro, group, chips, heads, *operands):
    x, first_rows, cot_rows, head_s, out_s, gate_s, up_s, down_s = operands[:8]
    own_rows, width = x.shape
    toks = own_rows // micro * 2
    all_rows = own_rows * 4
    pieces = micro * 2 * heads
    unit_rows, att_rows = (group + 2) * HEAD_SIZE, group * HEAD_SIZE
    shape = jax.ShapeDtypeStruct
    columns = [s.shape[1] // CORES for s in (head_s, out_s, gate_s, up_s, down_s)]
    any_spec, vmem_spec = pl.BlockSpec(memory_space=pl.ANY), pl.BlockSpec(memory_space=pltpu.VMEM)
    any_outs = [shape((width, c), low) for c in columns] + [shape((all_rows, width), low)] * 3
    any_outs += [shape((pieces, unit_rows, toks), low), shape((pieces, att_rows, toks), low)]
    vmem_outs = [shape((group, DOCUMENT_LIMIT), f32), shape((own_rows, width), f32)]
    scratch = [pltpu.VMEM((width, c), low) for c in columns]
    scratch += [
        pltpu.VMEM((all_rows, width), low),
        pltpu.VMEM((own_rows, width), low),
        pltpu.VMEM((all_rows, width), low),
        pltpu.VMEM((all_rows, width), low),
        pltpu.VMEM((pieces, unit_rows, toks), low),
        pltpu.VMEM((pieces, unit_rows, toks), low),
        pltpu.VMEM((unit_rows, DOCUMENT_LIMIT), low),
        pltpu.VMEM((pieces, att_rows, toks), low),
        pltpu.VMEM((pieces, att_rows, toks), low),
        pltpu.VMEM((all_rows, width), low),
        pltpu.VMEM((all_rows // 2, width), low),
        pltpu.VMEM((own_rows, width), low),
        pltpu.VMEM((own_rows, width), low),
        pltpu.SemaphoreType.DMA((96,)),
        pltpu.SemaphoreType.DMA((96,)),
        pltpu.SemaphoreType.DMA((5,)),
        pltpu.SemaphoreType.DMA((10,)),
    ]
    return pl.pallas_call(
        functools.partial(forward_kernel, micro, group, chips),
        out_shape=tuple(any_outs + vmem_outs),
        in_specs=[vmem_spec] * 3 + [any_spec] * 5 + [vmem_spec] * (len(operands) - 8),
        out_specs=tuple([any_spec] * len(any_outs) + [vmem_spec] * len(vmem_outs)),
        scratch_shapes=scratch,
        compiler_params=pltpu.CompilerParams(collective_id=0, has_side_effects=True, vmem_limit_bytes=60 << 20),
    )(*operands)


def vmem_call(kernel, outs, scratch, flops, *operands):
    spec = pl.BlockSpec(memory_space=pltpu.VMEM)
    moved = sum(math.prod(a.shape) * a.dtype.itemsize for a in operands + tuple(outs))
    return pl.pallas_call(
        kernel,
        out_shape=tuple(outs),
        in_specs=[spec] * len(operands),
        out_specs=tuple([spec] * len(outs)),
        scratch_shapes=scratch,
        cost_estimate=pl.CostEstimate(flops=flops, bytes_accessed=moved, transcendentals=2 * DOCUMENT_LIMIT**2),
        compiler_params=pltpu.CompilerParams(vmem_limit_bytes=48 << 20),
    )(*operands)


def on_device(
    block_input,
    segments,
    positions,
    query_weight,
    key_matrix,
    value_matrix,
    out_weight,
    gate_weight,
    up_weight,
    down_weight,
    gain_first,
    gain_second,
    cotangent,
):
    chips, tp_count = lax.axis_size("chip"), lax.axis_size("tp")
    chip, core = lax.axis_index("chip"), lax.axis_index("core")
    cp_count, cp_index = chips * CORES, chip * CORES + core
    micro, tok_dev, width = block_input.shape
    dim = HEAD_SIZE
    block_rows = tok_dev * tp_count // 2
    query_heads, value_heads = query_weight.shape[1] // dim, key_matrix.shape[1] // dim
    group = query_heads // value_heads
    unit_rows = (group + 2) * dim
    head_cores = CORES if value_heads % CORES == 0 else 1
    heads = value_heads // head_cores
    toks = head_cores * block_rows
    pieces = DOCUMENT_LIMIT // toks
    assert pieces == micro * 2 * heads and cp_count % (pieces * head_cores) == 0

    by_head = jnp.concatenate(
        [
            query_weight.reshape(-1, value_heads, group * dim),
            key_matrix.reshape(-1, value_heads, dim),
            value_matrix.reshape(-1, value_heads, dim),
        ],
        axis=2,
    ).reshape(query_weight.shape[0], -1)
    out_t, down_t = out_weight.T, down_weight.T

    def halves(matrix):
        half = matrix.shape[1] // 2
        return matrix[:, :half], matrix[:, half:]

    def gather_head_weight(matrix):
        if head_cores == 2:
            return ring_gather(core_split(*halves(matrix)))
        return lax.all_gather(matrix, ("chip", "core"), axis=0, tiled=True)

    def scatter_head_weight(grads):
        if head_cores == 2:
            return jnp.concatenate(core_merge(ring_scatter(grads)), axis=1)
        return lax.psum_scatter(grads, ("chip", "core"), scatter_dimension=0, tiled=True).astype(f32)

    fused = tp_count == 2 and head_cores == CORES and pieces == chips
    if not fused:
        head_full = gather_head_weight(by_head)
        out_full = gather_head_weight(out_t)
        gate_full = ring_gather(core_split(*halves(gate_weight)))
        up_full = ring_gather(core_split(*halves(up_weight)))
        down_full = ring_gather(core_split(*halves(down_t)))

    by_block = lambda line: line.reshape(micro, cp_count, 2, block_rows)
    group_cp = pieces * head_cores
    first_cp = cp_index // head_cores * head_cores
    row_pos = lax.dynamic_slice_in_dim(by_block(positions), first_cp, head_cores, 1)
    row_pos = row_pos.transpose(0, 2, 1, 3).reshape(-1)
    unit_index = cp_index // head_cores % pieces
    unit_micro, unit_half = unit_index // (2 * heads), unit_index // heads % 2

    def unit_line(line):
        mine = lax.dynamic_slice(
            by_block(line),
            (unit_micro, cp_index // group_cp * group_cp, unit_half, 0),
            (1, group_cp, 1, block_rows),
        )
        return mine.reshape(1, DOCUMENT_LIMIT)

    unit_pos, unit_seg = unit_line(positions), unit_line(segments)
    first_code = unit_seg * DOCUMENT_LIMIT
    last_code = first_code + unit_pos
    code_column = last_code.reshape(DOCUMENT_LIMIT, 1)
    cosine, sine = angles_of(row_pos)
    unit_cosine, unit_sine = angles_of(unit_pos.reshape(-1))

    if head_cores == 2:
        exchange_axis = "chip"
        groups = [[g + i for i in range(pieces)] for g in range(0, chips, pieces)]
    else:
        exchange_axis = ("chip", "core")
        groups = [[g + i for i in range(pieces)] for g in range(0, cp_count, pieces)]
    groups = None if len(groups) == 1 else groups

    def exchange(values):
        return lax.all_to_all(values, exchange_axis, 0, 0, axis_index_groups=groups)

    def to_units(values):
        rows = values.shape[0] // heads
        return values.reshape(heads, rows, micro * 2, toks).transpose(2, 0, 1, 3).reshape(pieces, rows, toks)

    def from_units(values):
        rows = values.shape[1]
        return values.reshape(micro * 2, heads, rows, toks).transpose(1, 2, 0, 3).reshape(heads * rows, -1)

    gather_head_rows = functools.partial(gather_rows, micro_count=micro, cores=head_cores)
    scatter_head_rows = functools.partial(scatter_rows, micro_count=micro, cores=head_cores)
    gather_all_rows = functools.partial(gather_rows, micro_count=micro, cores=CORES)
    scatter_all_rows = functools.partial(scatter_rows, micro_count=micro, cores=CORES)

    own_input = block_input.reshape(-1, width).astype(f32)
    cot_own = cotangent.reshape(-1, width)
    first_own = (own_input * norm_scale(own_input) * gain_first).astype(low)
    square = DOCUMENT_LIMIT * DOCUMENT_LIMIT * dim * 2 * group
    if fused:
        (
            head_full, out_full, gate_full, up_full, down_full, first_rows, second_rows, cot_rows, unit, att_pieces, unit_stat, residual
        ) = forward_call(
            micro, group, chips, heads,
            own_input, first_own, cot_own, by_head, out_t, gate_weight, up_weight, down_t,
            gain_second.reshape(1, -1), cosine, sine, code_column, last_code, first_code,
        )
        attended = from_units(att_pieces)
    else:
        first_rows = gather_head_rows(first_own)
        projected = mm(head_full, first_rows, ((0,), (1,))).reshape(heads, unit_rows, -1)
        turned = projected[:, : (group + 1) * dim].reshape(heads, group + 1, 2, dim // 2, -1)
        front, back = turned[:, :, 0], turned[:, :, 1]
        turned = jnp.stack([front * cosine - back * sine, back * cosine + front * sine], axis=2)
        projected = jnp.concatenate(
            [turned.reshape(heads, (group + 1) * dim, -1).astype(low), projected[:, (group + 1) * dim :].astype(low)], axis=1
        )
        unit = exchange(to_units(projected.reshape(heads * unit_rows, -1)))
        unit_out, unit_stat = vmem_call(
            functools.partial(attend_kernel, group),
            (
                jax.ShapeDtypeStruct((pieces, group * dim, toks), low),
                jax.ShapeDtypeStruct((group, DOCUMENT_LIMIT), f32),
            ),
            [pltpu.VMEM((unit_rows, DOCUMENT_LIMIT), low)],
            2 * square,
            unit,
            code_column,
            last_code,
            first_code,
        )
        attended = from_units(exchange(unit_out))
        residual = own_input + scatter_head_rows(mm(attended, out_full, ((0,), (1,))).astype(low))

        second_rows = gather_all_rows((residual * norm_scale(residual) * gain_second).astype(low))
        cot_rows = gather_all_rows(cot_own)
    gate_value = mm(second_rows, gate_full, ((1,), (0,)))
    upward = mm(second_rows, up_full, ((1,), (0,)))
    sigma = jax.nn.sigmoid(gate_value)
    active = gate_value * sigma
    hidden = (active * upward).astype(low)
    grad_hidden = mm(cot_rows, down_full, ((1,), (0,)))
    gate_back = (grad_hidden * upward * (sigma * (1.0 + gate_value * (1.0 - sigma)))).astype(low)
    up_back = (grad_hidden * active).astype(low)
    second_parts = (mm(gate_back, gate_full, ((1,), (1,))) + mm(up_back, up_full, ((1,), (1,)))).astype(low)
    grad_second_rows = scatter_all_rows(second_parts)
    down_grad = ring_scatter(mm(cot_rows, hidden, ((0,), (0,))).astype(low))
    gate_grad = ring_scatter(mm(second_rows, gate_back, ((0,), (0,))).astype(low))
    up_grad = ring_scatter(mm(second_rows, up_back, ((0,), (0,))).astype(low))
    output_rows = residual + scatter_all_rows(mm(hidden, down_full, ((1,), (1,))).astype(low))

    residual_part, gain_two = norm_back(residual, gain_second, grad_second_rows)
    grad_residual = cot_own.astype(f32) + residual_part
    grad_rows = gather_head_rows(grad_residual.astype(low))
    grad_attended = mm(out_full, grad_rows, ((0,), (1,))).astype(low)
    unit_grad = exchange(to_units(grad_attended))
    (unit_back,) = vmem_call(
        functools.partial(attend_back_kernel, group),
        (jax.ShapeDtypeStruct((pieces, unit_rows, toks), low),),
        [
            pltpu.VMEM((unit_rows, DOCUMENT_LIMIT), low),
            pltpu.VMEM((group * dim, DOCUMENT_LIMIT), low),
            pltpu.VMEM((dim, DOCUMENT_LIMIT), f32),
            pltpu.VMEM((dim, DOCUMENT_LIMIT), f32),
        ],
        5 * square,
        unit,
        unit_grad,
        code_column,
        last_code,
        first_code,
        unit_stat,
        unit_cosine,
        unit_sine,
    )
    back_rows = from_units(exchange(unit_back))
    grad_first_rows = scatter_head_rows(mm(back_rows, head_full, ((0,), (1,))).astype(low))
    head_grad = scatter_head_weight(mm(first_rows, back_rows, ((0,), (1,))).astype(low))
    out_grad = scatter_head_weight(mm(grad_rows, attended, ((0,), (1,))).astype(low))
    input_part, gain_one = norm_back(own_input, gain_first, grad_first_rows)
    input_grad = (grad_residual + input_part).astype(low)
    gain_sums = all_sum(jnp.stack([gain_one, gain_two]))

    head_grad = head_grad.reshape(-1, value_heads, unit_rows)
    columns = query_weight.shape[0]
    return (
        output_rows.astype(low).reshape(block_input.shape),
        input_grad.reshape(block_input.shape),
        head_grad[:, :, : group * dim].reshape(columns, -1),
        head_grad[:, :, group * dim : (group + 1) * dim].reshape(columns, -1),
        head_grad[:, :, (group + 1) * dim :].reshape(columns, -1),
        out_grad.T,
        jnp.concatenate(core_merge(gate_grad), axis=1),
        jnp.concatenate(core_merge(up_grad), axis=1),
        jnp.concatenate(core_merge(down_grad), axis=1).T,
        gain_sums[0],
        gain_sums[1],
    )


def solution(mesh):
    cp_count, tp_count = mesh.shape["cp"], mesh.shape["tp"]
    fine = Mesh(mesh.devices.reshape(cp_count // CORES, CORES, tp_count), ("chip", "core", "tp"))
    cp = ("chip", "core")
    rows = P(None, cp + ("tp",), None)
    wide, tall = P(cp, "tp"), P("tp", cp)
    return jax.shard_map(
        on_device,
        mesh=fine,
        in_specs=(rows, P(), P(), wide, wide, wide, tall, wide, wide, tall, P(), P(), rows),
        out_specs=(rows, rows, wide, wide, wide, tall, wide, wide, tall, P(), P()),
        check_vma=False,
    )
```

```python
import functools
import math

import jax
import jax.numpy as jnp
from jax import lax
from jax.experimental import pallas as pl
from jax.experimental.pallas import tpu as pltpu
from jax.sharding import Mesh
from jax.sharding import PartitionSpec as P

HEAD_SIZE = 96
DOCUMENT_LIMIT = 1024
CORES = 2

eps_norm = 1e-05
rope_base = 100000.0
masked_score = -1e30


f32 = jnp.float32
low = jnp.bfloat16


def mm(left, right, dims):
    return lax.dot_general(left, right, (dims, ((), ())), preferred_element_type=f32)


def pair_swap(values, axis):
    return lax.ppermute(values, axis, [(0, 1), (1, 0)])


def both(values, axis):
    other = pair_swap(values, axis)
    first = lax.axis_index(axis) == 0
    return jnp.stack([jnp.where(first, values, other), jnp.where(first, other, values)])


def split_pair(low_part, high_part, axis):
    first = lax.axis_index(axis) == 0
    return jnp.where(first, low_part, high_part), jnp.where(first, high_part, low_part)


def ring_of(count):
    order = list(range(0, count, 2)) + list(range(count - 1, 0, -2))
    place = [order.index(chip) for chip in range(count)]
    ahead = [(order[i], order[(i + 1) % count]) for i in range(count)]
    back = [(order[i], order[(i - 1) % count]) for i in range(count)]
    return order, place, ahead, back


def ring_gather(block):
    count = lax.axis_size("chip")
    order, place, ahead, back = ring_of(count)
    spot = jnp.array(place)[lax.axis_index("chip")]
    half_way, half_rows = count // 2, block.shape[0] // 2

    def put(whole, piece, step):
        owner = jnp.array(order)[(spot + step) % count]
        return lax.dynamic_update_index_in_dim(whole, piece, owner, 0)

    whole = put(jnp.zeros((count,) + block.shape, block.dtype), block, 0)
    up = down = block
    for step in range(1, half_way):
        up, down = lax.ppermute(up, "chip", ahead), lax.ppermute(down, "chip", back)
        whole = put(put(whole, up, count - step), down, step)
    up = lax.ppermute(up[:half_rows], "chip", ahead)
    down = lax.ppermute(down[half_rows:], "chip", back)
    whole = put(whole, jnp.concatenate([up, down], axis=0), half_way)
    return whole.reshape((count * block.shape[0],) + block.shape[1:])


def ring_scatter(terms):
    count = lax.axis_size("chip")
    order, place, ahead, back = ring_of(count)
    spot = jnp.array(place)[lax.axis_index("chip")]
    rows = terms.shape[0] // count
    half_way, half_rows = count // 2, rows // 2
    terms = terms.reshape((count, rows) + terms.shape[1:])

    def own(step):
        owner = jnp.array(order)[(spot + step) % count]
        return lax.dynamic_index_in_dim(terms, owner, 0, keepdims=False).astype(f32)

    far = own(half_way).astype(low)
    up = lax.ppermute(far[:half_rows], "chip", ahead)
    down = lax.ppermute(far[half_rows:], "chip", back)
    for step in range(half_way - 1, 0, -1):
        own_up, own_down = own(step), own(count - step)
        if step == half_way - 1:
            up = jnp.concatenate([own_up[:half_rows] + up.astype(f32), own_up[half_rows:]], axis=0)
            down = jnp.concatenate([own_down[:half_rows], own_down[half_rows:] + down.astype(f32)], axis=0)
        else:
            up, down = own_up + up.astype(f32), own_down + down.astype(f32)
        up = lax.ppermute(up.astype(low), "chip", ahead)
        down = lax.ppermute(down.astype(low), "chip", back)
    return own(0) + up.astype(f32) + down.astype(f32)


def core_split(low_part, high_part):
    kept, sent = split_pair(low_part, high_part, "core")
    other = pair_swap(sent, "core")
    first = lax.axis_index("core") == 0
    return jnp.concatenate([jnp.where(first, kept, other), jnp.where(first, other, kept)], axis=0)


def core_merge(rows):
    half = rows.shape[0] // 2
    kept, sent = split_pair(rows[:half], rows[half:], "core")
    other = pair_swap(sent.astype(low), "core").astype(f32)
    first = lax.axis_index("core") == 0
    return jnp.where(first, kept, other), jnp.where(first, other, kept)


def all_sum(values):
    for axis in ("tp", "core", "chip"):
        step = 1
        while step < lax.axis_size(axis):
            pairs = [(i, i ^ step) for i in range(lax.axis_size(axis))]
            values = values + lax.ppermute(values, axis, pairs)
            step *= 2
    return values


def gather_rows(rows, micro_count, cores):
    width = rows.shape[-1]
    tp_count = lax.axis_size("tp")
    joined = both(rows, "tp") if tp_count == 2 else lax.all_gather(rows, "tp", axis=0)
    joined = both(joined, "core") if cores == 2 else joined
    joined = joined.reshape((cores, 2, tp_count // 2, micro_count, -1, width))
    return joined.transpose((3, 1, 0, 2, 4, 5)).reshape((-1, width))


def scatter_rows(parts, micro_count, cores):
    width = parts.shape[-1]
    tp_count = lax.axis_size("tp")
    parts = parts.reshape((micro_count, 2, cores, tp_count // 2, -1, width)).transpose((2, 1, 3, 0, 4, 5))
    parts = parts.reshape((cores, tp_count, -1, width))
    if cores == 2:
        kept, sent = split_pair(parts[0], parts[1], "core")
        parts = (kept.astype(f32) + pair_swap(sent, "core").astype(f32)).astype(low)
    else:
        parts = parts[0]
    if tp_count == 2:
        kept, sent = split_pair(parts[0], parts[1], "tp")
        return kept.astype(f32) + pair_swap(sent, "tp").astype(f32)
    return lax.psum_scatter(parts, "tp", scatter_dimension=0, tiled=False).astype(f32)


def norm_scale(values):
    return lax.rsqrt(jnp.mean(values * values, axis=-1, keepdims=True) + eps_norm)


def norm_back(values, gain, grads):
    rho = norm_scale(values)
    scaled = grads * gain
    inner = jnp.mean(scaled * values, axis=-1, keepdims=True)
    return rho * scaled - values * (rho * rho * rho * inner), jnp.sum(grads * values * rho, axis=0)


def angles_of(spots):
    half_dim = HEAD_SIZE // 2
    frequency = jnp.exp(jnp.arange(half_dim, dtype=f32) * (-2.0 * math.log(rope_base) / HEAD_SIZE))
    angles = frequency[:, None] * spots.astype(f32)[None, :]
    return jnp.cos(angles), jnp.sin(angles)


def unit_chunks(tokens):
    width = min(256, tokens)
    return [slice(start, start + width) for start in range(0, tokens, width)]


def lay_out(pieces_ref, flat):
    count, _, width = pieces_ref.shape
    for piece in range(count):
        flat[:, piece * width : (piece + 1) * width] = pieces_ref[piece]


def allowed_keys(code_column, last_row, first_row):
    return (code_column <= last_row) & (code_column >= first_row)


def attend_kernel(group, pieces_ref, code_ref, last_ref, first_ref, out_ref, stat_ref, flat):
    dim = HEAD_SIZE
    count, _, width = pieces_ref.shape
    tokens = count * width
    score_scale = dim ** (-0.5)
    lay_out(pieces_ref, flat)
    key_rows = flat[group * dim : (group + 1) * dim, :].astype(f32).T.astype(low)
    value_t = flat[(group + 1) * dim :, :]
    for cols in unit_chunks(tokens):
        keep = allowed_keys(code_ref[...], last_ref[:, cols], first_ref[:, cols])
        for head in range(group):
            query_t = flat[head * dim : (head + 1) * dim, cols]
            scores = mm(key_rows, query_t, ((1,), (0,))) * score_scale
            scores = jnp.where(keep, scores, masked_score)
            maximum = jnp.max(scores, axis=0, keepdims=True)
            weights = jnp.exp(scores - maximum)
            totals = jnp.sum(weights, axis=0, keepdims=True)
            probs = (weights * (1.0 / totals)).astype(low)
            stat_ref[head : head + 1, cols] = maximum + jnp.log(totals)
            result = mm(value_t, probs, ((1,), (0,))).astype(low)
            for piece in range(cols.start // width, cols.stop // width):
                start = piece * width - cols.start
                out_ref[piece, head * dim : (head + 1) * dim, :] = result[:, start : start + width]


def attend_back_kernel(
    group, pieces_ref, grads_ref, code_ref, last_ref, first_ref, stat_ref, cos_ref, sin_ref, out_ref, flat, grad_flat, key_sum, value_sum
):
    dim = HEAD_SIZE
    half = dim // 2
    count, _, width = pieces_ref.shape
    tokens = count * width
    score_scale = dim ** (-0.5)
    lay_out(pieces_ref, flat)
    lay_out(grads_ref, grad_flat)
    key_t = flat[group * dim : (group + 1) * dim, :]
    key_rows = key_t.astype(f32).T.astype(low)
    value_rows = flat[(group + 1) * dim :, :].astype(f32).T.astype(low)

    def store(values, base, cols):
        for piece in range(cols.start // width, cols.stop // width):
            start = piece * width - cols.start
            out_ref[piece, base : base + values.shape[0], :] = values[:, start : start + width]

    def unturn(values, base, cols):
        front, back = values[:half] * score_scale, values[half:] * score_scale
        cosine, sine = cos_ref[:, cols], sin_ref[:, cols]
        store((front * cosine + back * sine).astype(low), base, cols)
        store((back * cosine - front * sine).astype(low), base + half, cols)

    for index, cols in enumerate(unit_chunks(tokens)):
        keep = allowed_keys(code_ref[...], last_ref[:, cols], first_ref[:, cols])
        for head in range(group):
            rows = slice(head * dim, (head + 1) * dim)
            query_t, grad_t = flat[rows, cols], grad_flat[rows, cols]
            scores = mm(key_rows, query_t, ((1,), (0,))) * score_scale
            probs = jnp.where(keep, jnp.exp(scores - stat_ref[head : head + 1, cols]), 0.0)
            grad_probs = mm(value_rows, grad_t, ((1,), (0,)))
            delta = jnp.sum(probs * grad_probs, axis=0, keepdims=True)
            grad_scores = (probs * (grad_probs - delta)).astype(low)
            unturn(mm(key_t, grad_scores, ((1,), (0,))), head * dim, cols)
            key_part = mm(query_t, grad_scores, ((1,), (1,)))
            value_part = mm(grad_t, probs.astype(low), ((1,), (1,)))
            if index == 0 and head == 0:
                key_sum[...] = key_part
                value_sum[...] = value_part
            else:
                key_sum[...] += key_part
                value_sum[...] += value_part
    everything = slice(0, tokens)
    unturn(key_sum[...], group * dim, everything)
    store(value_sum[...].astype(low), (group + 1) * dim, everything)


MESH_ID = pl.DeviceIdType.MESH


class Sems:
    def __init__(self, send, recv):
        self.send, self.recv, self.used = send, recv, 0

    def take(self, count=1):
        base = self.used
        self.used += count
        return base


def remote(sems, index, source, target, there, arrive=None):
    return pltpu.make_async_remote_copy(
        src_ref=source,
        dst_ref=target,
        send_sem=sems.send.at[index],
        recv_sem=sems.recv.at[index if arrive is None else arrive],
        device_id=there,
        device_id_type=MESH_ID,
    )


def greet(chips, chip, core, tp):
    barrier = pltpu.get_barrier_semaphore()

    @pl.loop(1, chips)
    def _(step):
        pl.semaphore_signal(barrier, inc=1, device_id={"chip": (chip + step) % chips}, device_id_type=MESH_ID)

    pl.semaphore_signal(barrier, inc=1, device_id={"core": 1 - core}, device_id_type=MESH_ID)
    pl.semaphore_signal(barrier, inc=1, device_id={"tp": 1 - tp}, device_id_type=MESH_ID)
    pl.semaphore_wait(barrier, chips + 1)


def spot_of(chip, count):
    odd = chip % 2
    return (1 - odd) * (chip // 2) + odd * (count - 1 - chip // 2)


def chip_at(spot, count):
    spot = (spot + count) % count
    far = spot // (count // 2)
    return (1 - far) * 2 * spot + far * (2 * (count - 1 - spot) + 1)


class Ring:
    def __init__(self, sems, whole, rows, count, chip):
        self.sems, self.whole, self.rows, self.count = sems, whole, rows, count
        self.spot = spot_of(chip, count)
        self.half = count // 2
        self.base = sems.take(2 * self.half)
        self.ways = (1, -1)

    def copy(self, side, hop, behind):
        way = self.ways[side]
        start = chip_at(self.spot - way * behind, self.count) * self.rows
        size = self.rows
        if hop == self.half:
            size = self.rows // 2
            start = start + side * size
        piece = self.whole.at[pl.ds(pl.multiple_of(start, 16), size), :]
        there = {"chip": chip_at(self.spot + way, self.count)}
        return remote(self.sems, self.base + side * self.half + hop - 1, piece, piece, there)

    def start(self, hop):
        for side in (0, 1):
            self.copy(side, hop, hop - 1).start()

    def arrive(self, hop):
        for side in (0, 1):
            self.copy(side, hop, hop).wait_recv()

    def relay(self, hop):
        for side in (0, 1):
            if hop > 1:
                self.copy(side, hop - 1, hop - 1).wait_recv()
            self.copy(side, hop, hop - 1).start()

    def drain(self):
        for side in (0, 1):
            for hop in range(1, self.half + 1):
                self.copy(side, hop, hop - 1).wait_send()


class Spread:
    def __init__(self, sems, source, whole, micro, chip_core_tp):
        self.sems, self.source, self.whole, self.micro = sems, source, whole, micro
        _, self.core, self.tp = chip_core_tp
        self.rows = source.shape[0] // micro
        self.base = sems.take(3 * micro)

    def place(self, m, half, core):
        start = ((m * 2 + half) * 2 + core) * self.rows
        return self.whole.at[pl.ds(pl.multiple_of(start, 16), self.rows), :]

    def own(self, m):
        return self.source.at[m * self.rows : (m + 1) * self.rows, :]

    def over_tp(self, m, half):
        target = self.place(m, half, self.core)
        return remote(self.sems, self.base + m, self.own(m), target, {"tp": 1 - self.tp})

    def over_core(self, m, core):
        target = self.place(m, self.tp, core)
        return remote(self.sems, self.base + self.micro + m, self.own(m), target, {"core": 1 - self.core})

    def passed_on(self, m, core):
        piece = self.place(m, 1 - self.tp, core)
        return remote(self.sems, self.base + 2 * self.micro + m, piece, piece, {"core": 1 - self.core})

    def start(self):
        for m in range(self.micro):
            self.over_tp(m, self.tp).start()
            self.over_core(m, self.core).start()

    def keep(self):
        for m in range(self.micro):
            start = ((m * 2 + self.tp) * 2 + self.core) * self.rows
            self.whole[pl.ds(pl.multiple_of(start, 16), self.rows), :] = self.source[m * self.rows : (m + 1) * self.rows, :]

    def pass_on(self):
        for m in range(self.micro):
            self.over_tp(m, 1 - self.tp).wait_recv()
            self.passed_on(m, self.core).start()

    def finish(self):
        for m in range(self.micro):
            self.over_core(m, 1 - self.core).wait_recv()
            self.passed_on(m, 1 - self.core).wait_recv()

    def drain(self):
        for m in range(self.micro):
            self.over_tp(m, self.tp).wait_send()
            self.over_core(m, self.core).wait_send()
            self.passed_on(m, self.core).wait_send()


class Fold:
    def __init__(self, sems, parts, from_core, to_tp, from_tp, micro, chip_core_tp):
        self.sems, self.parts, self.from_core, self.to_tp, self.from_tp = sems, parts, from_core, to_tp, from_tp
        self.micro = micro
        _, self.core, self.tp = chip_core_tp
        self.rows = from_tp.shape[0] // micro
        self.base = sems.take(3 * micro)

    def piece(self, m, half, core):
        start = ((m * 2 + half) * 2 + core) * self.rows
        return pl.ds(pl.multiple_of(start, 16), self.rows)

    def landing(self, m, half):
        return pl.ds(pl.multiple_of((m * 2 + half) * self.rows, 16), self.rows)

    def over_core(self, m, half):
        source = self.parts.at[self.piece(m, half, 1 - self.core), :]
        index = self.base + m * 2 + half
        return remote(self.sems, index, source, self.from_core.at[self.landing(m, half), :], {"core": 1 - self.core})

    def over_tp(self, m):
        rows = pl.ds(m * self.rows, self.rows)
        index = self.base + 2 * self.micro + m
        return remote(self.sems, index, self.to_tp.at[rows, :], self.from_tp.at[rows, :], {"tp": 1 - self.tp})

    def start(self, m, half):
        self.over_core(m, half).start()

    def summed(self, m, half):
        mine = self.parts[self.piece(m, half, self.core), :].astype(f32)
        return mine + self.from_core[self.landing(m, half), :].astype(f32)

    def send(self, m):
        for half in (0, 1):
            self.over_core(m, half).wait_recv()
        self.to_tp[m * self.rows : (m + 1) * self.rows, :] = self.summed(m, 1 - self.tp).astype(low)
        self.over_tp(m).start()

    def result(self, m):
        kept = self.summed(m, self.tp)
        self.over_tp(m).wait_recv()
        return kept + self.from_tp[m * self.rows : (m + 1) * self.rows, :].astype(f32)

    def drain(self):
        for m in range(self.micro):
            for half in (0, 1):
                self.over_core(m, half).wait_send()
            self.over_tp(m).wait_send()


class Exchange:
    def __init__(self, sems, outgoing, incoming, chips, chip):
        self.sems, self.outgoing, self.incoming, self.chips, self.chip = sems, outgoing, incoming, chips, chip
        self.base = sems.take(chips)

    def copy(self, to):
        return remote(
            self.sems, self.base + to, self.outgoing.at[to], self.incoming.at[self.chip], {"chip": to}, self.base + self.chip
        )

    def send(self, to):
        @pl.when(to != self.chip)
        def _():
            self.copy(to).start()

        @pl.when(to == self.chip)
        def _():
            self.incoming[to] = self.outgoing[to]

    def finish(self):
        @pl.loop(1, self.chips)
        def _(step):
            source = (self.chip + step) % self.chips
            remote(
                self.sems, self.base + source, self.outgoing.at[source], self.incoming.at[source], {"chip": source}
            ).wait_recv()

    def drain(self):
        @pl.loop(1, self.chips)
        def _(step):
            self.copy((self.chip + step) % self.chips).wait_send()


class Actions:
    def __init__(self, steps):
        self.steps = list(steps)

    def run(self, count=None):
        count = len(self.steps) if count is None else count
        for step in self.steps[:count]:
            step()
        self.steps = self.steps[count:]


def forward_kernel(
    micro, group, chips,
    x_ref, first_ref, cot_ref, head_ref, out_ref, gate_ref, up_ref, down_ref, gain_ref, cos_ref, sin_ref, code_ref, last_ref, start_ref,
    head_o, out_o, gate_o, up_o, down_o, first_o, second_o, cot_o, unit_o, att_o, stat_ref, residual_ref,
    head_w, out_w, gate_w, up_w, down_w, first_all, second_own, second_all, cot_all, unit_send, unit_in, flat, att_send, att_in,
    parts, from_core, to_tp, from_tp, send_sem, recv_sem, local_sem, save_sem,
):
    dim = HEAD_SIZE
    half = dim // 2
    chip, core, tp = lax.axis_index("chip"), lax.axis_index("core"), lax.axis_index("tp")
    where = (chip, core, tp)
    sems = Sems(send_sem, recv_sem)
    rows = x_ref.shape[0] // micro
    toks = 2 * rows
    heads = head_w.shape[1] // ((group + 2) * dim)
    unit_rows = (group + 2) * dim
    greet(chips, chip, core, tp)

    depth = head_ref.shape[0]
    weights = ((head_ref, head_w, head_o), (out_ref, out_w, out_o), (down_ref, down_w, down_o), (gate_ref, gate_w, gate_o), (up_ref, up_w, up_o))
    rings, swaps, keeps = [], [], []
    for index, (shard, whole, _) in enumerate(weights):
        columns = whole.shape[1]
        mine = whole.at[pl.ds(pl.multiple_of((chip * 2 + core) * depth, 16), depth), :]
        theirs = whole.at[pl.ds(pl.multiple_of((chip * 2 + 1 - core) * depth, 16), depth), :]
        at = sems.take()
        give = shard.at[:, pl.ds(pl.multiple_of((1 - core) * columns, 128), columns)]
        hold = shard.at[:, pl.ds(pl.multiple_of(core * columns, 128), columns)]
        swaps.append((remote(sems, at, give, mine, {"core": 1 - core}), remote(sems, at, give, theirs, {"core": 1 - core})))
        keeps.append(pltpu.make_async_copy(hold, mine, local_sem.at[index]))
        rings.append(Ring(sems, whole, 2 * depth, chips, chip))
    first, second, cot = (
        Spread(sems, first_ref, first_all, micro, where),
        Spread(sems, second_own, second_all, micro, where),
        Spread(sems, cot_ref, cot_all, micro, where),
    )
    to_unit = Exchange(sems, unit_send, unit_in, chips, chip)
    from_unit = Exchange(sems, att_send, att_in, chips, chip)
    fold = Fold(sems, parts, from_core, to_tp, from_tp, micro, where)

    for index in (0, 1):
        swaps[index][0].start()
        keeps[index].start()
    first.start()
    for index in (2, 3, 4):
        swaps[index][0].start()
        keeps[index].start()
    first.keep()
    head_ring, out_ring, down_ring, gate_ring, up_ring = rings
    for index in (0, 1):
        keeps[index].wait()
        swaps[index][1].wait_recv()
        rings[index].start(1)
    first.pass_on()
    for hop in range(2, chips // 2 + 1):
        head_ring.relay(hop)
        out_ring.relay(hop)
    for index in (2, 3, 4):
        keeps[index].wait()
        swaps[index][1].wait_recv()
    down_ring.start(1)
    first.finish()
    head_ring.arrive(chips // 2)
    later = Actions(
        [lambda ring=ring: ring.start(1) for ring in (gate_ring, up_ring)]
        + [lambda ring=ring, hop=hop: ring.relay(hop) for hop in range(2, chips // 2 + 1) for ring in (down_ring, gate_ring, up_ring)]
    )

    @pl.loop(0, micro * 2 * heads)
    def _(u):
        block, head = u // heads, u % heads
        tokens = pl.ds(pl.multiple_of(block * toks, 128), toks)
        columns = pl.ds(pl.multiple_of(head * unit_rows, 128), unit_rows)
        lines = mm(first_all[tokens, :], head_w[:, columns], ((1,), (0,))).T
        cosine, sine = cos_ref[:, tokens], sin_ref[:, tokens]
        for turn in range(group + 1):
            front = lines[turn * dim : turn * dim + half]
            back = lines[turn * dim + half : (turn + 1) * dim]
            unit_send[u, turn * dim : turn * dim + half, :] = (front * cosine - back * sine).astype(low)
            unit_send[u, turn * dim + half : (turn + 1) * dim, :] = (back * cosine + front * sine).astype(low)
        unit_send[u, (group + 1) * dim :, :] = lines[(group + 1) * dim :].astype(low)
        to_unit.send(u)

    later.run(1)
    cot.start()
    cot.keep()
    out_ring.arrive(chips // 2)
    saves = [
        pltpu.make_async_copy(head_w, head_o, save_sem.at[0]),
        pltpu.make_async_copy(out_w, out_o, save_sem.at[1]),
        pltpu.make_async_copy(first_all, first_o, save_sem.at[2]),
    ]
    for save in saves:
        save.start()
    later.run(2)
    cot.pass_on()
    to_unit.finish()

    score_scale = dim ** (-0.5)
    lay_out(unit_in, flat)
    saves.append(pltpu.make_async_copy(unit_in, unit_o, save_sem.at[3]))
    saves[-1].start()
    tokens = chips * toks
    key_rows = flat[group * dim : (group + 1) * dim, :].astype(f32).T.astype(low)
    for number, cols in enumerate(unit_chunks(tokens)):
        keep = allowed_keys(code_ref[...], last_ref[:, cols], start_ref[:, cols])
        for head in range(group):
            query_t = flat[head * dim : (head + 1) * dim, cols]
            scores = mm(key_rows, query_t, ((1,), (0,))) * score_scale
            scores = jnp.where(keep, scores, masked_score)
            maximum = jnp.max(scores, axis=0, keepdims=True)
            exponents = jnp.exp(scores - maximum)
            totals = jnp.sum(exponents, axis=0, keepdims=True)
            probs = (exponents * (1.0 / totals)).astype(low)
            stat_ref[head : head + 1, cols] = maximum + jnp.log(totals)
            result = mm(flat[(group + 1) * dim :, :], probs, ((1,), (0,))).astype(low)
            for piece in range(cols.start // toks, cols.stop // toks):
                start = piece * toks - cols.start
                att_send[piece, head * dim : (head + 1) * dim, :] = result[:, start : start + toks]
        for piece in range(cols.start // toks, cols.stop // toks):
            from_unit.send(piece)
        if number == 1:
            later.run(1)
    later.run(1)
    cot.finish()
    saves.append(pltpu.make_async_copy(cot_all, cot_o, save_sem.at[4]))
    saves[-1].start()
    from_unit.finish()
    saves.append(pltpu.make_async_copy(att_in, att_o, save_sem.at[5]))
    saves[-1].start()

    @pl.loop(0, micro * 2)
    def _(block):
        lines = jnp.concatenate([att_in[block * heads + head] for head in range(heads)], axis=0)
        lines = lines.astype(f32).T.astype(low)
        sums = mm(lines, out_w[...], ((1,), (1,)))
        parts[pl.ds(pl.multiple_of(block * toks, 128), toks), :] = sums.astype(low)
        fold.start(block // 2, block % 2)

    for m in range(micro):
        fold.send(m)
    later.run(1)
    for m in range(micro):
        own = slice(m * rows, (m + 1) * rows)
        residual = x_ref[own, :] + fold.result(m)
        residual_ref[own, :] = residual
        second_own[own, :] = (residual * norm_scale(residual) * gain_ref[...]).astype(low)
    second.start()
    second.keep()
    later.run(2)
    second.pass_on()
    second.finish()
    saves.append(pltpu.make_async_copy(second_all, second_o, save_sem.at[6]))
    saves[-1].start()
    later.run()
    for index, ring in enumerate((down_ring, gate_ring, up_ring)):
        ring.arrive(chips // 2)
        saves.append(pltpu.make_async_copy(weights[2 + index][1], weights[2 + index][2], save_sem.at[7 + index]))
        saves[-1].start()
    for save in saves:
        save.wait()
    for swap, _ in swaps:
        swap.wait_send()
    for part in rings + [first, second, cot, to_unit, from_unit, fold]:
        part.drain()


def forward_call(micro, group, chips, heads, *operands):
    x, first_rows, cot_rows, head_s, out_s, gate_s, up_s, down_s = operands[:8]
    own_rows, width = x.shape
    toks = own_rows // micro * 2
    all_rows = own_rows * 4
    pieces = micro * 2 * heads
    unit_rows, att_rows = (group + 2) * HEAD_SIZE, group * HEAD_SIZE
    shape = jax.ShapeDtypeStruct
    columns = [s.shape[1] // CORES for s in (head_s, out_s, gate_s, up_s, down_s)]
    any_spec, vmem_spec = pl.BlockSpec(memory_space=pl.ANY), pl.BlockSpec(memory_space=pltpu.VMEM)
    any_outs = [shape((width, c), low) for c in columns] + [shape((all_rows, width), low)] * 3
    any_outs += [shape((pieces, unit_rows, toks), low), shape((pieces, att_rows, toks), low)]
    vmem_outs = [shape((group, DOCUMENT_LIMIT), f32), shape((own_rows, width), f32)]
    scratch = [pltpu.VMEM((width, c), low) for c in columns]
    scratch += [
        pltpu.VMEM((all_rows, width), low),
        pltpu.VMEM((own_rows, width), low),
        pltpu.VMEM((all_rows, width), low),
        pltpu.VMEM((all_rows, width), low),
        pltpu.VMEM((pieces, unit_rows, toks), low),
        pltpu.VMEM((pieces, unit_rows, toks), low),
        pltpu.VMEM((unit_rows, DOCUMENT_LIMIT), low),
        pltpu.VMEM((pieces, att_rows, toks), low),
        pltpu.VMEM((pieces, att_rows, toks), low),
        pltpu.VMEM((all_rows, width), low),
        pltpu.VMEM((all_rows // 2, width), low),
        pltpu.VMEM((own_rows, width), low),
        pltpu.VMEM((own_rows, width), low),
        pltpu.SemaphoreType.DMA((96,)),
        pltpu.SemaphoreType.DMA((96,)),
        pltpu.SemaphoreType.DMA((5,)),
        pltpu.SemaphoreType.DMA((10,)),
    ]
    return pl.pallas_call(
        functools.partial(forward_kernel, micro, group, chips),
        out_shape=tuple(any_outs + vmem_outs),
        in_specs=[vmem_spec] * 3 + [any_spec] * 5 + [vmem_spec] * (len(operands) - 8),
        out_specs=tuple([any_spec] * len(any_outs) + [vmem_spec] * len(vmem_outs)),
        scratch_shapes=scratch,
        compiler_params=pltpu.CompilerParams(collective_id=0, has_side_effects=True, vmem_limit_bytes=60 << 20),
    )(*operands)


class RingSum:
    def __init__(self, sems, terms, slots, count, chip, core):
        self.sems, self.terms, self.slots, self.count, self.chip, self.core = sems, terms, slots, count, chip, core
        self.rows = terms.shape[0] // count
        self.spot = spot_of(chip, count)
        self.half = count // 2
        self.base = sems.take(2 * self.half)
        self.ways = (1, -1)

    def slot(self, side, hop):
        return (side * self.half + hop - 1) * self.rows

    def term(self, side, distance):
        return chip_at(self.spot + self.ways[side] * distance, self.count) * self.rows

    def copy(self, side, hop):
        there = {"chip": chip_at(self.spot + self.ways[side], self.count)}
        index = self.base + side * self.half + hop - 1
        if hop == 1:
            size = self.rows // 2
            source = self.terms.at[pl.ds(pl.multiple_of(self.term(side, self.half) + side * size, 16), size), :]
            target = self.slots.at[pl.ds(self.slot(side, 1) + side * size, size), :]
        else:
            source = self.slots.at[pl.ds(self.slot(side, hop - 1), self.rows), :]
            target = self.slots.at[pl.ds(self.slot(side, hop), self.rows), :]
        return remote(self.sems, index, source, target, there)

    def start(self):
        for side in (0, 1):
            self.copy(side, 1).start()

    def relay(self, hop):
        size = self.rows // 2
        for side in (0, 1):
            self.copy(side, hop - 1).wait_recv()
            start, at = self.term(side, self.half - hop + 1), self.slot(side, hop - 1)
            for part in (0, 1):
                here = pl.ds(at + part * size, size)
                own = self.terms[pl.ds(pl.multiple_of(start + part * size, 16), size), :]
                if hop == 2 and part != side:
                    self.slots[here, :] = own
                else:
                    self.slots[here, :] = (own.astype(f32) + self.slots[here, :].astype(f32)).astype(low)
            self.copy(side, hop).start()

    def arrive(self):
        for side in (0, 1):
            self.copy(side, self.half).wait_recv()

    def result(self, part):
        size = self.rows // 2
        own = self.terms[pl.ds(pl.multiple_of(self.chip * self.rows + part * size, 16), size), :].astype(f32)
        for side in (0, 1):
            own = own + self.slots[pl.ds(pl.multiple_of(self.slot(side, self.half) + part * size, 16), size), :].astype(f32)
        return own

    def drain(self):
        for side in (0, 1):
            for hop in range(1, self.half + 1):
                self.copy(side, hop).wait_send()


class Merge:
    def __init__(self, sems, ring, leaving, landing, out, core):
        self.sems, self.ring, self.leaving, self.landing, self.out, self.core = sems, ring, leaving, landing, out, core
        self.index = sems.take()

    def copy(self):
        return remote(self.sems, self.index, self.leaving, self.landing, {"core": 1 - self.core})

    def send(self):
        self.ring.arrive()
        self.leaving[...] = self.ring.result(1 - self.core).astype(low)
        self.copy().start()
        columns = self.leaving.shape[1]
        self.out[:, pl.ds(pl.multiple_of(self.core * columns, 128), columns)] = self.ring.result(self.core)

    def finish(self):
        columns = self.leaving.shape[1]
        self.copy().wait_recv()
        self.out[:, pl.ds(pl.multiple_of((1 - self.core) * columns, 128), columns)] = self.landing[...].astype(f32)

    def drain(self):
        self.copy().wait_send()


class Butterfly:
    def __init__(self, sems, leaving, landing, chips, where):
        self.sems, self.leaving, self.landing = sems, leaving, landing
        chip, core, tp = where
        self.partners = [{"tp": 1 - tp}, {"core": 1 - core}]
        step = 1
        while step < chips:
            self.partners.append({"chip": chip + step - 2 * step * (chip // step % 2)})
            step *= 2
        self.base = sems.take(len(self.partners))

    def copy(self, stage):
        return remote(self.sems, self.base + stage, self.leaving.at[stage], self.landing.at[stage], self.partners[stage])

    def start(self, values):
        self.leaving[0] = values
        self.copy(0).start()

    def step(self, stage):
        self.copy(stage).wait_recv()
        values = self.leaving[stage] + self.landing[stage]
        if stage + 1 < len(self.partners):
            self.leaving[stage + 1] = values
            self.copy(stage + 1).start()
        return values

    def drain(self):
        for stage in range(len(self.partners)):
            self.copy(stage).wait_send()


def backward_kernel(
    micro, group, chips,
    x_ref, residual_ref, cot_ref, gain_one_ref, gain_two_ref, second_parts, output_parts, down_terms, gate_terms, up_terms,
    head_w, out_w, first_t, att_ref, unit_ref, code_ref, last_ref, start_ref, stat_ref, cos_ref, sin_ref,
    output_ref, input_grad_ref, head_g, out_g, gate_g, up_g, down_g, gains_ref,
    core_a, to_tp_a, from_tp_a, core_b, to_tp_b, from_tp_b, core_c, to_tp_c, from_tp_c, grad_residual, grad_own, grad_all,
    grad_send, grad_in, flat, grad_flat, key_sum, value_sum, back_send, back_in, att_flat, back_flat, back_rows, first_parts,
    head_terms, out_terms, head_slots, out_slots, down_slots, gate_slots, up_slots,
    head_leave, out_leave, down_leave, gate_leave, up_leave, head_land, out_land, down_land, gate_land, up_land,
    gain_leave, gain_land, send_sem, recv_sem,
):
    dim = HEAD_SIZE
    half = dim // 2
    chip, core, tp = lax.axis_index("chip"), lax.axis_index("core"), lax.axis_index("tp")
    where = (chip, core, tp)
    sems = Sems(send_sem, recv_sem)
    rows = x_ref.shape[0] // micro
    toks = 2 * rows
    unit_rows = (group + 2) * dim
    heads = head_w.shape[1] // unit_rows
    blocks = micro * 2
    greet(chips, chip, core, tp)

    down_ring, gate_ring, up_ring, out_ring, head_ring = (
        RingSum(sems, down_terms, down_slots, chips, chip, core),
        RingSum(sems, gate_terms, gate_slots, chips, chip, core),
        RingSum(sems, up_terms, up_slots, chips, chip, core),
        RingSum(sems, out_terms, out_slots, chips, chip, core),
        RingSum(sems, head_terms, head_slots, chips, chip, core),
    )
    down_merge, gate_merge, up_merge, out_merge, head_merge = (
        Merge(sems, down_ring, down_leave, down_land, down_g, core),
        Merge(sems, gate_ring, gate_leave, gate_land, gate_g, core),
        Merge(sems, up_ring, up_leave, up_land, up_g, core),
        Merge(sems, out_ring, out_leave, out_land, out_g, core),
        Merge(sems, head_ring, head_leave, head_land, head_g, core),
    )
    second_fold = Fold(sems, second_parts, core_a, to_tp_a, from_tp_a, micro, where)
    output_fold = Fold(sems, output_parts, core_b, to_tp_b, from_tp_b, micro, where)
    first_fold = Fold(sems, first_parts, core_c, to_tp_c, from_tp_c, micro, where)
    spread = Spread(sems, grad_own, grad_all, micro, where)
    to_unit = Exchange(sems, grad_send, grad_in, chips, chip)
    from_unit = Exchange(sems, back_send, back_in, chips, chip)
    butterfly = Butterfly(sems, gain_leave, gain_land, chips, where)
    hops = chips // 2
    later = Actions([lambda ring=ring, hop=hop: ring.relay(hop) for hop in range(2, hops + 1) for ring in (down_ring, gate_ring, up_ring)])

    for m in range(micro):
        for side in (0, 1):
            second_fold.start(m, side)
    for ring in (down_ring, gate_ring, up_ring):
        ring.start()

    def norm_rows_back(values, gain, grads):
        rho = norm_scale(values)
        scaled = grads * gain
        inner = jnp.mean(scaled * values, axis=-1, keepdims=True)
        return rho * scaled - values * (rho * rho * rho * inner), jnp.sum(grads * values * rho, axis=0, keepdims=True)

    for m in range(micro):
        second_fold.send(m)
    later.run(1)
    gain_two = None
    for m in range(micro):
        own = slice(m * rows, (m + 1) * rows)
        part, gain_now = norm_rows_back(residual_ref[own, :], gain_two_ref[...], second_fold.result(m))
        gain_two = gain_now if gain_two is None else gain_two + gain_now
        grads = cot_ref[own, :].astype(f32) + part
        grad_residual[own, :] = grads
        grad_own[own, :] = grads.astype(low)
    spread.start()
    spread.keep()
    for m in range(micro):
        for side in (0, 1):
            output_fold.start(m, side)
    lay_out(unit_ref, flat)
    for piece in range(blocks * heads):
        block, head = piece // heads, piece % heads
        att_flat[head * group * dim : (head + 1) * group * dim, block * toks : (block + 1) * toks] = att_ref[piece]
    key_t = flat[group * dim : (group + 1) * dim, :]
    key_rows = key_t.astype(f32).T.astype(low)
    value_rows = flat[(group + 1) * dim :, :].astype(f32).T.astype(low)
    later.run(1)
    spread.pass_on()
    later.run(1)
    spread.finish()

    @pl.loop(0, blocks)
    def _(block):
        tokens = pl.ds(pl.multiple_of(block * toks, 128), toks)
        lines = mm(grad_all[tokens, :], out_w[...], ((1,), (0,))).T.astype(low)
        for head in range(heads):
            piece = block * heads + head
            grad_send[piece] = lines[head * group * dim : (head + 1) * group * dim]
            to_unit.send(piece)

    later.run(1)
    for m in range(micro):
        output_fold.send(m)
    lanes = 256

    @pl.loop(0, grad_all.shape[1] // lanes)
    def _(part):
        columns = pl.ds(pl.multiple_of(part * lanes, 128), lanes)
        out_terms[columns, :] = mm(att_flat[...], grad_all[:, columns], ((1,), (0,))).T.astype(low)

    out_ring.start()
    later.run(1)
    to_unit.finish()
    lay_out(grad_in, grad_flat)

    score_scale = dim ** (-0.5)
    tokens_all = chips * toks

    def store(values, base, cols):
        for piece in range(cols.start // toks, cols.stop // toks):
            start = piece * toks - cols.start
            back_send[piece, base : base + values.shape[0], :] = values[:, start : start + toks]

    def unturn(values, base, cols):
        front, back = values[:half] * score_scale, values[half:] * score_scale
        cosine, sine = cos_ref[:, cols], sin_ref[:, cols]
        store((front * cosine + back * sine).astype(low), base, cols)
        store((back * cosine - front * sine).astype(low), base + half, cols)

    for index, cols in enumerate(unit_chunks(tokens_all)):
        keep = allowed_keys(code_ref[...], last_ref[:, cols], start_ref[:, cols])
        for head in range(group):
            lines = slice(head * dim, (head + 1) * dim)
            query_t, grad_t = flat[lines, cols], grad_flat[lines, cols]
            scores = mm(key_rows, query_t, ((1,), (0,))) * score_scale
            probs = jnp.where(keep, jnp.exp(scores - stat_ref[head : head + 1, cols]), 0.0)
            grad_probs = mm(value_rows, grad_t, ((1,), (0,)))
            delta = jnp.sum(probs * grad_probs, axis=0, keepdims=True)
            grad_scores = (probs * (grad_probs - delta)).astype(low)
            unturn(mm(key_t, grad_scores, ((1,), (0,))), head * dim, cols)
            key_part = mm(query_t, grad_scores, ((1,), (1,)))
            value_part = mm(grad_t, probs.astype(low), ((1,), (1,)))
            if index == 0 and head == 0:
                key_sum[...] = key_part
                value_sum[...] = value_part
            else:
                key_sum[...] += key_part
                value_sum[...] += value_part
        if index == 1:
            later.run(1)
    everything = slice(0, tokens_all)
    unturn(key_sum[...], group * dim, everything)
    store(value_sum[...].astype(low), (group + 1) * dim, everything)
    for piece in range(chips):
        from_unit.send(piece)
    later.run(1)
    for m in range(micro):
        own = slice(m * rows, (m + 1) * rows)
        output_ref[own, :] = (residual_ref[own, :] + output_fold.result(m)).astype(low)
    later.run(1)
    from_unit.finish()

    @pl.loop(0, blocks)
    def _(block):
        lines = jnp.concatenate([back_in[block * heads + head] for head in range(heads)], axis=0)
        tokens = pl.ds(pl.multiple_of(block * toks, 128), toks)
        back_flat[:, tokens] = lines
        back_rows[tokens, :] = lines.astype(f32).T.astype(low)

    depth = head_ring.rows

    def head_term(side, distance):
        here = pl.ds(pl.multiple_of(head_ring.term(side, distance), 16), depth)
        head_terms[here, :] = mm(first_t[here, :], back_flat[...], ((1,), (1,))).astype(low)

    head_term(0, hops)
    head_ring.start()
    for block in range(blocks):
        tokens = slice(block * toks, (block + 1) * toks)
        first_parts[tokens, :] = mm(back_rows[tokens, :], head_w[...], ((1,), (1,))).astype(low)
        first_fold.start(block // 2, block % 2)
    head_term(0, hops - 1)
    head_term(1, hops - 1)
    later.run(1)
    head_ring.relay(2)
    for m in range(micro):
        first_fold.send(m)
    for distance in range(hops - 2, 0, -1):
        head_term(0, distance)
        head_term(1, distance)
    head_term(0, 0)
    later.run()
    for hop in range(2, hops + 1):
        if hop > 2:
            head_ring.relay(hop)
        out_ring.relay(hop)
        if hop == 2:
            down_merge.send()
    gain_one = None
    for m in range(micro):
        own = slice(m * rows, (m + 1) * rows)
        part, gain_now = norm_rows_back(x_ref[own, :], gain_one_ref[...], first_fold.result(m))
        gain_one = gain_now if gain_one is None else gain_one + gain_now
        input_grad_ref[own, :] = (grad_residual[own, :] + part).astype(low)
    butterfly.start(jnp.concatenate([gain_one, gain_two], axis=0))
    gate_merge.send()
    butterfly.step(0)
    up_merge.send()
    butterfly.step(1)
    down_merge.finish()
    for stage in range(2, len(butterfly.partners) - 1):
        butterfly.step(stage)
    out_merge.send()
    gate_merge.finish()
    head_merge.send()
    up_merge.finish()
    gains_ref[...] = butterfly.step(len(butterfly.partners) - 1)
    out_merge.finish()
    head_merge.finish()
    parts = [down_ring, gate_ring, up_ring, out_ring, head_ring, down_merge, gate_merge, up_merge, out_merge, head_merge]
    parts += [second_fold, output_fold, first_fold, spread, to_unit, from_unit, butterfly]
    for part in parts:
        part.drain()


def backward_call(micro, group, chips, heads, *operands):
    own_rows, width = operands[0].shape
    toks = own_rows // micro * 2
    all_rows = own_rows * 4
    pieces = micro * 2 * heads
    unit_rows, att_rows = (group + 2) * HEAD_SIZE, group * HEAD_SIZE
    shape = jax.ShapeDtypeStruct
    hidden = operands[7].shape[1]
    depth = width // chips
    columns = [heads * unit_rows, heads * att_rows, hidden, hidden, hidden]
    stages = 2 + (chips - 1).bit_length()
    spec = pl.BlockSpec(memory_space=pltpu.VMEM)
    outs = [shape((own_rows, width), low)] * 2 + [shape((depth // 2, 2 * c), f32) for c in columns] + [shape((2, width), f32)]
    fold_scratch = [pltpu.VMEM((all_rows // 2, width), low), pltpu.VMEM((own_rows, width), low), pltpu.VMEM((own_rows, width), low)]
    scratch = fold_scratch * 3
    scratch += [
        pltpu.VMEM((own_rows, width), f32),
        pltpu.VMEM((own_rows, width), low),
        pltpu.VMEM((all_rows, width), low),
        pltpu.VMEM((pieces, att_rows, toks), low),
        pltpu.VMEM((pieces, att_rows, toks), low),
        pltpu.VMEM((unit_rows, DOCUMENT_LIMIT), low),
        pltpu.VMEM((att_rows, DOCUMENT_LIMIT), low),
        pltpu.VMEM((HEAD_SIZE, DOCUMENT_LIMIT), f32),
        pltpu.VMEM((HEAD_SIZE, DOCUMENT_LIMIT), f32),
        pltpu.VMEM((pieces, unit_rows, toks), low),
        pltpu.VMEM((pieces, unit_rows, toks), low),
        pltpu.VMEM((heads * att_rows, all_rows), low),
        pltpu.VMEM((heads * unit_rows, all_rows), low),
        pltpu.VMEM((all_rows, heads * unit_rows), low),
        pltpu.VMEM((all_rows, width), low),
        pltpu.VMEM((width, heads * unit_rows), low),
        pltpu.VMEM((width, heads * att_rows), low),
    ]
    scratch += [pltpu.VMEM((chips * depth, c), low) for c in columns]
    scratch += [pltpu.VMEM((depth // 2, c), low) for c in columns] * 2
    scratch += [pltpu.VMEM((stages, 2, width), f32)] * 2
    scratch += [pltpu.SemaphoreType.DMA((128,))] * 2
    return pl.pallas_call(
        functools.partial(backward_kernel, micro, group, chips),
        out_shape=tuple(outs),
        in_specs=[spec] * len(operands),
        out_specs=tuple([spec] * len(outs)),
        scratch_shapes=scratch,
        compiler_params=pltpu.CompilerParams(collective_id=1, has_side_effects=True, vmem_limit_bytes=63 << 20),
    )(*operands)


def vmem_call(kernel, outs, scratch, flops, *operands):
    spec = pl.BlockSpec(memory_space=pltpu.VMEM)
    moved = sum(math.prod(a.shape) * a.dtype.itemsize for a in operands + tuple(outs))
    return pl.pallas_call(
        kernel,
        out_shape=tuple(outs),
        in_specs=[spec] * len(operands),
        out_specs=tuple([spec] * len(outs)),
        scratch_shapes=scratch,
        cost_estimate=pl.CostEstimate(flops=flops, bytes_accessed=moved, transcendentals=2 * DOCUMENT_LIMIT**2),
        compiler_params=pltpu.CompilerParams(vmem_limit_bytes=48 << 20),
    )(*operands)


def on_device(
    block_input,
    segments,
    positions,
    query_weight,
    key_matrix,
    value_matrix,
    out_weight,
    gate_weight,
    up_weight,
    down_weight,
    gain_first,
    gain_second,
    cotangent,
):
    chips, tp_count = lax.axis_size("chip"), lax.axis_size("tp")
    chip, core = lax.axis_index("chip"), lax.axis_index("core")
    cp_count, cp_index = chips * CORES, chip * CORES + core
    micro, tok_dev, width = block_input.shape
    dim = HEAD_SIZE
    block_rows = tok_dev * tp_count // 2
    query_heads, value_heads = query_weight.shape[1] // dim, key_matrix.shape[1] // dim
    group = query_heads // value_heads
    unit_rows = (group + 2) * dim
    head_cores = CORES if value_heads % CORES == 0 else 1
    heads = value_heads // head_cores
    toks = head_cores * block_rows
    pieces = DOCUMENT_LIMIT // toks
    assert pieces == micro * 2 * heads and cp_count % (pieces * head_cores) == 0

    by_head = jnp.concatenate(
        [
            query_weight.reshape(-1, value_heads, group * dim),
            key_matrix.reshape(-1, value_heads, dim),
            value_matrix.reshape(-1, value_heads, dim),
        ],
        axis=2,
    ).reshape(query_weight.shape[0], -1)
    out_t, down_t = out_weight.T, down_weight.T

    def halves(matrix):
        half = matrix.shape[1] // 2
        return matrix[:, :half], matrix[:, half:]

    def gather_head_weight(matrix):
        if head_cores == 2:
            return ring_gather(core_split(*halves(matrix)))
        return lax.all_gather(matrix, ("chip", "core"), axis=0, tiled=True)

    def scatter_head_weight(grads):
        if head_cores == 2:
            return jnp.concatenate(core_merge(ring_scatter(grads)), axis=1)
        return lax.psum_scatter(grads, ("chip", "core"), scatter_dimension=0, tiled=True).astype(f32)

    fused = tp_count == 2 and head_cores == CORES and pieces == chips
    if not fused:
        head_full = gather_head_weight(by_head)
        out_full = gather_head_weight(out_t)
        gate_full = ring_gather(core_split(*halves(gate_weight)))
        up_full = ring_gather(core_split(*halves(up_weight)))
        down_full = ring_gather(core_split(*halves(down_t)))

    by_block = lambda line: line.reshape(micro, cp_count, 2, block_rows)
    group_cp = pieces * head_cores
    first_cp = cp_index // head_cores * head_cores
    row_pos = lax.dynamic_slice_in_dim(by_block(positions), first_cp, head_cores, 1)
    row_pos = row_pos.transpose(0, 2, 1, 3).reshape(-1)
    unit_index = cp_index // head_cores % pieces
    unit_micro, unit_half = unit_index // (2 * heads), unit_index // heads % 2

    def unit_line(line):
        mine = lax.dynamic_slice(
            by_block(line),
            (unit_micro, cp_index // group_cp * group_cp, unit_half, 0),
            (1, group_cp, 1, block_rows),
        )
        return mine.reshape(1, DOCUMENT_LIMIT)

    unit_pos, unit_seg = unit_line(positions), unit_line(segments)
    first_code = unit_seg * DOCUMENT_LIMIT
    last_code = first_code + unit_pos
    code_column = last_code.reshape(DOCUMENT_LIMIT, 1)
    cosine, sine = angles_of(row_pos)
    unit_cosine, unit_sine = angles_of(unit_pos.reshape(-1))

    if head_cores == 2:
        exchange_axis = "chip"
        groups = [[g + i for i in range(pieces)] for g in range(0, chips, pieces)]
    else:
        exchange_axis = ("chip", "core")
        groups = [[g + i for i in range(pieces)] for g in range(0, cp_count, pieces)]
    groups = None if len(groups) == 1 else groups

    def exchange(values):
        return lax.all_to_all(values, exchange_axis, 0, 0, axis_index_groups=groups)

    def to_units(values):
        rows = values.shape[0] // heads
        return values.reshape(heads, rows, micro * 2, toks).transpose(2, 0, 1, 3).reshape(pieces, rows, toks)

    def from_units(values):
        rows = values.shape[1]
        return values.reshape(micro * 2, heads, rows, toks).transpose(1, 2, 0, 3).reshape(heads * rows, -1)

    gather_head_rows = functools.partial(gather_rows, micro_count=micro, cores=head_cores)
    scatter_head_rows = functools.partial(scatter_rows, micro_count=micro, cores=head_cores)
    gather_all_rows = functools.partial(gather_rows, micro_count=micro, cores=CORES)
    scatter_all_rows = functools.partial(scatter_rows, micro_count=micro, cores=CORES)

    own_input = block_input.reshape(-1, width).astype(f32)
    cot_own = cotangent.reshape(-1, width)
    first_own = (own_input * norm_scale(own_input) * gain_first).astype(low)
    square = DOCUMENT_LIMIT * DOCUMENT_LIMIT * dim * 2 * group
    if fused:
        (
            head_full, out_full, gate_full, up_full, down_full, first_rows, second_rows, cot_rows, unit, att_pieces, unit_stat, residual
        ) = forward_call(
            micro, group, chips, heads,
            own_input, first_own, cot_own, by_head, out_t, gate_weight, up_weight, down_t,
            gain_second.reshape(1, -1), cosine, sine, code_column, last_code, first_code,
        )
    else:
        first_rows = gather_head_rows(first_own)
        projected = mm(head_full, first_rows, ((0,), (1,))).reshape(heads, unit_rows, -1)
        turned = projected[:, : (group + 1) * dim].reshape(heads, group + 1, 2, dim // 2, -1)
        front, back = turned[:, :, 0], turned[:, :, 1]
        turned = jnp.stack([front * cosine - back * sine, back * cosine + front * sine], axis=2)
        projected = jnp.concatenate(
            [turned.reshape(heads, (group + 1) * dim, -1).astype(low), projected[:, (group + 1) * dim :].astype(low)], axis=1
        )
        unit = exchange(to_units(projected.reshape(heads * unit_rows, -1)))
        unit_out, unit_stat = vmem_call(
            functools.partial(attend_kernel, group),
            (
                jax.ShapeDtypeStruct((pieces, group * dim, toks), low),
                jax.ShapeDtypeStruct((group, DOCUMENT_LIMIT), f32),
            ),
            [pltpu.VMEM((unit_rows, DOCUMENT_LIMIT), low)],
            2 * square,
            unit,
            code_column,
            last_code,
            first_code,
        )
        attended = from_units(exchange(unit_out))
        residual = own_input + scatter_head_rows(mm(attended, out_full, ((0,), (1,))).astype(low))

        second_rows = gather_all_rows((residual * norm_scale(residual) * gain_second).astype(low))
        cot_rows = gather_all_rows(cot_own)
    gate_value = mm(second_rows, gate_full, ((1,), (0,)))
    upward = mm(second_rows, up_full, ((1,), (0,)))
    sigma = jax.nn.sigmoid(gate_value)
    active = gate_value * sigma
    hidden = (active * upward).astype(low)
    grad_hidden = mm(cot_rows, down_full, ((1,), (0,)))
    gate_back = (grad_hidden * upward * (sigma * (1.0 + gate_value * (1.0 - sigma)))).astype(low)
    up_back = (grad_hidden * active).astype(low)
    second_parts = (mm(gate_back, gate_full, ((1,), (1,))) + mm(up_back, up_full, ((1,), (1,)))).astype(low)
    output_parts = mm(hidden, down_full, ((1,), (1,))).astype(low)
    down_terms = mm(cot_rows, hidden, ((0,), (0,))).astype(low)
    gate_terms = mm(second_rows, gate_back, ((0,), (0,))).astype(low)
    up_terms = mm(second_rows, up_back, ((0,), (0,))).astype(low)
    if fused:
        output_rows, input_grad, head_grad, out_grad, gate_grad, up_grad, down_grad, gain_sums = backward_call(
            micro, group, chips, heads,
            own_input, residual, cot_own, gain_first.reshape(1, -1), gain_second.reshape(1, -1),
            second_parts, output_parts, down_terms, gate_terms, up_terms,
            head_full, out_full, first_rows.T, att_pieces, unit, code_column, last_code, first_code, unit_stat, unit_cosine, unit_sine,
        )
    else:
        grad_second_rows = scatter_all_rows(second_parts)
        down_grad = jnp.concatenate(core_merge(ring_scatter(down_terms)), axis=1)
        gate_grad = jnp.concatenate(core_merge(ring_scatter(gate_terms)), axis=1)
        up_grad = jnp.concatenate(core_merge(ring_scatter(up_terms)), axis=1)
        output_rows = residual + scatter_all_rows(output_parts)

        residual_part, gain_two = norm_back(residual, gain_second, grad_second_rows)
        grad_residual = cot_own.astype(f32) + residual_part
        grad_rows = gather_head_rows(grad_residual.astype(low))
        grad_attended = mm(out_full, grad_rows, ((0,), (1,))).astype(low)
        unit_grad = exchange(to_units(grad_attended))
        (unit_back,) = vmem_call(
            functools.partial(attend_back_kernel, group),
            (jax.ShapeDtypeStruct((pieces, unit_rows, toks), low),),
            [
                pltpu.VMEM((unit_rows, DOCUMENT_LIMIT), low),
                pltpu.VMEM((group * dim, DOCUMENT_LIMIT), low),
                pltpu.VMEM((dim, DOCUMENT_LIMIT), f32),
                pltpu.VMEM((dim, DOCUMENT_LIMIT), f32),
            ],
            5 * square,
            unit,
            unit_grad,
            code_column,
            last_code,
            first_code,
            unit_stat,
            unit_cosine,
            unit_sine,
        )
        back_rows = from_units(exchange(unit_back))
        grad_first_rows = scatter_head_rows(mm(back_rows, head_full, ((0,), (1,))).astype(low))
        head_grad = scatter_head_weight(mm(first_rows, back_rows, ((0,), (1,))).astype(low))
        out_grad = scatter_head_weight(mm(grad_rows, attended, ((0,), (1,))).astype(low))
        input_part, gain_one = norm_back(own_input, gain_first, grad_first_rows)
        input_grad = (grad_residual + input_part).astype(low)
        gain_sums = all_sum(jnp.stack([gain_one, gain_two]))

    head_grad = head_grad.reshape(-1, value_heads, unit_rows)
    columns = query_weight.shape[0]
    return (
        output_rows.astype(low).reshape(block_input.shape),
        input_grad.reshape(block_input.shape),
        head_grad[:, :, : group * dim].reshape(columns, -1),
        head_grad[:, :, group * dim : (group + 1) * dim].reshape(columns, -1),
        head_grad[:, :, (group + 1) * dim :].reshape(columns, -1),
        out_grad.T,
        gate_grad,
        up_grad,
        down_grad.T,
        gain_sums[0],
        gain_sums[1],
    )


def solution(mesh):
    cp_count, tp_count = mesh.shape["cp"], mesh.shape["tp"]
    fine = Mesh(mesh.devices.reshape(cp_count // CORES, CORES, tp_count), ("chip", "core", "tp"))
    cp = ("chip", "core")
    rows = P(None, cp + ("tp",), None)
    wide, tall = P(cp, "tp"), P("tp", cp)
    return jax.shard_map(
        on_device,
        mesh=fine,
        in_specs=(rows, P(), P(), wide, wide, wide, tall, wide, wide, tall, P(), P(), rows),
        out_specs=(rows, rows, wide, wide, wide, tall, wide, wide, tall, P(), P()),
        check_vma=False,
    )
```

```python
import functools
import math

import jax
import jax.numpy as jnp
from jax import lax
from jax.experimental import pallas as pl
from jax.experimental.pallas import tpu as pltpu
from jax.sharding import Mesh
from jax.sharding import PartitionSpec as P

HEAD_SIZE = 96
DOCUMENT_LIMIT = 1024
CORES = 2

eps_norm = 1e-05
rope_base = 100000.0
masked_score = -1e30


f32 = jnp.float32
low = jnp.bfloat16


def mm(left, right, dims):
    return lax.dot_general(left, right, (dims, ((), ())), preferred_element_type=f32)


def pair_swap(values, axis):
    return lax.ppermute(values, axis, [(0, 1), (1, 0)])


def both(values, axis):
    other = pair_swap(values, axis)
    first = lax.axis_index(axis) == 0
    return jnp.stack([jnp.where(first, values, other), jnp.where(first, other, values)])


def split_pair(low_part, high_part, axis):
    first = lax.axis_index(axis) == 0
    return jnp.where(first, low_part, high_part), jnp.where(first, high_part, low_part)


def ring_of(count):
    order = list(range(0, count, 2)) + list(range(count - 1, 0, -2))
    place = [order.index(chip) for chip in range(count)]
    ahead = [(order[i], order[(i + 1) % count]) for i in range(count)]
    back = [(order[i], order[(i - 1) % count]) for i in range(count)]
    return order, place, ahead, back


def ring_gather(block):
    count = lax.axis_size("chip")
    order, place, ahead, back = ring_of(count)
    spot = jnp.array(place)[lax.axis_index("chip")]
    half_way, half_rows = count // 2, block.shape[0] // 2

    def put(whole, piece, step):
        owner = jnp.array(order)[(spot + step) % count]
        return lax.dynamic_update_index_in_dim(whole, piece, owner, 0)

    whole = put(jnp.zeros((count,) + block.shape, block.dtype), block, 0)
    up = down = block
    for step in range(1, half_way):
        up, down = lax.ppermute(up, "chip", ahead), lax.ppermute(down, "chip", back)
        whole = put(put(whole, up, count - step), down, step)
    up = lax.ppermute(up[:half_rows], "chip", ahead)
    down = lax.ppermute(down[half_rows:], "chip", back)
    whole = put(whole, jnp.concatenate([up, down], axis=0), half_way)
    return whole.reshape((count * block.shape[0],) + block.shape[1:])


def ring_scatter(terms):
    count = lax.axis_size("chip")
    order, place, ahead, back = ring_of(count)
    spot = jnp.array(place)[lax.axis_index("chip")]
    rows = terms.shape[0] // count
    half_way, half_rows = count // 2, rows // 2
    terms = terms.reshape((count, rows) + terms.shape[1:])

    def own(step):
        owner = jnp.array(order)[(spot + step) % count]
        return lax.dynamic_index_in_dim(terms, owner, 0, keepdims=False).astype(f32)

    far = own(half_way).astype(low)
    up = lax.ppermute(far[:half_rows], "chip", ahead)
    down = lax.ppermute(far[half_rows:], "chip", back)
    for step in range(half_way - 1, 0, -1):
        own_up, own_down = own(step), own(count - step)
        if step == half_way - 1:
            up = jnp.concatenate([own_up[:half_rows] + up.astype(f32), own_up[half_rows:]], axis=0)
            down = jnp.concatenate([own_down[:half_rows], own_down[half_rows:] + down.astype(f32)], axis=0)
        else:
            up, down = own_up + up.astype(f32), own_down + down.astype(f32)
        up = lax.ppermute(up.astype(low), "chip", ahead)
        down = lax.ppermute(down.astype(low), "chip", back)
    return own(0) + up.astype(f32) + down.astype(f32)


def core_split(low_part, high_part):
    kept, sent = split_pair(low_part, high_part, "core")
    other = pair_swap(sent, "core")
    first = lax.axis_index("core") == 0
    return jnp.concatenate([jnp.where(first, kept, other), jnp.where(first, other, kept)], axis=0)


def core_merge(rows):
    half = rows.shape[0] // 2
    kept, sent = split_pair(rows[:half], rows[half:], "core")
    other = pair_swap(sent.astype(low), "core").astype(f32)
    first = lax.axis_index("core") == 0
    return jnp.where(first, kept, other), jnp.where(first, other, kept)


def all_sum(values):
    for axis in ("tp", "core", "chip"):
        step = 1
        while step < lax.axis_size(axis):
            pairs = [(i, i ^ step) for i in range(lax.axis_size(axis))]
            values = values + lax.ppermute(values, axis, pairs)
            step *= 2
    return values


def gather_rows(rows, micro_count, cores):
    width = rows.shape[-1]
    tp_count = lax.axis_size("tp")
    joined = both(rows, "tp") if tp_count == 2 else lax.all_gather(rows, "tp", axis=0)
    joined = both(joined, "core") if cores == 2 else joined
    joined = joined.reshape((cores, 2, tp_count // 2, micro_count, -1, width))
    return joined.transpose((3, 1, 0, 2, 4, 5)).reshape((-1, width))


def scatter_rows(parts, micro_count, cores):
    width = parts.shape[-1]
    tp_count = lax.axis_size("tp")
    parts = parts.reshape((micro_count, 2, cores, tp_count // 2, -1, width)).transpose((2, 1, 3, 0, 4, 5))
    parts = parts.reshape((cores, tp_count, -1, width))
    if cores == 2:
        kept, sent = split_pair(parts[0], parts[1], "core")
        parts = (kept.astype(f32) + pair_swap(sent, "core").astype(f32)).astype(low)
    else:
        parts = parts[0]
    if tp_count == 2:
        kept, sent = split_pair(parts[0], parts[1], "tp")
        return kept.astype(f32) + pair_swap(sent, "tp").astype(f32)
    return lax.psum_scatter(parts, "tp", scatter_dimension=0, tiled=False).astype(f32)


def norm_scale(values):
    return lax.rsqrt(jnp.mean(values * values, axis=-1, keepdims=True) + eps_norm)


def norm_back(values, gain, grads):
    rho = norm_scale(values)
    scaled = grads * gain
    inner = jnp.mean(scaled * values, axis=-1, keepdims=True)
    return rho * scaled - values * (rho * rho * rho * inner), jnp.sum(grads * values * rho, axis=0)


def frequencies():
    return jnp.exp(jnp.arange(HEAD_SIZE // 2, dtype=f32) * (-2.0 * math.log(rope_base) / HEAD_SIZE))


def angles_of(spots):
    angles = frequencies()[:, None] * spots.astype(f32)[None, :]
    return jnp.cos(angles), jnp.sin(angles)


def unit_chunks(tokens):
    width = min(256, tokens)
    return [slice(start, start + width) for start in range(0, tokens, width)]


def lay_out(pieces_ref, flat):
    count, _, width = pieces_ref.shape
    for piece in range(count):
        flat[:, piece * width : (piece + 1) * width] = pieces_ref[piece]


def allowed_keys(code_column, last_row, first_row):
    return (code_column <= last_row) & (code_column >= first_row)


def attend_kernel(group, pieces_ref, code_ref, last_ref, first_ref, out_ref, stat_ref, flat):
    dim = HEAD_SIZE
    count, _, width = pieces_ref.shape
    tokens = count * width
    score_scale = dim ** (-0.5)
    lay_out(pieces_ref, flat)
    key_rows = flat[group * dim : (group + 1) * dim, :].astype(f32).T.astype(low)
    value_t = flat[(group + 1) * dim :, :]
    for cols in unit_chunks(tokens):
        keep = allowed_keys(code_ref[...], last_ref[:, cols], first_ref[:, cols])
        for head in range(group):
            query_t = flat[head * dim : (head + 1) * dim, cols]
            scores = mm(key_rows, query_t, ((1,), (0,))) * score_scale
            scores = jnp.where(keep, scores, masked_score)
            maximum = jnp.max(scores, axis=0, keepdims=True)
            weights = jnp.exp(scores - maximum)
            totals = jnp.sum(weights, axis=0, keepdims=True)
            probs = (weights * (1.0 / totals)).astype(low)
            stat_ref[head : head + 1, cols] = maximum + jnp.log(totals)
            result = mm(value_t, probs, ((1,), (0,))).astype(low)
            for piece in range(cols.start // width, cols.stop // width):
                start = piece * width - cols.start
                out_ref[piece, head * dim : (head + 1) * dim, :] = result[:, start : start + width]


def attend_back_kernel(
    group, pieces_ref, grads_ref, code_ref, last_ref, first_ref, stat_ref, cos_ref, sin_ref, out_ref, flat, grad_flat, key_sum, value_sum
):
    dim = HEAD_SIZE
    half = dim // 2
    count, _, width = pieces_ref.shape
    tokens = count * width
    score_scale = dim ** (-0.5)
    lay_out(pieces_ref, flat)
    lay_out(grads_ref, grad_flat)
    key_t = flat[group * dim : (group + 1) * dim, :]
    key_rows = key_t.astype(f32).T.astype(low)
    value_rows = flat[(group + 1) * dim :, :].astype(f32).T.astype(low)

    def store(values, base, cols):
        for piece in range(cols.start // width, cols.stop // width):
            start = piece * width - cols.start
            out_ref[piece, base : base + values.shape[0], :] = values[:, start : start + width]

    def unturn(values, base, cols):
        front, back = values[:half] * score_scale, values[half:] * score_scale
        cosine, sine = cos_ref[:, cols], sin_ref[:, cols]
        store((front * cosine + back * sine).astype(low), base, cols)
        store((back * cosine - front * sine).astype(low), base + half, cols)

    for index, cols in enumerate(unit_chunks(tokens)):
        keep = allowed_keys(code_ref[...], last_ref[:, cols], first_ref[:, cols])
        for head in range(group):
            rows = slice(head * dim, (head + 1) * dim)
            query_t, grad_t = flat[rows, cols], grad_flat[rows, cols]
            scores = mm(key_rows, query_t, ((1,), (0,))) * score_scale
            probs = jnp.where(keep, jnp.exp(scores - stat_ref[head : head + 1, cols]), 0.0)
            grad_probs = mm(value_rows, grad_t, ((1,), (0,)))
            delta = jnp.sum(probs * grad_probs, axis=0, keepdims=True)
            grad_scores = (probs * (grad_probs - delta)).astype(low)
            unturn(mm(key_t, grad_scores, ((1,), (0,))), head * dim, cols)
            key_part = mm(query_t, grad_scores, ((1,), (1,)))
            value_part = mm(grad_t, probs.astype(low), ((1,), (1,)))
            if index == 0 and head == 0:
                key_sum[...] = key_part
                value_sum[...] = value_part
            else:
                key_sum[...] += key_part
                value_sum[...] += value_part
    everything = slice(0, tokens)
    unturn(key_sum[...], group * dim, everything)
    store(value_sum[...].astype(low), (group + 1) * dim, everything)


MESH_ID = pl.DeviceIdType.MESH


class Sems:
    def __init__(self, send, recv):
        self.send, self.recv, self.used = send, recv, 0

    def take(self, count=1):
        base = self.used
        self.used += count
        return base


def remote(sems, index, source, target, there, arrive=None):
    return pltpu.make_async_remote_copy(
        src_ref=source,
        dst_ref=target,
        send_sem=sems.send.at[index],
        recv_sem=sems.recv.at[index if arrive is None else arrive],
        device_id=there,
        device_id_type=MESH_ID,
    )


def greet(chips, chip, core, tp):
    barrier = pltpu.get_barrier_semaphore()

    @pl.loop(1, chips)
    def _(step):
        pl.semaphore_signal(barrier, inc=1, device_id={"chip": (chip + step) % chips}, device_id_type=MESH_ID)

    pl.semaphore_signal(barrier, inc=1, device_id={"core": 1 - core}, device_id_type=MESH_ID)
    pl.semaphore_signal(barrier, inc=1, device_id={"tp": 1 - tp}, device_id_type=MESH_ID)
    pl.semaphore_wait(barrier, chips + 1)


def spot_of(chip, count):
    odd = chip % 2
    return (1 - odd) * (chip // 2) + odd * (count - 1 - chip // 2)


def chip_at(spot, count):
    spot = (spot + count) % count
    far = spot // (count // 2)
    return (1 - far) * 2 * spot + far * (2 * (count - 1 - spot) + 1)


class Ring:
    def __init__(self, sems, whole, rows, count, chip, saved, save_sem):
        self.sems, self.whole, self.rows, self.count = sems, whole, rows, count
        self.saved, self.save_sem = saved, save_sem
        self.spot = spot_of(chip, count)
        self.half = count // 2
        self.base = sems.take(2 * self.half)
        self.ways = (1, -1)

    def copy(self, side, hop, behind):
        way = self.ways[side]
        start = chip_at(self.spot - way * behind, self.count) * self.rows
        size = self.rows
        if hop == self.half:
            size = self.rows // 2
            start = start + side * size
        piece = self.whole.at[pl.ds(pl.multiple_of(start, 16), size), :]
        there = {"chip": chip_at(self.spot + way, self.count)}
        return remote(self.sems, self.base + side * self.half + hop - 1, piece, piece, there)

    def save(self, side, hop, behind):
        way = self.ways[side]
        start = chip_at(self.spot - way * behind, self.count) * self.rows
        size = self.rows
        if hop == self.half:
            size = self.rows // 2
            start = start + side * size
        piece = pl.ds(pl.multiple_of(start, 16), size)
        pltpu.make_async_copy(self.whole.at[piece, :], self.saved.at[piece, :], self.save_sem).start()

    def start(self):
        for side in (0, 1):
            self.copy(side, 1, 0).start()
        self.save(0, 1, 0)

    def arrive(self):
        for side in (0, 1):
            self.copy(side, self.half, self.half).wait_recv()
            self.save(side, self.half, self.half)

    def relay(self, hop):
        for side in (0, 1):
            self.copy(side, hop - 1, hop - 1).wait_recv()
            self.copy(side, hop, hop - 1).start()
        for side in (0, 1):
            self.save(side, hop - 1, hop - 1)

    def saves_done(self):
        pltpu.make_async_copy(self.whole, self.saved, self.save_sem).wait()

    def drain(self):
        for side in (0, 1):
            for hop in range(1, self.half + 1):
                self.copy(side, hop, hop - 1).wait_send()


class Spread:
    def __init__(self, sems, whole, micro, where):
        self.sems, self.whole, self.micro = sems, whole, micro
        _, self.core, self.tp = where
        self.rows = whole.shape[0] // (4 * micro)
        self.base = sems.take(3 * micro)

    def rows_of(self, m, half, core):
        return pl.ds(pl.multiple_of(((m * 2 + half) * 2 + core) * self.rows, 16), self.rows)

    def place(self, m, half, core):
        return self.whole.at[self.rows_of(m, half, core), :]

    def put(self, m, values):
        self.whole[self.rows_of(m, self.tp, self.core), :] = values

    def over_tp(self, m, half):
        piece = self.place(m, half, self.core)
        return remote(self.sems, self.base + m, piece, piece, {"tp": 1 - self.tp})

    def over_core(self, m, core):
        piece = self.place(m, self.tp, core)
        return remote(self.sems, self.base + self.micro + m, piece, piece, {"core": 1 - self.core})

    def passed_on(self, m, core):
        piece = self.place(m, 1 - self.tp, core)
        return remote(self.sems, self.base + 2 * self.micro + m, piece, piece, {"core": 1 - self.core})

    def start(self, m):
        self.over_tp(m, self.tp).start()
        self.over_core(m, self.core).start()

    def pass_on(self):
        for m in range(self.micro):
            self.over_tp(m, 1 - self.tp).wait_recv()
            self.passed_on(m, self.core).start()

    def finish(self):
        for m in range(self.micro):
            self.over_core(m, 1 - self.core).wait_recv()
            self.passed_on(m, 1 - self.core).wait_recv()

    def drain(self):
        for m in range(self.micro):
            self.over_tp(m, self.tp).wait_send()
            self.over_core(m, self.core).wait_send()
            self.passed_on(m, self.core).wait_send()


def turn_over(whole, turned):
    lanes = 256

    @pl.loop(0, whole.shape[1] // lanes)
    def _(part):
        columns = pl.ds(pl.multiple_of(part * lanes, 128), lanes)
        turned[columns, :] = whole[:, columns].astype(f32).T.astype(low)


def angle_tables(spots_ref, frequency_ref, cos_ref, sin_ref):
    angles = frequency_ref[...] * spots_ref[...].astype(f32)
    cos_ref[...] = jnp.cos(angles)
    sin_ref[...] = jnp.sin(angles)


def unit_codes(seg_ref, spots_ref, code_ref, last_ref, start_ref):
    first = (seg_ref[...] * DOCUMENT_LIMIT).astype(f32)
    last = first + spots_ref[...].astype(f32)
    last_ref[...] = last
    start_ref[...] = first
    code_ref[...] = jnp.broadcast_to(last, (8, last.shape[1])).T[:, :1]


class Fold:
    def __init__(self, sems, parts, from_core, to_tp, from_tp, micro, chip_core_tp):
        self.sems, self.parts, self.from_core, self.to_tp, self.from_tp = sems, parts, from_core, to_tp, from_tp
        self.micro = micro
        _, self.core, self.tp = chip_core_tp
        self.rows = from_tp.shape[0] // micro
        self.base = sems.take(3 * micro)

    def piece(self, m, half, core):
        start = ((m * 2 + half) * 2 + core) * self.rows
        return pl.ds(pl.multiple_of(start, 16), self.rows)

    def landing(self, m, half):
        return pl.ds(pl.multiple_of((m * 2 + half) * self.rows, 16), self.rows)

    def over_core(self, m, half):
        source = self.parts.at[self.piece(m, half, 1 - self.core), :]
        index = self.base + m * 2 + half
        return remote(self.sems, index, source, self.from_core.at[self.landing(m, half), :], {"core": 1 - self.core})

    def over_tp(self, m):
        rows = pl.ds(m * self.rows, self.rows)
        index = self.base + 2 * self.micro + m
        return remote(self.sems, index, self.to_tp.at[rows, :], self.from_tp.at[rows, :], {"tp": 1 - self.tp})

    def start(self, m, half):
        self.over_core(m, half).start()

    def summed(self, m, half):
        mine = self.parts[self.piece(m, half, self.core), :].astype(f32)
        return mine + self.from_core[self.landing(m, half), :].astype(f32)

    def send(self, m):
        for half in (0, 1):
            self.over_core(m, half).wait_recv()
        self.to_tp[m * self.rows : (m + 1) * self.rows, :] = self.summed(m, 1 - self.tp).astype(low)
        self.over_tp(m).start()

    def result(self, m):
        kept = self.summed(m, self.tp)
        self.over_tp(m).wait_recv()
        return kept + self.from_tp[m * self.rows : (m + 1) * self.rows, :].astype(f32)

    def drain(self):
        for m in range(self.micro):
            for half in (0, 1):
                self.over_core(m, half).wait_send()
            self.over_tp(m).wait_send()


class Exchange:
    def __init__(self, sems, outgoing, incoming, chips, chip):
        self.sems, self.outgoing, self.incoming, self.chips, self.chip = sems, outgoing, incoming, chips, chip
        self.base = sems.take(chips)

    def copy(self, to):
        return remote(
            self.sems, self.base + to, self.outgoing.at[to], self.incoming.at[self.chip], {"chip": to}, self.base + self.chip
        )

    def send(self, to):
        @pl.when(to != self.chip)
        def _():
            self.copy(to).start()

        @pl.when(to == self.chip)
        def _():
            self.incoming[to] = self.outgoing[to]

    def finish(self):
        @pl.loop(1, self.chips)
        def _(step):
            source = (self.chip + step) % self.chips
            remote(
                self.sems, self.base + source, self.outgoing.at[source], self.incoming.at[source], {"chip": source}
            ).wait_recv()

    def drain(self):
        @pl.loop(1, self.chips)
        def _(step):
            self.copy((self.chip + step) % self.chips).wait_send()


class Actions:
    def __init__(self, steps):
        self.steps = list(steps)

    def run(self, count=None):
        count = len(self.steps) if count is None else count
        for step in self.steps[:count]:
            step()
        self.steps = self.steps[count:]


def forward_kernel(
    micro, group, chips,
    x_ref, cot_ref, head_ref, out_ref, gate_ref, up_ref, down_ref, gain_one_ref, gain_two_ref, frequency_ref, row_pos_ref, unit_pos_ref, unit_seg_ref,
    head_o, out_o, gate_o, up_o, down_o, first_o, second_o, cot_o, second_t_o, cot_t_o, unit_o, att_o, stat_ref, residual_ref,
    head_w, out_w, gate_w, up_w, down_w, first_all, second_all, cot_all, first_t, second_t, cot_t, unit_send, unit_in, flat, att_send, att_in,
    parts, from_core, to_tp, from_tp, cos_ref, sin_ref, code_ref, last_ref, start_ref, send_sem, recv_sem, local_sem, save_sem,
):
    dim = HEAD_SIZE
    half = dim // 2
    chip, core, tp = lax.axis_index("chip"), lax.axis_index("core"), lax.axis_index("tp")
    where = (chip, core, tp)
    sems = Sems(send_sem, recv_sem)
    rows = x_ref.shape[0] // micro
    toks = 2 * rows
    unit_rows = (group + 2) * dim
    heads = head_w.shape[1] // unit_rows
    hops = chips // 2
    depth = head_ref.shape[0]
    greet(chips, chip, core, tp)

    weights = ((head_ref, head_w, head_o), (out_ref, out_w, out_o), (down_ref, down_w, down_o), (gate_ref, gate_w, gate_o), (up_ref, up_w, up_o))
    rings, swaps, keeps = [], [], []
    for index, (shard, whole, saved) in enumerate(weights):
        columns = whole.shape[1]
        mine = whole.at[pl.ds(pl.multiple_of((chip * 2 + core) * depth, 16), depth), :]
        theirs = whole.at[pl.ds(pl.multiple_of((chip * 2 + 1 - core) * depth, 16), depth), :]
        at = sems.take()
        give = shard.at[:, pl.ds(pl.multiple_of((1 - core) * columns, 128), columns)]
        hold = shard.at[:, pl.ds(pl.multiple_of(core * columns, 128), columns)]
        swaps.append((remote(sems, at, give, mine, {"core": 1 - core}), remote(sems, at, give, theirs, {"core": 1 - core})))
        keeps.append(pltpu.make_async_copy(hold, mine, local_sem.at[index]))
        rings.append(Ring(sems, whole, 2 * depth, chips, chip, saved, save_sem.at[index]))
    first, second, cot = (Spread(sems, whole, micro, where) for whole in (first_all, second_all, cot_all))
    to_unit = Exchange(sems, unit_send, unit_in, chips, chip)
    from_unit = Exchange(sems, att_send, att_in, chips, chip)
    fold = Fold(sems, parts, from_core, to_tp, from_tp, micro, where)
    saves = []

    def save(source, target):
        saves.append(pltpu.make_async_copy(source, target, save_sem.at[5 + len(saves)]))
        saves[-1].start()

    for index in (0, 1):
        swaps[index][0].start()
        keeps[index].start()
    for m in range(micro):
        values = x_ref[m * rows : (m + 1) * rows, :].astype(f32)
        first.put(m, (values * norm_scale(values) * gain_one_ref[...]).astype(low))
    for index in (2, 3, 4):
        swaps[index][0].start()
        keeps[index].start()
    for m in range(micro):
        cot.put(m, cot_ref[m * rows : (m + 1) * rows, :])
        first.start(m)
    head_ring, out_ring, down_ring, gate_ring, up_ring = rings
    for index in (0, 1):
        keeps[index].wait()
        swaps[index][1].wait_recv()
        rings[index].start()
    angle_tables(row_pos_ref, frequency_ref, cos_ref, sin_ref)
    first.pass_on()
    for hop in range(2, hops + 1):
        head_ring.relay(hop)
        out_ring.relay(hop)
    for index in (2, 3, 4):
        keeps[index].wait()
        swaps[index][1].wait_recv()
    down_ring.start()
    first.finish()
    head_ring.arrive()
    later = Actions(
        [ring.start for ring in (gate_ring, up_ring)]
        + [functools.partial(ring.relay, hop) for hop in range(2, hops + 1) for ring in (down_ring, gate_ring, up_ring)]
    )

    @pl.loop(0, micro * 2 * heads)
    def _(u):
        block, head = u // heads, u % heads
        tokens = pl.ds(pl.multiple_of(block * toks, 128), toks)
        columns = pl.ds(pl.multiple_of(head * unit_rows, 128), unit_rows)
        lines = mm(first_all[tokens, :], head_w[:, columns], ((1,), (0,))).T
        cosine, sine = cos_ref[:, tokens], sin_ref[:, tokens]
        for turn in range(group + 1):
            front = lines[turn * dim : turn * dim + half]
            back = lines[turn * dim + half : (turn + 1) * dim]
            unit_send[u, turn * dim : turn * dim + half, :] = (front * cosine - back * sine).astype(low)
            unit_send[u, turn * dim + half : (turn + 1) * dim, :] = (back * cosine + front * sine).astype(low)
        unit_send[u, (group + 1) * dim :, :] = lines[(group + 1) * dim :].astype(low)
        to_unit.send(u)

    later.run(1)
    for m in range(micro):
        cot.start(m)
    out_ring.arrive()
    unit_codes(unit_seg_ref, unit_pos_ref, code_ref, last_ref, start_ref)
    later.run(2)
    cot.pass_on()
    to_unit.finish()

    score_scale = dim ** (-0.5)
    lay_out(unit_in, flat)
    save(unit_in, unit_o)
    key_rows = flat[group * dim : (group + 1) * dim, :].astype(f32).T.astype(low)
    lanes = 256

    @pl.loop(0, chips * toks // lanes)
    def _(number):
        cols = pl.ds(pl.multiple_of(number * lanes, 128), lanes)
        keep = allowed_keys(code_ref[...], last_ref[:, cols], start_ref[:, cols])
        for head in range(group):
            query_t = flat[head * dim : (head + 1) * dim, cols]
            scores = mm(key_rows, query_t, ((1,), (0,))) * score_scale
            scores = jnp.where(keep, scores, masked_score)
            maximum = jnp.max(scores, axis=0, keepdims=True)
            exponents = jnp.exp(scores - maximum)
            totals = jnp.sum(exponents, axis=0, keepdims=True)
            probs = (exponents * (1.0 / totals)).astype(low)
            stat_ref[head : head + 1, cols] = maximum + jnp.log(totals)
            result = mm(flat[(group + 1) * dim :, :], probs, ((1,), (0,))).astype(low)
            for piece in range(lanes // toks):
                here = result[:, piece * toks : (piece + 1) * toks]
                att_send[number * (lanes // toks) + piece, head * dim : (head + 1) * dim, :] = here
        for piece in range(lanes // toks):
            from_unit.send(number * (lanes // toks) + piece)

        @pl.when(number == 1)
        def _():
            later.run(1)

    later.run(1)
    cot.finish()
    save(cot_all, cot_o)
    turn_over(cot_all, cot_t)
    save(cot_t, cot_t_o)
    turn_over(first_all, first_t)
    save(first_t, first_o)
    from_unit.finish()
    save(att_in, att_o)

    @pl.loop(0, micro * 2)
    def _(block):
        lines = jnp.concatenate([att_in[block * heads + head] for head in range(heads)], axis=0)
        lines = lines.astype(f32).T.astype(low)
        sums = mm(lines, out_w[...], ((1,), (1,)))
        parts[pl.ds(pl.multiple_of(block * toks, 128), toks), :] = sums.astype(low)
        fold.start(block // 2, block % 2)

    for m in range(micro):
        fold.send(m)
    later.run(1)
    for m in range(micro):
        own = slice(m * rows, (m + 1) * rows)
        residual = x_ref[own, :].astype(f32) + fold.result(m)
        residual_ref[own, :] = residual
        second.put(m, (residual * norm_scale(residual) * gain_two_ref[...]).astype(low))
        second.start(m)
    later.run(2)
    second.pass_on()
    second.finish()
    save(second_all, second_o)
    turn_over(second_all, second_t)
    save(second_t, second_t_o)
    later.run()
    for ring in (down_ring, gate_ring, up_ring):
        ring.arrive()
    for part in saves:
        part.wait()
    for ring in rings:
        ring.saves_done()
    for swap, _ in swaps:
        swap.wait_send()
    for part in rings + [first, second, cot, to_unit, from_unit, fold]:
        part.drain()


def forward_call(micro, group, chips, heads, *operands):
    x, _, head_s, out_s, gate_s, up_s, down_s = operands[:7]
    own_rows, width = x.shape
    toks = own_rows // micro * 2
    all_rows = own_rows * 4
    pieces = micro * 2 * heads
    unit_rows, att_rows = (group + 2) * HEAD_SIZE, group * HEAD_SIZE
    shape = jax.ShapeDtypeStruct
    columns = [s.shape[1] // CORES for s in (head_s, out_s, gate_s, up_s, down_s)]
    any_spec, vmem_spec = pl.BlockSpec(memory_space=pl.ANY), pl.BlockSpec(memory_space=pltpu.VMEM)
    any_outs = [shape((width, c), low) for c in columns]
    any_outs += [shape((width, all_rows), low)] + [shape((all_rows, width), low)] * 2 + [shape((width, all_rows), low)] * 2
    any_outs += [shape((pieces, unit_rows, toks), low), shape((pieces, att_rows, toks), low)]
    vmem_outs = [shape((group, DOCUMENT_LIMIT), f32), shape((own_rows, width), f32)]
    scratch = [pltpu.VMEM((width, c), low) for c in columns]
    scratch += [pltpu.VMEM((all_rows, width), low)] * 3 + [pltpu.VMEM((width, all_rows), low)] * 3
    scratch += [
        pltpu.VMEM((pieces, unit_rows, toks), low),
        pltpu.VMEM((pieces, unit_rows, toks), low),
        pltpu.VMEM((unit_rows, DOCUMENT_LIMIT), low),
        pltpu.VMEM((pieces, att_rows, toks), low),
        pltpu.VMEM((pieces, att_rows, toks), low),
        pltpu.VMEM((all_rows, width), low),
        pltpu.VMEM((all_rows // 2, width), low),
        pltpu.VMEM((own_rows, width), low),
        pltpu.VMEM((own_rows, width), low),
        pltpu.VMEM((HEAD_SIZE // 2, all_rows), f32),
        pltpu.VMEM((HEAD_SIZE // 2, all_rows), f32),
        pltpu.VMEM((DOCUMENT_LIMIT, 1), f32),
        pltpu.VMEM((1, DOCUMENT_LIMIT), f32),
        pltpu.VMEM((1, DOCUMENT_LIMIT), f32),
        pltpu.SemaphoreType.DMA((96,)),
        pltpu.SemaphoreType.DMA((96,)),
        pltpu.SemaphoreType.DMA((5,)),
        pltpu.SemaphoreType.DMA((16,)),
    ]
    return pl.pallas_call(
        functools.partial(forward_kernel, micro, group, chips),
        out_shape=tuple(any_outs + vmem_outs),
        in_specs=[vmem_spec] * 2 + [any_spec] * 5 + [vmem_spec] * (len(operands) - 7),
        out_specs=tuple([any_spec] * len(any_outs) + [vmem_spec] * len(vmem_outs)),
        scratch_shapes=scratch,
        compiler_params=pltpu.CompilerParams(collective_id=0, has_side_effects=True, vmem_limit_bytes=60 << 20),
    )(*operands)


class RingSum:
    def __init__(self, sems, make, far, slots, count, chip, core):
        self.sems, self.make, self.far, self.slots, self.count, self.chip, self.core = sems, make, far, slots, count, chip, core
        self.rows = far.shape[0]
        self.spot = spot_of(chip, count)
        self.half = count // 2
        self.base = sems.take(2 * self.half)
        self.ways = (1, -1)

    def slot(self, side, hop):
        return (side * self.half + hop - 1) * self.rows

    def term(self, side, distance):
        return chip_at(self.spot + self.ways[side] * distance, self.count) * self.rows

    def copy(self, side, hop):
        there = {"chip": chip_at(self.spot + self.ways[side], self.count)}
        index = self.base + side * self.half + hop - 1
        if hop == 1:
            size = self.rows // 2
            source = self.far.at[side * size : (side + 1) * size, :]
            target = self.slots.at[pl.ds(self.slot(side, 1) + side * size, size), :]
        else:
            source = self.slots.at[pl.ds(self.slot(side, hop - 1), self.rows), :]
            target = self.slots.at[pl.ds(self.slot(side, hop), self.rows), :]
        return remote(self.sems, index, source, target, there)

    def start(self):
        self.far[...] = self.make((self.term(0, self.half),), self.rows).astype(low)
        for side in (0, 1):
            self.copy(side, 1).start()

    def relay(self, hop):
        size = self.rows // 2
        own = self.make([self.term(side, self.half - hop + 1) for side in (0, 1)], self.rows)
        for side in (0, 1):
            self.copy(side, hop - 1).wait_recv()
            at = self.slot(side, hop - 1)
            for part in (0, 1):
                here = pl.ds(at + part * size, size)
                mine = own[side * self.rows + part * size : side * self.rows + (part + 1) * size]
                if hop == 2 and part != side:
                    self.slots[here, :] = mine.astype(low)
                else:
                    self.slots[here, :] = (mine + self.slots[here, :].astype(f32)).astype(low)
            self.copy(side, hop).start()

    def result(self):
        size = self.rows // 2
        offsets = [self.core * size, (1 - self.core) * size]
        own = self.make([self.chip * self.rows + offset for offset in offsets], size)
        for side in (0, 1):
            self.copy(side, self.half).wait_recv()
        sums = []
        for index, offset in enumerate(offsets):
            total = own[index * size : (index + 1) * size]
            for side in (0, 1):
                here = pl.ds(pl.multiple_of(self.slot(side, self.half) + offset, 16), size)
                total = total + self.slots[here, :].astype(f32)
            sums.append(total)
        return sums

    def drain(self):
        for side in (0, 1):
            for hop in range(1, self.half + 1):
                self.copy(side, hop).wait_send()


def rows_from(ref, starts, size):
    blocks = [ref[pl.ds(pl.multiple_of(start, 16), size), :] for start in starts]
    return blocks[0] if len(blocks) == 1 else jnp.concatenate(blocks, axis=0)


class Merge:
    def __init__(self, sems, ring, leaving, landing, out, core):
        self.sems, self.ring, self.leaving, self.landing, self.out, self.core = sems, ring, leaving, landing, out, core
        self.index = sems.take()

    def copy(self):
        return remote(self.sems, self.index, self.leaving, self.landing, {"core": 1 - self.core})

    def send(self):
        kept, sent = self.ring.result()
        self.leaving[...] = sent.astype(low)
        self.copy().start()
        columns = self.leaving.shape[1]
        self.out[:, pl.ds(pl.multiple_of(self.core * columns, 128), columns)] = kept

    def finish(self):
        columns = self.leaving.shape[1]
        self.copy().wait_recv()
        self.out[:, pl.ds(pl.multiple_of((1 - self.core) * columns, 128), columns)] = self.landing[...].astype(f32)

    def drain(self):
        self.copy().wait_send()


class Butterfly:
    def __init__(self, sems, leaving, landing, chips, where):
        self.sems, self.leaving, self.landing = sems, leaving, landing
        chip, core, tp = where
        self.partners = [{"tp": 1 - tp}, {"core": 1 - core}]
        step = 1
        while step < chips:
            self.partners.append({"chip": chip + step - 2 * step * (chip // step % 2)})
            step *= 2
        self.base = sems.take(len(self.partners))

    def copy(self, stage):
        return remote(self.sems, self.base + stage, self.leaving.at[stage], self.landing.at[stage], self.partners[stage])

    def start(self, values):
        self.leaving[0] = values
        self.copy(0).start()

    def step(self, stage):
        self.copy(stage).wait_recv()
        values = self.leaving[stage] + self.landing[stage]
        if stage + 1 < len(self.partners):
            self.leaving[stage + 1] = values
            self.copy(stage + 1).start()
        return values

    def drain(self):
        for stage in range(len(self.partners)):
            self.copy(stage).wait_send()


def backward_kernel(
    micro, group, chips,
    x_ref, residual_ref, cot_ref, gain_one_ref, gain_two_ref, stat_ref, frequency_ref, unit_pos_ref, unit_seg_ref,
    second_h, cot_t_h, hidden_h, second_t_h, gate_back_h, up_back_h, unit_h, att_h, down_h, out_h, first_t_h, head_h,
    output_ref, input_grad_ref, head_g, out_g, gate_g, up_g, down_g, gains_ref,
    second_parts, cot_t, hidden, second_t, gate_back, up_back, unit_ref, att_ref, down_w, out_w, first_t, head_w,
    core_a, to_tp_a, from_tp_a, core_b, to_tp_b, from_tp_b, core_c, to_tp_c, from_tp_c, grad_residual, grad_all, output_parts, first_parts,
    grad_send, grad_in, flat, grad_flat, key_sum, value_sum, back_send, back_in, att_flat, back_flat, out_terms,
    cos_ref, sin_ref, code_ref, last_ref, start_ref,
    head_far, out_far, down_far, gate_far, up_far, head_slots, out_slots, down_slots, gate_slots, up_slots,
    head_leave, out_leave, down_leave, gate_leave, up_leave, head_land, out_land, down_land, gate_land, up_land,
    gain_leave, gain_land, send_sem, recv_sem, local_sem,
):
    dim = HEAD_SIZE
    half = dim // 2
    chip, core, tp = lax.axis_index("chip"), lax.axis_index("core"), lax.axis_index("tp")
    where = (chip, core, tp)
    sems = Sems(send_sem, recv_sem)
    rows = x_ref.shape[0] // micro
    toks = 2 * rows
    unit_rows = (group + 2) * dim
    heads = head_w.shape[1] // unit_rows
    blocks = micro * 2
    hops = chips // 2
    sources = (second_h, cot_t_h, hidden_h, second_t_h, gate_back_h, up_back_h, unit_h, att_h, down_h, out_h, first_t_h, head_h)
    places = (second_parts, cot_t, hidden, second_t, gate_back, up_back, unit_ref, att_ref, down_w, out_w, first_t, head_w)
    loads = [pltpu.make_async_copy(a, b, local_sem.at[i]) for i, (a, b) in enumerate(zip(sources, places))]
    for load in loads:
        load.start()
    greet(chips, chip, core, tp)

    def ring_of_products(left, right, far, slots):
        make = lambda starts, size: mm(rows_from(left, starts, size), right[...], ((1,), (0,)))
        return RingSum(sems, make, far, slots, chips, chip, core)

    down_ring = ring_of_products(cot_t, hidden, down_far, down_slots)
    gate_ring = ring_of_products(second_t, gate_back, gate_far, gate_slots)
    up_ring = ring_of_products(second_t, up_back, up_far, up_slots)
    out_ring = RingSum(sems, lambda starts, size: rows_from(out_terms, starts, size).astype(f32), out_far, out_slots, chips, chip, core)
    head_ring = RingSum(
        sems, lambda starts, size: mm(rows_from(first_t, starts, size), back_flat[...], ((1,), (1,))), head_far, head_slots, chips, chip, core
    )
    down_merge, gate_merge, up_merge, out_merge, head_merge = (
        Merge(sems, down_ring, down_leave, down_land, down_g, core),
        Merge(sems, gate_ring, gate_leave, gate_land, gate_g, core),
        Merge(sems, up_ring, up_leave, up_land, up_g, core),
        Merge(sems, out_ring, out_leave, out_land, out_g, core),
        Merge(sems, head_ring, head_leave, head_land, head_g, core),
    )
    second_fold = Fold(sems, second_parts, core_a, to_tp_a, from_tp_a, micro, where)
    output_fold = Fold(sems, output_parts, core_b, to_tp_b, from_tp_b, micro, where)
    first_fold = Fold(sems, first_parts, core_c, to_tp_c, from_tp_c, micro, where)
    spread = Spread(sems, grad_all, micro, where)
    to_unit = Exchange(sems, grad_send, grad_in, chips, chip)
    from_unit = Exchange(sems, back_send, back_in, chips, chip)
    butterfly = Butterfly(sems, gain_leave, gain_land, chips, where)
    later = Actions([functools.partial(ring.relay, hop) for hop in range(2, hops + 1) for ring in (down_ring, gate_ring, up_ring)])

    loads[0].wait()
    for m in range(micro):
        for side in (0, 1):
            second_fold.start(m, side)
    for load in loads[1:3]:
        load.wait()
    down_ring.start()
    for m in range(micro):
        second_fold.send(m)
    for load in loads[3:6]:
        load.wait()
    gate_ring.start()
    up_ring.start()

    def norm_rows_back(values, gain, grads):
        rho = norm_scale(values)
        scaled = grads * gain
        inner = jnp.mean(scaled * values, axis=-1, keepdims=True)
        return rho * scaled - values * (rho * rho * rho * inner), jnp.sum(grads * values * rho, axis=0, keepdims=True)

    later.run(1)
    gain_two = None
    for m in range(micro):
        own = slice(m * rows, (m + 1) * rows)
        part, gain_now = norm_rows_back(residual_ref[own, :], gain_two_ref[...], second_fold.result(m))
        gain_two = gain_now if gain_two is None else gain_two + gain_now
        grads = cot_ref[own, :].astype(f32) + part
        grad_residual[own, :] = grads
        spread.put(m, grads.astype(low))
        spread.start(m)
    for load in loads[6:8]:
        load.wait()
    lay_out(unit_ref, flat)
    for piece in range(blocks * heads):
        block, head = piece // heads, piece % heads
        att_flat[head * group * dim : (head + 1) * group * dim, block * toks : (block + 1) * toks] = att_ref[piece]
    key_t = flat[group * dim : (group + 1) * dim, :]
    key_rows = key_t.astype(f32).T.astype(low)
    value_rows = flat[(group + 1) * dim :, :].astype(f32).T.astype(low)
    unit_codes(unit_seg_ref, unit_pos_ref, code_ref, last_ref, start_ref)
    later.run(1)
    spread.pass_on()
    angle_tables(unit_pos_ref, frequency_ref, cos_ref, sin_ref)
    for load in loads[8:10]:
        load.wait()
    later.run(1)
    spread.finish()

    @pl.loop(0, blocks)
    def _(block):
        tokens = pl.ds(pl.multiple_of(block * toks, 128), toks)
        lines = mm(grad_all[tokens, :], out_w[...], ((1,), (0,))).T.astype(low)
        for head in range(heads):
            piece = block * heads + head
            grad_send[piece] = lines[head * group * dim : (head + 1) * group * dim]
            to_unit.send(piece)

    later.run(1)

    @pl.loop(0, blocks)
    def _(block):
        tokens = pl.ds(pl.multiple_of(block * toks, 128), toks)
        output_parts[tokens, :] = mm(hidden[tokens, :], down_w[...], ((1,), (1,))).astype(low)
        output_fold.start(block // 2, block % 2)

    lanes = 256

    @pl.loop(0, grad_all.shape[1] // lanes)
    def _(part):
        columns = pl.ds(pl.multiple_of(part * lanes, 128), lanes)
        out_terms[columns, :] = mm(att_flat[...], grad_all[:, columns], ((1,), (0,))).T.astype(low)

    out_ring.start()
    later.run(1)
    for m in range(micro):
        output_fold.send(m)
    to_unit.finish()
    lay_out(grad_in, grad_flat)

    score_scale = dim ** (-0.5)
    tokens_all = chips * toks
    key_sum[...] = jnp.zeros_like(key_sum)
    value_sum[...] = jnp.zeros_like(value_sum)

    def store(values, base, first_piece):
        for piece in range(values.shape[1] // toks):
            back_send[first_piece + piece, base : base + values.shape[0], :] = values[:, piece * toks : (piece + 1) * toks]

    def unturn(values, base, cols, first_piece):
        front, back = values[:half] * score_scale, values[half:] * score_scale
        cosine, sine = cos_ref[:, cols], sin_ref[:, cols]
        store((front * cosine + back * sine).astype(low), base, first_piece)
        store((back * cosine - front * sine).astype(low), base + half, first_piece)

    @pl.loop(0, tokens_all // lanes)
    def _(number):
        cols = pl.ds(pl.multiple_of(number * lanes, 128), lanes)
        keep = allowed_keys(code_ref[...], last_ref[:, cols], start_ref[:, cols])
        for head in range(group):
            lines = slice(head * dim, (head + 1) * dim)
            query_t, grad_t = flat[lines, cols], grad_flat[lines, cols]
            scores = mm(key_rows, query_t, ((1,), (0,))) * score_scale
            probs = jnp.where(keep, jnp.exp(scores - stat_ref[head : head + 1, cols]), 0.0)
            grad_probs = mm(value_rows, grad_t, ((1,), (0,)))
            delta = jnp.sum(probs * grad_probs, axis=0, keepdims=True)
            grad_scores = (probs * (grad_probs - delta)).astype(low)
            unturn(mm(key_t, grad_scores, ((1,), (0,))), head * dim, cols, number * (lanes // toks))
            key_sum[...] += mm(query_t, grad_scores, ((1,), (1,)))
            value_sum[...] += mm(grad_t, probs.astype(low), ((1,), (1,)))

        @pl.when(number == 1)
        def _():
            later.run(1)

    unturn(key_sum[...], group * dim, slice(0, tokens_all), 0)
    store(value_sum[...].astype(low), (group + 1) * dim, 0)

    @pl.loop(0, chips)
    def _(piece):
        from_unit.send(piece)

    later.run(1)
    for m in range(micro):
        own = slice(m * rows, (m + 1) * rows)
        output_ref[own, :] = (residual_ref[own, :] + output_fold.result(m)).astype(low)
    later.run(1)
    for load in loads[10:]:
        load.wait()
    from_unit.finish()

    for block in range(blocks):
        for head in range(heads):
            back_flat[head * unit_rows : (head + 1) * unit_rows, block * toks : (block + 1) * toks] = back_in[block * heads + head]
    head_ring.start()

    @pl.loop(0, blocks)
    def _(block):
        tokens = pl.ds(pl.multiple_of(block * toks, 128), toks)
        lines = back_flat[:, tokens].astype(f32).T.astype(low)
        first_parts[tokens, :] = mm(lines, head_w[...], ((1,), (1,))).astype(low)
        first_fold.start(block // 2, block % 2)

    later.run(1)
    head_ring.relay(2)
    for m in range(micro):
        first_fold.send(m)
    later.run()
    for hop in range(2, hops + 1):
        if hop > 2:
            head_ring.relay(hop)
        out_ring.relay(hop)
        if hop == 2:
            down_merge.send()
    gain_one = None
    for m in range(micro):
        own = slice(m * rows, (m + 1) * rows)
        part, gain_now = norm_rows_back(x_ref[own, :].astype(f32), gain_one_ref[...], first_fold.result(m))
        gain_one = gain_now if gain_one is None else gain_one + gain_now
        input_grad_ref[own, :] = (grad_residual[own, :] + part).astype(low)
    butterfly.start(jnp.concatenate([gain_one, gain_two], axis=0))
    gate_merge.send()
    butterfly.step(0)
    up_merge.send()
    butterfly.step(1)
    down_merge.finish()
    for stage in range(2, len(butterfly.partners) - 1):
        butterfly.step(stage)
    out_merge.send()
    gate_merge.finish()
    head_merge.send()
    up_merge.finish()
    gains_ref[...] = butterfly.step(len(butterfly.partners) - 1)
    out_merge.finish()
    head_merge.finish()
    parts = [down_ring, gate_ring, up_ring, out_ring, head_ring, down_merge, gate_merge, up_merge, out_merge, head_merge]
    parts += [second_fold, output_fold, first_fold, spread, to_unit, from_unit, butterfly]
    for part in parts:
        part.drain()


def backward_call(micro, group, chips, heads, near, *far):
    own_rows, width = near[0].shape
    toks = own_rows // micro * 2
    all_rows = own_rows * 4
    pieces = micro * 2 * heads
    unit_rows, att_rows = (group + 2) * HEAD_SIZE, group * HEAD_SIZE
    shape = jax.ShapeDtypeStruct
    hidden = far[2].shape[1]
    depth = width // chips
    columns = [heads * unit_rows, heads * att_rows, hidden, hidden, hidden]
    stages = 2 + (chips - 1).bit_length()
    any_spec, vmem_spec = pl.BlockSpec(memory_space=pl.ANY), pl.BlockSpec(memory_space=pltpu.VMEM)
    outs = [shape((own_rows, width), low)] * 2 + [shape((depth // 2, 2 * c), f32) for c in columns] + [shape((2, width), f32)]
    scratch = [pltpu.VMEM(a.shape, a.dtype) for a in far]
    scratch += [pltpu.VMEM((all_rows // 2, width), low), pltpu.VMEM((own_rows, width), low), pltpu.VMEM((own_rows, width), low)] * 3
    scratch += [
        pltpu.VMEM((own_rows, width), f32),
        pltpu.VMEM((all_rows, width), low),
        pltpu.VMEM((all_rows, width), low),
        pltpu.VMEM((all_rows, width), low),
        pltpu.VMEM((pieces, att_rows, toks), low),
        pltpu.VMEM((pieces, att_rows, toks), low),
        pltpu.VMEM((unit_rows, DOCUMENT_LIMIT), low),
        pltpu.VMEM((att_rows, DOCUMENT_LIMIT), low),
        pltpu.VMEM((HEAD_SIZE, DOCUMENT_LIMIT), f32),
        pltpu.VMEM((HEAD_SIZE, DOCUMENT_LIMIT), f32),
        pltpu.VMEM((pieces, unit_rows, toks), low),
        pltpu.VMEM((pieces, unit_rows, toks), low),
        pltpu.VMEM((heads * att_rows, all_rows), low),
        pltpu.VMEM((heads * unit_rows, all_rows), low),
        pltpu.VMEM((width, heads * att_rows), low),
        pltpu.VMEM((HEAD_SIZE // 2, DOCUMENT_LIMIT), f32),
        pltpu.VMEM((HEAD_SIZE // 2, DOCUMENT_LIMIT), f32),
        pltpu.VMEM((DOCUMENT_LIMIT, 1), f32),
        pltpu.VMEM((1, DOCUMENT_LIMIT), f32),
        pltpu.VMEM((1, DOCUMENT_LIMIT), f32),
    ]
    scratch += [pltpu.VMEM((depth, c), low) for c in columns]
    scratch += [pltpu.VMEM((chips * depth, c), low) for c in columns]
    scratch += [pltpu.VMEM((depth // 2, c), low) for c in columns] * 2
    scratch += [pltpu.VMEM((stages, 2, width), f32)] * 2
    scratch += [pltpu.SemaphoreType.DMA((128,))] * 2 + [pltpu.SemaphoreType.DMA((len(far),))]
    return pl.pallas_call(
        functools.partial(backward_kernel, micro, group, chips),
        out_shape=tuple(outs),
        in_specs=[vmem_spec] * len(near) + [any_spec] * len(far),
        out_specs=tuple([vmem_spec] * len(outs)),
        scratch_shapes=scratch,
        compiler_params=pltpu.CompilerParams(collective_id=1, has_side_effects=True, vmem_limit_bytes=63 << 20),
    )(*near, *far)


def vmem_call(kernel, outs, scratch, flops, *operands):
    spec = pl.BlockSpec(memory_space=pltpu.VMEM)
    moved = sum(math.prod(a.shape) * a.dtype.itemsize for a in operands + tuple(outs))
    return pl.pallas_call(
        kernel,
        out_shape=tuple(outs),
        in_specs=[spec] * len(operands),
        out_specs=tuple([spec] * len(outs)),
        scratch_shapes=scratch,
        cost_estimate=pl.CostEstimate(flops=flops, bytes_accessed=moved, transcendentals=2 * DOCUMENT_LIMIT**2),
        compiler_params=pltpu.CompilerParams(vmem_limit_bytes=48 << 20),
    )(*operands)


def on_device(
    block_input,
    segments,
    positions,
    query_weight,
    key_matrix,
    value_matrix,
    out_weight,
    gate_weight,
    up_weight,
    down_weight,
    gain_first,
    gain_second,
    cotangent,
):
    chips, tp_count = lax.axis_size("chip"), lax.axis_size("tp")
    chip, core = lax.axis_index("chip"), lax.axis_index("core")
    cp_count, cp_index = chips * CORES, chip * CORES + core
    micro, tok_dev, width = block_input.shape
    dim = HEAD_SIZE
    block_rows = tok_dev * tp_count // 2
    query_heads, value_heads = query_weight.shape[1] // dim, key_matrix.shape[1] // dim
    group = query_heads // value_heads
    unit_rows = (group + 2) * dim
    head_cores = CORES if value_heads % CORES == 0 else 1
    heads = value_heads // head_cores
    toks = head_cores * block_rows
    pieces = DOCUMENT_LIMIT // toks
    assert pieces == micro * 2 * heads and cp_count % (pieces * head_cores) == 0

    by_head = jnp.concatenate(
        [
            query_weight.reshape(-1, value_heads, group * dim),
            key_matrix.reshape(-1, value_heads, dim),
            value_matrix.reshape(-1, value_heads, dim),
        ],
        axis=2,
    ).reshape(query_weight.shape[0], -1)
    out_t, down_t = out_weight.T, down_weight.T

    def halves(matrix):
        half = matrix.shape[1] // 2
        return matrix[:, :half], matrix[:, half:]

    def gather_head_weight(matrix):
        if head_cores == 2:
            return ring_gather(core_split(*halves(matrix)))
        return lax.all_gather(matrix, ("chip", "core"), axis=0, tiled=True)

    def scatter_head_weight(grads):
        if head_cores == 2:
            return jnp.concatenate(core_merge(ring_scatter(grads)), axis=1)
        return lax.psum_scatter(grads, ("chip", "core"), scatter_dimension=0, tiled=True).astype(f32)

    fused = tp_count == 2 and head_cores == CORES and pieces == chips
    if not fused:
        head_full = gather_head_weight(by_head)
        out_full = gather_head_weight(out_t)
        gate_full = ring_gather(core_split(*halves(gate_weight)))
        up_full = ring_gather(core_split(*halves(up_weight)))
        down_full = ring_gather(core_split(*halves(down_t)))

    by_block = lambda line: line.reshape(micro, cp_count, 2, block_rows)
    group_cp = pieces * head_cores
    first_cp = cp_index // head_cores * head_cores
    row_pos = lax.dynamic_slice_in_dim(by_block(positions), first_cp, head_cores, 1)
    row_pos = row_pos.transpose(0, 2, 1, 3).reshape(-1)
    unit_index = cp_index // head_cores % pieces
    unit_micro, unit_half = unit_index // (2 * heads), unit_index // heads % 2

    def unit_line(line):
        mine = lax.dynamic_slice(
            by_block(line),
            (unit_micro, cp_index // group_cp * group_cp, unit_half, 0),
            (1, group_cp, 1, block_rows),
        )
        return mine.reshape(1, DOCUMENT_LIMIT)

    unit_pos, unit_seg = unit_line(positions), unit_line(segments)
    if not fused:
        first_code = unit_seg * DOCUMENT_LIMIT
        last_code = first_code + unit_pos
        code_column = last_code.reshape(DOCUMENT_LIMIT, 1)
        cosine, sine = angles_of(row_pos)
        unit_cosine, unit_sine = angles_of(unit_pos.reshape(-1))

    if head_cores == 2:
        exchange_axis = "chip"
        groups = [[g + i for i in range(pieces)] for g in range(0, chips, pieces)]
    else:
        exchange_axis = ("chip", "core")
        groups = [[g + i for i in range(pieces)] for g in range(0, cp_count, pieces)]
    groups = None if len(groups) == 1 else groups

    def exchange(values):
        return lax.all_to_all(values, exchange_axis, 0, 0, axis_index_groups=groups)

    def to_units(values):
        rows = values.shape[0] // heads
        return values.reshape(heads, rows, micro * 2, toks).transpose(2, 0, 1, 3).reshape(pieces, rows, toks)

    def from_units(values):
        rows = values.shape[1]
        return values.reshape(micro * 2, heads, rows, toks).transpose(1, 2, 0, 3).reshape(heads * rows, -1)

    gather_head_rows = functools.partial(gather_rows, micro_count=micro, cores=head_cores)
    scatter_head_rows = functools.partial(scatter_rows, micro_count=micro, cores=head_cores)
    gather_all_rows = functools.partial(gather_rows, micro_count=micro, cores=CORES)
    scatter_all_rows = functools.partial(scatter_rows, micro_count=micro, cores=CORES)

    own_input = block_input.reshape(-1, width).astype(f32)
    cot_own = cotangent.reshape(-1, width)
    square = DOCUMENT_LIMIT * DOCUMENT_LIMIT * dim * 2 * group
    own_rows = block_input.reshape(-1, width)
    gains = [gain_first.reshape(1, -1), gain_second.reshape(1, -1)]
    frequency = frequencies().reshape(-1, 1)
    if fused:
        (
            head_full, out_full, gate_full, up_full, down_full, first_t, second_rows, cot_rows, second_t, cot_t, unit, att_pieces, unit_stat, residual
        ) = forward_call(
            micro, group, chips, heads,
            own_rows, cot_own, by_head, out_t, gate_weight, up_weight, down_t, *gains, frequency, row_pos.reshape(1, -1), unit_pos, unit_seg,
        )
    else:
        first_rows = gather_head_rows((own_input * norm_scale(own_input) * gain_first).astype(low))
        projected = mm(head_full, first_rows, ((0,), (1,))).reshape(heads, unit_rows, -1)
        turned = projected[:, : (group + 1) * dim].reshape(heads, group + 1, 2, dim // 2, -1)
        front, back = turned[:, :, 0], turned[:, :, 1]
        turned = jnp.stack([front * cosine - back * sine, back * cosine + front * sine], axis=2)
        projected = jnp.concatenate(
            [turned.reshape(heads, (group + 1) * dim, -1).astype(low), projected[:, (group + 1) * dim :].astype(low)], axis=1
        )
        unit = exchange(to_units(projected.reshape(heads * unit_rows, -1)))
        unit_out, unit_stat = vmem_call(
            functools.partial(attend_kernel, group),
            (
                jax.ShapeDtypeStruct((pieces, group * dim, toks), low),
                jax.ShapeDtypeStruct((group, DOCUMENT_LIMIT), f32),
            ),
            [pltpu.VMEM((unit_rows, DOCUMENT_LIMIT), low)],
            2 * square,
            unit,
            code_column,
            last_code,
            first_code,
        )
        attended = from_units(exchange(unit_out))
        residual = own_input + scatter_head_rows(mm(attended, out_full, ((0,), (1,))).astype(low))

        second_rows = gather_all_rows((residual * norm_scale(residual) * gain_second).astype(low))
        cot_rows = gather_all_rows(cot_own)
    gate_value = mm(second_rows, gate_full, ((1,), (0,)))
    upward = mm(second_rows, up_full, ((1,), (0,)))
    sigma = jax.nn.sigmoid(gate_value)
    active = gate_value * sigma
    hidden = (active * upward).astype(low)
    grad_hidden = mm(cot_rows, down_full, ((1,), (0,)))
    gate_back = (grad_hidden * upward * (sigma * (1.0 + gate_value * (1.0 - sigma)))).astype(low)
    up_back = (grad_hidden * active).astype(low)
    second_parts = (mm(gate_back, gate_full, ((1,), (1,))) + mm(up_back, up_full, ((1,), (1,)))).astype(low)
    if fused:
        output_rows, input_grad, head_grad, out_grad, gate_grad, up_grad, down_grad, gain_sums = backward_call(
            micro, group, chips, heads,
            (own_rows, residual, cot_own, *gains, unit_stat, frequency, unit_pos, unit_seg),
            second_parts, cot_t, hidden, second_t, gate_back, up_back, unit, att_pieces, down_full, out_full, first_t, head_full,
        )
    else:
        grad_second_rows = scatter_all_rows(second_parts)
        down_grad = jnp.concatenate(core_merge(ring_scatter(mm(cot_rows, hidden, ((0,), (0,))).astype(low))), axis=1)
        gate_grad = jnp.concatenate(core_merge(ring_scatter(mm(second_rows, gate_back, ((0,), (0,))).astype(low))), axis=1)
        up_grad = jnp.concatenate(core_merge(ring_scatter(mm(second_rows, up_back, ((0,), (0,))).astype(low))), axis=1)
        output_rows = residual + scatter_all_rows(mm(hidden, down_full, ((1,), (1,))).astype(low))

        residual_part, gain_two = norm_back(residual, gain_second, grad_second_rows)
        grad_residual = cot_own.astype(f32) + residual_part
        grad_rows = gather_head_rows(grad_residual.astype(low))
        grad_attended = mm(out_full, grad_rows, ((0,), (1,))).astype(low)
        unit_grad = exchange(to_units(grad_attended))
        (unit_back,) = vmem_call(
            functools.partial(attend_back_kernel, group),
            (jax.ShapeDtypeStruct((pieces, unit_rows, toks), low),),
            [
                pltpu.VMEM((unit_rows, DOCUMENT_LIMIT), low),
                pltpu.VMEM((group * dim, DOCUMENT_LIMIT), low),
                pltpu.VMEM((dim, DOCUMENT_LIMIT), f32),
                pltpu.VMEM((dim, DOCUMENT_LIMIT), f32),
            ],
            5 * square,
            unit,
            unit_grad,
            code_column,
            last_code,
            first_code,
            unit_stat,
            unit_cosine,
            unit_sine,
        )
        back_rows = from_units(exchange(unit_back))
        grad_first_rows = scatter_head_rows(mm(back_rows, head_full, ((0,), (1,))).astype(low))
        head_grad = scatter_head_weight(mm(first_rows, back_rows, ((0,), (1,))).astype(low))
        out_grad = scatter_head_weight(mm(grad_rows, attended, ((0,), (1,))).astype(low))
        input_part, gain_one = norm_back(own_input, gain_first, grad_first_rows)
        input_grad = (grad_residual + input_part).astype(low)
        gain_sums = all_sum(jnp.stack([gain_one, gain_two]))

    head_grad = head_grad.reshape(-1, value_heads, unit_rows)
    columns = query_weight.shape[0]
    return (
        output_rows.astype(low).reshape(block_input.shape),
        input_grad.reshape(block_input.shape),
        head_grad[:, :, : group * dim].reshape(columns, -1),
        head_grad[:, :, group * dim : (group + 1) * dim].reshape(columns, -1),
        head_grad[:, :, (group + 1) * dim :].reshape(columns, -1),
        out_grad.T,
        gate_grad,
        up_grad,
        down_grad.T,
        gain_sums[0],
        gain_sums[1],
    )


def solution(mesh):
    cp_count, tp_count = mesh.shape["cp"], mesh.shape["tp"]
    fine = Mesh(mesh.devices.reshape(cp_count // CORES, CORES, tp_count), ("chip", "core", "tp"))
    cp = ("chip", "core")
    rows = P(None, cp + ("tp",), None)
    wide, tall = P(cp, "tp"), P("tp", cp)
    return jax.shard_map(
        on_device,
        mesh=fine,
        in_specs=(rows, P(), P(), wide, wide, wide, tall, wide, wide, tall, P(), P(), rows),
        out_specs=(rows, rows, wide, wide, wide, tall, wide, wide, tall, P(), P()),
        check_vma=False,
    )
```

```python
import functools
import math

import jax
import jax.numpy as jnp
from jax import lax
from jax.experimental import pallas as pl
from jax.experimental.pallas import tpu as pltpu
from jax.sharding import Mesh
from jax.sharding import PartitionSpec as P

HEAD_SIZE = 96
DOCUMENT_LIMIT = 1024
CORES = 2

eps_norm = 1e-05
rope_base = 100000.0
masked_score = -1e30


f32 = jnp.float32
low = jnp.bfloat16


def mm(left, right, dims):
    return lax.dot_general(left, right, (dims, ((), ())), preferred_element_type=f32)


def pair_swap(values, axis):
    return lax.ppermute(values, axis, [(0, 1), (1, 0)])


def both(values, axis):
    other = pair_swap(values, axis)
    first = lax.axis_index(axis) == 0
    return jnp.stack([jnp.where(first, values, other), jnp.where(first, other, values)])


def split_pair(low_part, high_part, axis):
    first = lax.axis_index(axis) == 0
    return jnp.where(first, low_part, high_part), jnp.where(first, high_part, low_part)


def ring_of(count):
    order = list(range(0, count, 2)) + list(range(count - 1, 0, -2))
    place = [order.index(chip) for chip in range(count)]
    ahead = [(order[i], order[(i + 1) % count]) for i in range(count)]
    back = [(order[i], order[(i - 1) % count]) for i in range(count)]
    return order, place, ahead, back


def ring_gather(block):
    count = lax.axis_size("chip")
    order, place, ahead, back = ring_of(count)
    spot = jnp.array(place)[lax.axis_index("chip")]
    half_way, half_rows = count // 2, block.shape[0] // 2

    def put(whole, piece, step):
        owner = jnp.array(order)[(spot + step) % count]
        return lax.dynamic_update_index_in_dim(whole, piece, owner, 0)

    whole = put(jnp.zeros((count,) + block.shape, block.dtype), block, 0)
    up = down = block
    for step in range(1, half_way):
        up, down = lax.ppermute(up, "chip", ahead), lax.ppermute(down, "chip", back)
        whole = put(put(whole, up, count - step), down, step)
    up = lax.ppermute(up[:half_rows], "chip", ahead)
    down = lax.ppermute(down[half_rows:], "chip", back)
    whole = put(whole, jnp.concatenate([up, down], axis=0), half_way)
    return whole.reshape((count * block.shape[0],) + block.shape[1:])


def ring_scatter(terms):
    count = lax.axis_size("chip")
    order, place, ahead, back = ring_of(count)
    spot = jnp.array(place)[lax.axis_index("chip")]
    rows = terms.shape[0] // count
    half_way, half_rows = count // 2, rows // 2
    terms = terms.reshape((count, rows) + terms.shape[1:])

    def own(step):
        owner = jnp.array(order)[(spot + step) % count]
        return lax.dynamic_index_in_dim(terms, owner, 0, keepdims=False).astype(f32)

    far = own(half_way).astype(low)
    up = lax.ppermute(far[:half_rows], "chip", ahead)
    down = lax.ppermute(far[half_rows:], "chip", back)
    for step in range(half_way - 1, 0, -1):
        own_up, own_down = own(step), own(count - step)
        if step == half_way - 1:
            up = jnp.concatenate([own_up[:half_rows] + up.astype(f32), own_up[half_rows:]], axis=0)
            down = jnp.concatenate([own_down[:half_rows], own_down[half_rows:] + down.astype(f32)], axis=0)
        else:
            up, down = own_up + up.astype(f32), own_down + down.astype(f32)
        up = lax.ppermute(up.astype(low), "chip", ahead)
        down = lax.ppermute(down.astype(low), "chip", back)
    return own(0) + up.astype(f32) + down.astype(f32)


def core_split(low_part, high_part):
    kept, sent = split_pair(low_part, high_part, "core")
    other = pair_swap(sent, "core")
    first = lax.axis_index("core") == 0
    return jnp.concatenate([jnp.where(first, kept, other), jnp.where(first, other, kept)], axis=0)


def core_merge(rows):
    half = rows.shape[0] // 2
    kept, sent = split_pair(rows[:half], rows[half:], "core")
    other = pair_swap(sent.astype(low), "core").astype(f32)
    first = lax.axis_index("core") == 0
    return jnp.where(first, kept, other), jnp.where(first, other, kept)


def all_sum(values):
    for axis in ("tp", "core", "chip"):
        step = 1
        while step < lax.axis_size(axis):
            pairs = [(i, i ^ step) for i in range(lax.axis_size(axis))]
            values = values + lax.ppermute(values, axis, pairs)
            step *= 2
    return values


def gather_rows(rows, micro_count, cores):
    width = rows.shape[-1]
    tp_count = lax.axis_size("tp")
    joined = both(rows, "tp") if tp_count == 2 else lax.all_gather(rows, "tp", axis=0)
    joined = both(joined, "core") if cores == 2 else joined
    joined = joined.reshape((cores, 2, tp_count // 2, micro_count, -1, width))
    return joined.transpose((3, 1, 0, 2, 4, 5)).reshape((-1, width))


def scatter_rows(parts, micro_count, cores):
    width = parts.shape[-1]
    tp_count = lax.axis_size("tp")
    parts = parts.reshape((micro_count, 2, cores, tp_count // 2, -1, width)).transpose((2, 1, 3, 0, 4, 5))
    parts = parts.reshape((cores, tp_count, -1, width))
    if cores == 2:
        kept, sent = split_pair(parts[0], parts[1], "core")
        parts = (kept.astype(f32) + pair_swap(sent, "core").astype(f32)).astype(low)
    else:
        parts = parts[0]
    if tp_count == 2:
        kept, sent = split_pair(parts[0], parts[1], "tp")
        return kept.astype(f32) + pair_swap(sent, "tp").astype(f32)
    return lax.psum_scatter(parts, "tp", scatter_dimension=0, tiled=False).astype(f32)


def norm_scale(values):
    return lax.rsqrt(jnp.mean(values * values, axis=-1, keepdims=True) + eps_norm)


def norm_back(values, gain, grads):
    rho = norm_scale(values)
    scaled = grads * gain
    inner = jnp.mean(scaled * values, axis=-1, keepdims=True)
    return rho * scaled - values * (rho * rho * rho * inner), jnp.sum(grads * values * rho, axis=0)


def frequencies():
    return jnp.exp(jnp.arange(HEAD_SIZE // 2, dtype=f32) * (-2.0 * math.log(rope_base) / HEAD_SIZE))


def angles_of(spots):
    angles = frequencies()[:, None] * spots.astype(f32)[None, :]
    return jnp.cos(angles), jnp.sin(angles)


def unit_chunks(tokens):
    width = min(256, tokens)
    return [slice(start, start + width) for start in range(0, tokens, width)]


def lay_out(pieces_ref, flat):
    count, _, width = pieces_ref.shape
    for piece in range(count):
        flat[:, piece * width : (piece + 1) * width] = pieces_ref[piece]


def allowed_keys(code_column, last_row, first_row):
    return (code_column <= last_row) & (code_column >= first_row)


def attend_kernel(group, pieces_ref, code_ref, last_ref, first_ref, out_ref, stat_ref, flat):
    dim = HEAD_SIZE
    count, _, width = pieces_ref.shape
    tokens = count * width
    score_scale = dim ** (-0.5)
    lay_out(pieces_ref, flat)
    key_rows = flat[group * dim : (group + 1) * dim, :].astype(f32).T.astype(low)
    value_t = flat[(group + 1) * dim :, :]
    for cols in unit_chunks(tokens):
        keep = allowed_keys(code_ref[...], last_ref[:, cols], first_ref[:, cols])
        for head in range(group):
            query_t = flat[head * dim : (head + 1) * dim, cols]
            scores = mm(key_rows, query_t, ((1,), (0,))) * score_scale
            scores = jnp.where(keep, scores, masked_score)
            maximum = jnp.max(scores, axis=0, keepdims=True)
            weights = jnp.exp(scores - maximum)
            totals = jnp.sum(weights, axis=0, keepdims=True)
            probs = (weights * (1.0 / totals)).astype(low)
            stat_ref[head : head + 1, cols] = maximum + jnp.log(totals)
            result = mm(value_t, probs, ((1,), (0,))).astype(low)
            for piece in range(cols.start // width, cols.stop // width):
                start = piece * width - cols.start
                out_ref[piece, head * dim : (head + 1) * dim, :] = result[:, start : start + width]


def attend_back_kernel(
    group, pieces_ref, grads_ref, code_ref, last_ref, first_ref, stat_ref, cos_ref, sin_ref, out_ref, flat, grad_flat, key_sum, value_sum
):
    dim = HEAD_SIZE
    half = dim // 2
    count, _, width = pieces_ref.shape
    tokens = count * width
    score_scale = dim ** (-0.5)
    lay_out(pieces_ref, flat)
    lay_out(grads_ref, grad_flat)
    key_t = flat[group * dim : (group + 1) * dim, :]
    key_rows = key_t.astype(f32).T.astype(low)
    value_rows = flat[(group + 1) * dim :, :].astype(f32).T.astype(low)

    def store(values, base, cols):
        for piece in range(cols.start // width, cols.stop // width):
            start = piece * width - cols.start
            out_ref[piece, base : base + values.shape[0], :] = values[:, start : start + width]

    def unturn(values, base, cols):
        front, back = values[:half] * score_scale, values[half:] * score_scale
        cosine, sine = cos_ref[:, cols], sin_ref[:, cols]
        store((front * cosine + back * sine).astype(low), base, cols)
        store((back * cosine - front * sine).astype(low), base + half, cols)

    for index, cols in enumerate(unit_chunks(tokens)):
        keep = allowed_keys(code_ref[...], last_ref[:, cols], first_ref[:, cols])
        for head in range(group):
            rows = slice(head * dim, (head + 1) * dim)
            query_t, grad_t = flat[rows, cols], grad_flat[rows, cols]
            scores = mm(key_rows, query_t, ((1,), (0,))) * score_scale
            probs = jnp.where(keep, jnp.exp(scores - stat_ref[head : head + 1, cols]), 0.0)
            grad_probs = mm(value_rows, grad_t, ((1,), (0,)))
            delta = jnp.sum(probs * grad_probs, axis=0, keepdims=True)
            grad_scores = (probs * (grad_probs - delta)).astype(low)
            unturn(mm(key_t, grad_scores, ((1,), (0,))), head * dim, cols)
            key_part = mm(query_t, grad_scores, ((1,), (1,)))
            value_part = mm(grad_t, probs.astype(low), ((1,), (1,)))
            if index == 0 and head == 0:
                key_sum[...] = key_part
                value_sum[...] = value_part
            else:
                key_sum[...] += key_part
                value_sum[...] += value_part
    everything = slice(0, tokens)
    unturn(key_sum[...], group * dim, everything)
    store(value_sum[...].astype(low), (group + 1) * dim, everything)


MESH_ID = pl.DeviceIdType.MESH


class Sems:
    def __init__(self, send, recv):
        self.send, self.recv, self.used = send, recv, 0

    def take(self, count=1):
        base = self.used
        self.used += count
        return base


def remote(sems, index, source, target, there, arrive=None):
    return pltpu.make_async_remote_copy(
        src_ref=source,
        dst_ref=target,
        send_sem=sems.send.at[index],
        recv_sem=sems.recv.at[index if arrive is None else arrive],
        device_id=there,
        device_id_type=MESH_ID,
    )


def greet(chips, chip, core, tp):
    barrier = pltpu.get_barrier_semaphore()

    @pl.loop(1, chips)
    def _(step):
        pl.semaphore_signal(barrier, inc=1, device_id={"chip": (chip + step) % chips}, device_id_type=MESH_ID)

    pl.semaphore_signal(barrier, inc=1, device_id={"core": 1 - core}, device_id_type=MESH_ID)
    pl.semaphore_signal(barrier, inc=1, device_id={"tp": 1 - tp}, device_id_type=MESH_ID)
    pl.semaphore_wait(barrier, chips + 1)


def spot_of(chip, count):
    odd = chip % 2
    return (1 - odd) * (chip // 2) + odd * (count - 1 - chip // 2)


def chip_at(spot, count):
    spot = (spot + count) % count
    far = spot // (count // 2)
    return (1 - far) * 2 * spot + far * (2 * (count - 1 - spot) + 1)


class Ring:
    def __init__(self, sems, whole, rows, count, chip, saved, save_sem):
        self.sems, self.whole, self.rows, self.count = sems, whole, rows, count
        self.saved, self.save_sem = saved, save_sem
        self.spot = spot_of(chip, count)
        self.half = count // 2
        self.base = sems.take(2 * self.half)
        self.ways = (1, -1)

    def copy(self, side, hop, behind):
        way = self.ways[side]
        start = chip_at(self.spot - way * behind, self.count) * self.rows
        size = self.rows
        if hop == self.half:
            size = self.rows // 2
            start = start + side * size
        piece = self.whole.at[pl.ds(pl.multiple_of(start, 16), size), :]
        there = {"chip": chip_at(self.spot + way, self.count)}
        return remote(self.sems, self.base + side * self.half + hop - 1, piece, piece, there)

    def save(self, side, hop, behind):
        way = self.ways[side]
        start = chip_at(self.spot - way * behind, self.count) * self.rows
        size = self.rows
        if hop == self.half:
            size = self.rows // 2
            start = start + side * size
        if self.saved is None:
            return
        piece = pl.ds(pl.multiple_of(start, 16), size)
        pltpu.make_async_copy(self.whole.at[piece, :], self.saved.at[piece, :], self.save_sem).start()

    def start(self):
        for side in (0, 1):
            self.copy(side, 1, 0).start()
        self.save(0, 1, 0)

    def arrive(self):
        for side in (0, 1):
            self.copy(side, self.half, self.half).wait_recv()
            self.save(side, self.half, self.half)

    def relay(self, hop):
        for side in (0, 1):
            self.copy(side, hop - 1, hop - 1).wait_recv()
            self.copy(side, hop, hop - 1).start()
        for side in (0, 1):
            self.save(side, hop - 1, hop - 1)

    def saves_done(self):
        if self.saved is not None:
            pltpu.make_async_copy(self.whole, self.saved, self.save_sem).wait()

    def drain(self):
        for side in (0, 1):
            for hop in range(1, self.half + 1):
                self.copy(side, hop, hop - 1).wait_send()


class Spread:
    def __init__(self, sems, whole, micro, where):
        self.sems, self.whole, self.micro = sems, whole, micro
        _, self.core, self.tp = where
        self.rows = whole.shape[0] // (4 * micro)
        self.base = sems.take(3 * micro)

    def rows_of(self, m, half, core):
        return pl.ds(pl.multiple_of(((m * 2 + half) * 2 + core) * self.rows, 16), self.rows)

    def place(self, m, half, core):
        return self.whole.at[self.rows_of(m, half, core), :]

    def put(self, m, values):
        self.whole[self.rows_of(m, self.tp, self.core), :] = values

    def over_tp(self, m, half):
        piece = self.place(m, half, self.core)
        return remote(self.sems, self.base + m, piece, piece, {"tp": 1 - self.tp})

    def over_core(self, m, core):
        piece = self.place(m, self.tp, core)
        return remote(self.sems, self.base + self.micro + m, piece, piece, {"core": 1 - self.core})

    def passed_on(self, m, core):
        piece = self.place(m, 1 - self.tp, core)
        return remote(self.sems, self.base + 2 * self.micro + m, piece, piece, {"core": 1 - self.core})

    def start(self, m):
        self.over_tp(m, self.tp).start()
        self.over_core(m, self.core).start()

    def pass_on(self):
        for m in range(self.micro):
            self.over_tp(m, 1 - self.tp).wait_recv()
            self.passed_on(m, self.core).start()

    def finish(self):
        for m in range(self.micro):
            self.over_core(m, 1 - self.core).wait_recv()
            self.passed_on(m, 1 - self.core).wait_recv()

    def drain(self):
        for m in range(self.micro):
            self.over_tp(m, self.tp).wait_send()
            self.over_core(m, self.core).wait_send()
            self.passed_on(m, self.core).wait_send()


def turn_over(whole, turned):
    lanes = 256

    @pl.loop(0, whole.shape[1] // lanes)
    def _(part):
        columns = pl.ds(pl.multiple_of(part * lanes, 128), lanes)
        turned[columns, :] = whole[:, columns].astype(f32).T.astype(low)


def gain_row(gain_ref):
    return gain_ref[...].reshape(1, gain_ref.shape[0])


def half_blocks(front, back, which):
    lanes = front.shape[1]
    front, back = jnp.broadcast_to(front, (8, lanes)), jnp.broadcast_to(back, (8, lanes))
    front = jnp.where(which == 0, front, pltpu.roll(front, lanes // 2, 1))
    back = jnp.where(which == 0, pltpu.roll(back, lanes // 2, 1), back)
    return jnp.where(lax.broadcasted_iota(jnp.int32, (8, lanes), 1) < lanes // 2, front, back)[:1]


def angle_tables(spots, columns, cos_ref, sin_ref):
    place = lax.broadcasted_iota(jnp.int32, (HEAD_SIZE // 2, spots.shape[1]), 0).astype(f32)
    angles = jnp.exp(place * (-2.0 * math.log(rope_base) / HEAD_SIZE)) * spots.astype(f32)
    cos_ref[:, columns] = jnp.cos(angles)
    sin_ref[:, columns] = jnp.sin(angles)


def chip_line(ref, row, chip, which, toks):
    start = pl.multiple_of(chip * 2 * toks, 256)
    parts = []
    for at in (start, start + toks):
        lines = ref[:, pl.ds(at, toks)]
        line = lines[:1]
        for other in range(1, lines.shape[0]):
            line = jnp.where(row == other, lines[other : other + 1], line)
        parts.append(line)
    return half_blocks(*parts, which)


def unit_codes(seg_ref, pos_ref, code_ref, last_ref, start_ref, chips, chip, heads, tables=None):
    micro, half = chip // (2 * heads), chip // heads % 2
    toks = DOCUMENT_LIMIT // chips
    for source in range(chips):
        columns = slice(source * toks, (source + 1) * toks)
        spots = chip_line(pos_ref, micro, source, half, toks)
        first = (chip_line(seg_ref, micro, source, half, toks) * DOCUMENT_LIMIT).astype(f32)
        start_ref[:, columns] = first
        last_ref[:, columns] = first + spots.astype(f32)
        if tables is not None:
            angle_tables(spots, columns, *tables)
    code_ref[...] = jnp.broadcast_to(last_ref[...], (8, DOCUMENT_LIMIT)).T[:, :1]


class Fold:
    def __init__(self, sems, parts, from_core, to_tp, from_tp, micro, chip_core_tp):
        self.sems, self.parts, self.from_core, self.to_tp, self.from_tp = sems, parts, from_core, to_tp, from_tp
        self.micro = micro
        _, self.core, self.tp = chip_core_tp
        self.rows = from_tp.shape[0] // micro
        self.base = sems.take(3 * micro)

    def piece(self, m, half, core):
        start = ((m * 2 + half) * 2 + core) * self.rows
        return pl.ds(pl.multiple_of(start, 16), self.rows)

    def landing(self, m, half):
        return pl.ds(pl.multiple_of((m * 2 + half) * self.rows, 16), self.rows)

    def over_core(self, m, half):
        source = self.parts.at[self.piece(m, half, 1 - self.core), :]
        index = self.base + m * 2 + half
        return remote(self.sems, index, source, self.from_core.at[self.landing(m, half), :], {"core": 1 - self.core})

    def over_tp(self, m):
        rows = pl.ds(m * self.rows, self.rows)
        index = self.base + 2 * self.micro + m
        return remote(self.sems, index, self.to_tp.at[rows, :], self.from_tp.at[rows, :], {"tp": 1 - self.tp})

    def start(self, m, half):
        self.over_core(m, half).start()

    def summed(self, m, half):
        mine = self.parts[self.piece(m, half, self.core), :].astype(f32)
        return mine + self.from_core[self.landing(m, half), :].astype(f32)

    def send(self, m):
        for half in (0, 1):
            self.over_core(m, half).wait_recv()
        self.to_tp[m * self.rows : (m + 1) * self.rows, :] = self.summed(m, 1 - self.tp).astype(low)
        self.over_tp(m).start()

    def result(self, m):
        kept = self.summed(m, self.tp)
        self.over_tp(m).wait_recv()
        return kept + self.from_tp[m * self.rows : (m + 1) * self.rows, :].astype(f32)

    def drain(self):
        for m in range(self.micro):
            for half in (0, 1):
                self.over_core(m, half).wait_send()
            self.over_tp(m).wait_send()


class Exchange:
    def __init__(self, sems, outgoing, incoming, chips, chip):
        self.sems, self.outgoing, self.incoming, self.chips, self.chip = sems, outgoing, incoming, chips, chip
        self.base = sems.take(chips)

    def copy(self, to):
        return remote(
            self.sems, self.base + to, self.outgoing.at[to], self.incoming.at[self.chip], {"chip": to}, self.base + self.chip
        )

    def send(self, to):
        @pl.when(to != self.chip)
        def _():
            self.copy(to).start()

        @pl.when(to == self.chip)
        def _():
            self.incoming[to] = self.outgoing[to]

    def finish(self):
        @pl.loop(1, self.chips)
        def _(step):
            source = (self.chip + step) % self.chips
            remote(
                self.sems, self.base + source, self.outgoing.at[source], self.incoming.at[source], {"chip": source}
            ).wait_recv()

    def drain(self):
        @pl.loop(1, self.chips)
        def _(step):
            self.copy((self.chip + step) % self.chips).wait_send()


class Actions:
    def __init__(self, steps):
        self.steps = list(steps)

    def run(self, count=None):
        count = len(self.steps) if count is None else count
        for step in self.steps[:count]:
            step()
        self.steps = self.steps[count:]


def unit_sources(group, heads, head):
    queries = [(head * group + member) * HEAD_SIZE for member in range(group)]
    return queries + [(heads * group + head) * HEAD_SIZE, (heads * group + heads + head) * HEAD_SIZE]


def forward_kernel(
    micro, group, chips,
    x_ref, cot_ref, head_ref, out_ref, gate_ref, up_ref, down_ref, gain_one_ref, gain_two_ref, pos_ref, seg_ref,
    head_o, out_o, down_o, first_o, second_t_o, cot_t_o, unit_o, att_o, hidden_o, gate_back_o, up_back_o, second_o, stat_ref, residual_ref,
    head_w, out_w, gate_w, up_w, down_w, first_all, second_all, cot_all, first_t, second_t, cot_t, unit_send, unit_in, flat, att_send, att_in,
    parts, from_core, to_tp, from_tp, cos_ref, sin_ref, code_ref, last_ref, start_ref,
    gate_value, grad_hidden, hidden, gate_back, up_back, second_parts, send_sem, recv_sem, local_sem, save_sem,
):
    dim = HEAD_SIZE
    half = dim // 2
    chip, core, tp = lax.axis_index("chip"), lax.axis_index("core"), lax.axis_index("tp")
    where = (chip, core, tp)
    sems = Sems(send_sem, recv_sem)
    rows = x_ref.shape[0] // micro
    toks = 2 * rows
    unit_rows = (group + 2) * dim
    heads = head_w.shape[1] // unit_rows
    hops = chips // 2
    depth = head_ref.shape[0]
    greet(chips, chip, core, tp)

    weights = ((head_ref, head_w, head_o), (out_ref, out_w, out_o), (down_ref, down_w, down_o), (gate_ref, gate_w, None), (up_ref, up_w, None))
    rings, swaps, keeps = [], [], []
    for index, (shard, whole, saved) in enumerate(weights):
        columns = whole.shape[1]
        mine = whole.at[pl.ds(pl.multiple_of((chip * 2 + core) * depth, 16), depth), :]
        theirs = whole.at[pl.ds(pl.multiple_of((chip * 2 + 1 - core) * depth, 16), depth), :]
        at = sems.take()
        give = shard.at[:, pl.ds(pl.multiple_of((1 - core) * columns, 128), columns)]
        hold = shard.at[:, pl.ds(pl.multiple_of(core * columns, 128), columns)]
        swaps.append((remote(sems, at, give, mine, {"core": 1 - core}), remote(sems, at, give, theirs, {"core": 1 - core})))
        keeps.append(pltpu.make_async_copy(hold, mine, local_sem.at[index]))
        rings.append(Ring(sems, whole, 2 * depth, chips, chip, saved, save_sem.at[index]))
    first, second, cot = (Spread(sems, whole, micro, where) for whole in (first_all, second_all, cot_all))
    to_unit = Exchange(sems, unit_send, unit_in, chips, chip)
    from_unit = Exchange(sems, att_send, att_in, chips, chip)
    fold = Fold(sems, parts, from_core, to_tp, from_tp, micro, where)
    saves = []

    def save(source, target):
        saves.append(pltpu.make_async_copy(source, target, save_sem.at[5 + len(saves)]))
        saves[-1].start()

    for index in (0, 1):
        swaps[index][0].start()
        keeps[index].start()
    for m in range(micro):
        values = x_ref[m * rows : (m + 1) * rows, :].astype(f32)
        first.put(m, (values * norm_scale(values) * gain_row(gain_one_ref)).astype(low))
    for index in (2, 3, 4):
        swaps[index][0].start()
        keeps[index].start()
    for m in range(micro):
        cot.put(m, cot_ref[m * rows : (m + 1) * rows, :])
        first.start(m)
    head_ring, out_ring, down_ring, gate_ring, up_ring = rings
    for index in (0, 1):
        keeps[index].wait()
        swaps[index][1].wait_recv()
        rings[index].start()
    for m in range(micro):
        for side in (0, 1):
            columns = slice((m * 2 + side) * toks, (m * 2 + side + 1) * toks)
            angle_tables(chip_line(pos_ref, m, chip, side, toks), columns, cos_ref, sin_ref)
    first.pass_on()
    for hop in range(2, hops + 1):
        head_ring.relay(hop)
        out_ring.relay(hop)
    for index in (2, 3, 4):
        keeps[index].wait()
        swaps[index][1].wait_recv()
    down_ring.start()
    first.finish()
    head_ring.arrive()
    later = Actions(
        [ring.start for ring in (gate_ring, up_ring)]
        + [functools.partial(ring.relay, hop) for hop in range(2, hops + 1) for ring in (down_ring, gate_ring, up_ring)]
    )

    @pl.loop(0, micro * 2)
    def _(block):
        tokens = pl.ds(pl.multiple_of(block * toks, 128), toks)
        lines = mm(first_all[tokens, :], head_w[...], ((1,), (0,))).T
        cosine, sine = cos_ref[:, tokens], sin_ref[:, tokens]
        for head in range(heads):
            u = block * heads + head
            for turn, source in enumerate(unit_sources(group, heads, head)):
                front, back = lines[source : source + half], lines[source + half : source + dim]
                if turn < group + 1:
                    front, back = front * cosine - back * sine, back * cosine + front * sine
                unit_send[u, turn * dim : turn * dim + half, :] = front.astype(low)
                unit_send[u, turn * dim + half : (turn + 1) * dim, :] = back.astype(low)
            to_unit.send(u)

    later.run(1)
    for m in range(micro):
        cot.start(m)
    out_ring.arrive()
    unit_codes(seg_ref, pos_ref, code_ref, last_ref, start_ref, chips, chip, heads)
    later.run(2)
    cot.pass_on()
    to_unit.finish()

    score_scale = dim ** (-0.5)
    lay_out(unit_in, flat)
    save(unit_in, unit_o)
    key_rows = flat[group * dim : (group + 1) * dim, :].astype(f32).T.astype(low)
    lanes = 256

    @pl.loop(0, chips * toks // lanes)
    def _(number):
        cols = pl.ds(pl.multiple_of(number * lanes, 128), lanes)
        keep = allowed_keys(code_ref[...], last_ref[:, cols], start_ref[:, cols])
        for head in range(group):
            query_t = flat[head * dim : (head + 1) * dim, cols]
            scores = mm(key_rows, query_t, ((1,), (0,))) * score_scale
            scores = jnp.where(keep, scores, masked_score)
            maximum = jnp.max(scores, axis=0, keepdims=True)
            exponents = jnp.exp(scores - maximum)
            totals = jnp.sum(exponents, axis=0, keepdims=True)
            probs = (exponents * (1.0 / totals)).astype(low)
            stat_ref[head : head + 1, cols] = maximum + jnp.log(totals)
            result = mm(flat[(group + 1) * dim :, :], probs, ((1,), (0,))).astype(low)
            for piece in range(lanes // toks):
                here = result[:, piece * toks : (piece + 1) * toks]
                att_send[number * (lanes // toks) + piece, head * dim : (head + 1) * dim, :] = here
        for piece in range(lanes // toks):
            from_unit.send(number * (lanes // toks) + piece)

        @pl.when(number == 1)
        def _():
            later.run(1)

    later.run(1)
    cot.finish()
    turn_over(cot_all, cot_t)
    save(cot_t, cot_t_o)
    turn_over(first_all, first_t)
    save(first_t, first_o)
    from_unit.finish()
    save(att_in, att_o)

    @pl.loop(0, micro * 2)
    def _(block):
        lines = jnp.concatenate([att_in[block * heads + head] for head in range(heads)], axis=0)
        lines = lines.astype(f32).T.astype(low)
        sums = mm(lines, out_w[...], ((1,), (1,)))
        parts[pl.ds(pl.multiple_of(block * toks, 128), toks), :] = sums.astype(low)
        fold.start(block // 2, block % 2)

    for m in range(micro):
        fold.send(m)
    later.run(1)
    for m in range(micro):
        own = slice(m * rows, (m + 1) * rows)
        residual = x_ref[own, :].astype(f32) + fold.result(m)
        residual_ref[own, :] = residual
        second.put(m, (residual * norm_scale(residual) * gain_row(gain_two_ref)).astype(low))
        second.start(m)
    later.run(2)
    second.pass_on()
    second.finish()
    turn_over(second_all, second_t)
    save(second_t, second_t_o)
    later.run()

    lanes = 256
    hidden_blocks = gate_w.shape[1] // lanes

    def block_of(part):
        return pl.ds(pl.multiple_of(part * lanes, 128), lanes)

    down_ring.arrive()

    @pl.loop(0, hidden_blocks)
    def _(part):
        cols = block_of(part)
        grad_hidden[:, cols] = mm(cot_all[...], down_w[:, cols], ((1,), (0,)))

    gate_ring.arrive()

    @pl.loop(0, hidden_blocks)
    def _(part):
        cols = block_of(part)
        gate_value[:, cols] = mm(second_all[...], gate_w[:, cols], ((1,), (0,)))

    up_ring.arrive()

    @pl.loop(0, hidden_blocks)
    def _(part):
        cols = block_of(part)
        upward = mm(second_all[...], up_w[:, cols], ((1,), (0,)))
        value, grads = gate_value[:, cols], grad_hidden[:, cols]
        sigma = 1.0 / (1.0 + jnp.exp(-value))
        active = value * sigma
        hidden[:, cols] = (active * upward).astype(low)
        gate_back[:, cols] = (grads * upward * (sigma * (1.0 + value * (1.0 - sigma)))).astype(low)
        up_back[:, cols] = (grads * active).astype(low)

    save(hidden, hidden_o)
    save(gate_back, gate_back_o)
    save(up_back, up_back_o)

    @pl.loop(0, second_parts.shape[1] // lanes)
    def _(part):
        cols = block_of(part)
        sums = mm(gate_back[...], gate_w[cols, :], ((1,), (1,))) + mm(up_back[...], up_w[cols, :], ((1,), (1,)))
        second_parts[:, cols] = sums.astype(low)

    save(second_parts, second_o)
    for part in saves:
        part.wait()
    for ring in rings:
        ring.saves_done()
    for swap, _ in swaps:
        swap.wait_send()
    for part in rings + [first, second, cot, to_unit, from_unit, fold]:
        part.drain()


def forward_call(micro, group, chips, heads, *operands):
    x, _, head_s, out_s, gate_s, up_s, down_s = operands[:7]
    own_rows, width = x.shape
    toks = own_rows // micro * 2
    all_rows = own_rows * 4
    pieces = micro * 2 * heads
    unit_rows, att_rows = (group + 2) * HEAD_SIZE, group * HEAD_SIZE
    shape = jax.ShapeDtypeStruct
    columns = [s.shape[1] // CORES for s in (head_s, out_s, gate_s, up_s, down_s)]
    any_spec, vmem_spec = pl.BlockSpec(memory_space=pl.ANY), pl.BlockSpec(memory_space=pltpu.VMEM)
    hidden = columns[-1]
    any_outs = [shape((width, c), low) for c in (columns[0], columns[1], hidden)] + [shape((width, all_rows), low)] * 3
    any_outs += [shape((pieces, unit_rows, toks), low), shape((pieces, att_rows, toks), low)]
    any_outs += [shape((all_rows, hidden), low)] * 3 + [shape((all_rows, width), low)]
    vmem_outs = [shape((group, DOCUMENT_LIMIT), f32), shape((own_rows, width), f32)]
    scratch = [pltpu.VMEM((width, c), low) for c in columns]
    scratch += [pltpu.VMEM((all_rows, width), low)] * 3 + [pltpu.VMEM((width, all_rows), low)] * 3
    scratch += [
        pltpu.VMEM((pieces, unit_rows, toks), low),
        pltpu.VMEM((pieces, unit_rows, toks), low),
        pltpu.VMEM((unit_rows, DOCUMENT_LIMIT), low),
        pltpu.VMEM((pieces, att_rows, toks), low),
        pltpu.VMEM((pieces, att_rows, toks), low),
        pltpu.VMEM((all_rows, width), low),
        pltpu.VMEM((all_rows // 2, width), low),
        pltpu.VMEM((own_rows, width), low),
        pltpu.VMEM((own_rows, width), low),
        pltpu.VMEM((HEAD_SIZE // 2, all_rows), f32),
        pltpu.VMEM((HEAD_SIZE // 2, all_rows), f32),
        pltpu.VMEM((DOCUMENT_LIMIT, 1), f32),
        pltpu.VMEM((1, DOCUMENT_LIMIT), f32),
        pltpu.VMEM((1, DOCUMENT_LIMIT), f32),
        pltpu.VMEM((all_rows, hidden), f32),
        pltpu.VMEM((all_rows, hidden), f32),
        pltpu.VMEM((all_rows, hidden), low),
        pltpu.VMEM((all_rows, hidden), low),
        pltpu.VMEM((all_rows, hidden), low),
        pltpu.VMEM((all_rows, width), low),
        pltpu.SemaphoreType.DMA((96,)),
        pltpu.SemaphoreType.DMA((96,)),
        pltpu.SemaphoreType.DMA((5,)),
        pltpu.SemaphoreType.DMA((16,)),
    ]
    return pl.pallas_call(
        functools.partial(forward_kernel, micro, group, chips),
        out_shape=tuple(any_outs + vmem_outs),
        in_specs=[vmem_spec] * 2 + [any_spec] * 5 + [vmem_spec] * (len(operands) - 7),
        out_specs=tuple([any_spec] * len(any_outs) + [vmem_spec] * len(vmem_outs)),
        scratch_shapes=scratch,
        compiler_params=pltpu.CompilerParams(collective_id=0, has_side_effects=True, vmem_limit_bytes=60 << 20),
    )(*operands)


class RingSum:
    def __init__(self, sems, make, far, slots, count, chip, core):
        self.sems, self.make, self.far, self.slots, self.count, self.chip, self.core = sems, make, far, slots, count, chip, core
        self.rows = far.shape[0]
        self.spot = spot_of(chip, count)
        self.half = count // 2
        self.base = sems.take(2 * self.half)
        self.ways = (1, -1)

    def slot(self, side, hop):
        return (side * self.half + hop - 1) * self.rows

    def term(self, side, distance):
        return chip_at(self.spot + self.ways[side] * distance, self.count) * self.rows

    def copy(self, side, hop):
        there = {"chip": chip_at(self.spot + self.ways[side], self.count)}
        index = self.base + side * self.half + hop - 1
        if hop == 1:
            size = self.rows // 2
            source = self.far.at[side * size : (side + 1) * size, :]
            target = self.slots.at[pl.ds(self.slot(side, 1) + side * size, size), :]
        else:
            source = self.slots.at[pl.ds(self.slot(side, hop - 1), self.rows), :]
            target = self.slots.at[pl.ds(self.slot(side, hop), self.rows), :]
        return remote(self.sems, index, source, target, there)

    def start(self):
        self.far[...] = self.make((self.term(0, self.half),), self.rows).astype(low)
        for side in (0, 1):
            self.copy(side, 1).start()

    def relay(self, hop):
        size = self.rows // 2
        own = self.make([self.term(side, self.half - hop + 1) for side in (0, 1)], self.rows)
        for side in (0, 1):
            self.copy(side, hop - 1).wait_recv()
            at = self.slot(side, hop - 1)
            for part in (0, 1):
                here = pl.ds(at + part * size, size)
                mine = own[side * self.rows + part * size : side * self.rows + (part + 1) * size]
                if hop == 2 and part != side:
                    self.slots[here, :] = mine.astype(low)
                else:
                    self.slots[here, :] = (mine + self.slots[here, :].astype(f32)).astype(low)
            self.copy(side, hop).start()

    def result(self):
        size = self.rows // 2
        offsets = [self.core * size, (1 - self.core) * size]
        own = self.make([self.chip * self.rows + offset for offset in offsets], size)
        for side in (0, 1):
            self.copy(side, self.half).wait_recv()
        sums = []
        for index, offset in enumerate(offsets):
            total = own[index * size : (index + 1) * size]
            for side in (0, 1):
                here = pl.ds(pl.multiple_of(self.slot(side, self.half) + offset, 16), size)
                total = total + self.slots[here, :].astype(f32)
            sums.append(total)
        return sums

    def drain(self):
        for side in (0, 1):
            for hop in range(1, self.half + 1):
                self.copy(side, hop).wait_send()


def rows_from(ref, starts, size):
    blocks = [ref[pl.ds(pl.multiple_of(start, 16), size), :] for start in starts]
    return blocks[0] if len(blocks) == 1 else jnp.concatenate(blocks, axis=0)


class Merge:
    def __init__(self, sems, ring, leaving, landing, out, core):
        self.sems, self.ring, self.leaving, self.landing, self.out, self.core = sems, ring, leaving, landing, out, core
        self.index = sems.take()

    def copy(self):
        return remote(self.sems, self.index, self.leaving, self.landing, {"core": 1 - self.core})

    def send(self):
        kept, sent = self.ring.result()
        self.leaving[...] = sent.astype(low)
        self.copy().start()
        columns = self.leaving.shape[1]
        self.out[:, pl.ds(pl.multiple_of(self.core * columns, 128), columns)] = kept

    def finish(self):
        columns = self.leaving.shape[1]
        self.copy().wait_recv()
        self.out[:, pl.ds(pl.multiple_of((1 - self.core) * columns, 128), columns)] = self.landing[...].astype(f32)

    def drain(self):
        self.copy().wait_send()


class Butterfly:
    def __init__(self, sems, leaving, landing, chips, where):
        self.sems, self.leaving, self.landing = sems, leaving, landing
        chip, core, tp = where
        self.partners = [{"tp": 1 - tp}, {"core": 1 - core}]
        step = 1
        while step < chips:
            self.partners.append({"chip": chip + step - 2 * step * (chip // step % 2)})
            step *= 2
        self.base = sems.take(len(self.partners))

    def copy(self, stage):
        return remote(self.sems, self.base + stage, self.leaving.at[stage], self.landing.at[stage], self.partners[stage])

    def start(self, values):
        self.leaving[0] = values
        self.copy(0).start()

    def step(self, stage):
        self.copy(stage).wait_recv()
        values = self.leaving[stage] + self.landing[stage]
        if stage + 1 < len(self.partners):
            self.leaving[stage + 1] = values
            self.copy(stage + 1).start()
        return values

    def drain(self):
        for stage in range(len(self.partners)):
            self.copy(stage).wait_send()


def backward_kernel(
    micro, group, chips,
    x_ref, residual_ref, cot_ref, gain_one_ref, gain_two_ref, stat_ref, pos_ref, seg_ref,
    second_h, cot_t_h, hidden_h, second_t_h, gate_back_h, up_back_h, unit_h, att_h, down_h, out_h, first_t_h, head_h,
    output_ref, input_grad_ref, head_g, out_g, gate_g, up_g, down_g, gain_one_g, gain_two_g,
    second_parts, cot_t, hidden, second_t, gate_back, up_back, unit_ref, att_ref, down_w, out_w, first_t, head_w,
    core_a, to_tp_a, from_tp_a, core_b, to_tp_b, from_tp_b, core_c, to_tp_c, from_tp_c, grad_residual, grad_all, output_parts, first_parts,
    grad_send, grad_in, flat, grad_flat, key_sum, value_sum, back_send, back_in, att_flat, back_flat, out_terms,
    cos_ref, sin_ref, code_ref, last_ref, start_ref,
    head_far, out_far, down_far, gate_far, up_far, head_slots, out_slots, down_slots, gate_slots, up_slots,
    head_leave, out_leave, down_leave, gate_leave, up_leave, head_land, out_land, down_land, gate_land, up_land,
    gain_leave, gain_land, send_sem, recv_sem, local_sem,
):
    dim = HEAD_SIZE
    half = dim // 2
    chip, core, tp = lax.axis_index("chip"), lax.axis_index("core"), lax.axis_index("tp")
    where = (chip, core, tp)
    sems = Sems(send_sem, recv_sem)
    rows = x_ref.shape[0] // micro
    toks = 2 * rows
    unit_rows = (group + 2) * dim
    heads = head_w.shape[1] // unit_rows
    blocks = micro * 2
    hops = chips // 2
    sources = (second_h, cot_t_h, hidden_h, second_t_h, gate_back_h, up_back_h, unit_h, att_h, down_h, out_h, first_t_h, head_h)
    places = (second_parts, cot_t, hidden, second_t, gate_back, up_back, unit_ref, att_ref, down_w, out_w, first_t, head_w)
    loads = [pltpu.make_async_copy(a, b, local_sem.at[i]) for i, (a, b) in enumerate(zip(sources, places))]
    for load in loads:
        load.start()
    greet(chips, chip, core, tp)

    def ring_of_products(left, right, far, slots):
        make = lambda starts, size: mm(rows_from(left, starts, size), right[...], ((1,), (0,)))
        return RingSum(sems, make, far, slots, chips, chip, core)

    down_ring = ring_of_products(cot_t, hidden, down_far, down_slots)
    gate_ring = ring_of_products(second_t, gate_back, gate_far, gate_slots)
    up_ring = ring_of_products(second_t, up_back, up_far, up_slots)
    out_ring = RingSum(sems, lambda starts, size: rows_from(out_terms, starts, size).astype(f32), out_far, out_slots, chips, chip, core)
    head_ring = RingSum(
        sems, lambda starts, size: mm(rows_from(first_t, starts, size), back_flat[...], ((1,), (1,))), head_far, head_slots, chips, chip, core
    )
    down_merge, gate_merge, up_merge, out_merge, head_merge = (
        Merge(sems, down_ring, down_leave, down_land, down_g, core),
        Merge(sems, gate_ring, gate_leave, gate_land, gate_g, core),
        Merge(sems, up_ring, up_leave, up_land, up_g, core),
        Merge(sems, out_ring, out_leave, out_land, out_g, core),
        Merge(sems, head_ring, head_leave, head_land, head_g, core),
    )
    second_fold = Fold(sems, second_parts, core_a, to_tp_a, from_tp_a, micro, where)
    output_fold = Fold(sems, output_parts, core_b, to_tp_b, from_tp_b, micro, where)
    first_fold = Fold(sems, first_parts, core_c, to_tp_c, from_tp_c, micro, where)
    spread = Spread(sems, grad_all, micro, where)
    to_unit = Exchange(sems, grad_send, grad_in, chips, chip)
    from_unit = Exchange(sems, back_send, back_in, chips, chip)
    butterfly = Butterfly(sems, gain_leave, gain_land, chips, where)
    later = Actions([functools.partial(ring.relay, hop) for hop in range(2, hops + 1) for ring in (down_ring, gate_ring, up_ring)])

    loads[0].wait()
    for m in range(micro):
        for side in (0, 1):
            second_fold.start(m, side)
    for load in loads[1:3]:
        load.wait()
    down_ring.start()
    for m in range(micro):
        second_fold.send(m)
    for load in loads[3:6]:
        load.wait()
    gate_ring.start()
    up_ring.start()

    def norm_rows_back(values, gain, grads):
        rho = norm_scale(values)
        scaled = grads * gain
        inner = jnp.mean(scaled * values, axis=-1, keepdims=True)
        return rho * scaled - values * (rho * rho * rho * inner), jnp.sum(grads * values * rho, axis=0, keepdims=True)

    later.run(1)
    gain_two = None
    for m in range(micro):
        own = slice(m * rows, (m + 1) * rows)
        part, gain_now = norm_rows_back(residual_ref[own, :], gain_row(gain_two_ref), second_fold.result(m))
        gain_two = gain_now if gain_two is None else gain_two + gain_now
        grads = cot_ref[own, :].astype(f32) + part
        grad_residual[own, :] = grads
        spread.put(m, grads.astype(low))
        spread.start(m)
    for load in loads[6:8]:
        load.wait()
    lay_out(unit_ref, flat)
    for piece in range(blocks * heads):
        block, head = piece // heads, piece % heads
        att_flat[head * group * dim : (head + 1) * group * dim, block * toks : (block + 1) * toks] = att_ref[piece]
    key_t = flat[group * dim : (group + 1) * dim, :]
    key_rows = key_t.astype(f32).T.astype(low)
    value_rows = flat[(group + 1) * dim :, :].astype(f32).T.astype(low)
    unit_codes(seg_ref, pos_ref, code_ref, last_ref, start_ref, chips, chip, heads, (cos_ref, sin_ref))
    later.run(1)
    spread.pass_on()
    for load in loads[8:10]:
        load.wait()
    later.run(1)
    spread.finish()

    @pl.loop(0, blocks)
    def _(block):
        tokens = pl.ds(pl.multiple_of(block * toks, 128), toks)
        lines = mm(grad_all[tokens, :], out_w[...], ((1,), (0,))).T.astype(low)
        for head in range(heads):
            piece = block * heads + head
            grad_send[piece] = lines[head * group * dim : (head + 1) * group * dim]
            to_unit.send(piece)

    later.run(1)

    @pl.loop(0, blocks)
    def _(block):
        tokens = pl.ds(pl.multiple_of(block * toks, 128), toks)
        output_parts[tokens, :] = mm(hidden[tokens, :], down_w[...], ((1,), (1,))).astype(low)
        output_fold.start(block // 2, block % 2)

    lanes = 256

    @pl.loop(0, grad_all.shape[1] // lanes)
    def _(part):
        columns = pl.ds(pl.multiple_of(part * lanes, 128), lanes)
        out_terms[columns, :] = mm(att_flat[...], grad_all[:, columns], ((1,), (0,))).T.astype(low)

    out_ring.start()
    later.run(1)
    for m in range(micro):
        output_fold.send(m)
    to_unit.finish()
    lay_out(grad_in, grad_flat)

    score_scale = dim ** (-0.5)
    tokens_all = chips * toks
    key_sum[...] = jnp.zeros_like(key_sum)
    value_sum[...] = jnp.zeros_like(value_sum)

    def store(values, base, first_piece):
        for piece in range(values.shape[1] // toks):
            back_send[first_piece + piece, base : base + values.shape[0], :] = values[:, piece * toks : (piece + 1) * toks]

    def unturn(values, base, cols, first_piece):
        front, back = values[:half] * score_scale, values[half:] * score_scale
        cosine, sine = cos_ref[:, cols], sin_ref[:, cols]
        store((front * cosine + back * sine).astype(low), base, first_piece)
        store((back * cosine - front * sine).astype(low), base + half, first_piece)

    @pl.loop(0, tokens_all // lanes)
    def _(number):
        cols = pl.ds(pl.multiple_of(number * lanes, 128), lanes)
        keep = allowed_keys(code_ref[...], last_ref[:, cols], start_ref[:, cols])
        for head in range(group):
            lines = slice(head * dim, (head + 1) * dim)
            query_t, grad_t = flat[lines, cols], grad_flat[lines, cols]
            scores = mm(key_rows, query_t, ((1,), (0,))) * score_scale
            probs = jnp.where(keep, jnp.exp(scores - stat_ref[head : head + 1, cols]), 0.0)
            grad_probs = mm(value_rows, grad_t, ((1,), (0,)))
            delta = jnp.sum(probs * grad_probs, axis=0, keepdims=True)
            grad_scores = (probs * (grad_probs - delta)).astype(low)
            unturn(mm(key_t, grad_scores, ((1,), (0,))), head * dim, cols, number * (lanes // toks))
            key_sum[...] += mm(query_t, grad_scores, ((1,), (1,)))
            value_sum[...] += mm(grad_t, probs.astype(low), ((1,), (1,)))

        @pl.when(number == 1)
        def _():
            later.run(1)

    unturn(key_sum[...], group * dim, slice(0, tokens_all), 0)
    store(value_sum[...].astype(low), (group + 1) * dim, 0)

    @pl.loop(0, chips)
    def _(piece):
        from_unit.send(piece)

    later.run(1)
    for m in range(micro):
        own = slice(m * rows, (m + 1) * rows)
        output_ref[own, :] = (residual_ref[own, :] + output_fold.result(m)).astype(low)
    later.run(1)
    for load in loads[10:]:
        load.wait()
    from_unit.finish()

    for block in range(blocks):
        for head in range(heads):
            for turn, target in enumerate(unit_sources(group, heads, head)):
                piece = back_in[block * heads + head, turn * dim : (turn + 1) * dim, :]
                back_flat[target : target + dim, block * toks : (block + 1) * toks] = piece
    head_ring.start()

    @pl.loop(0, blocks)
    def _(block):
        tokens = pl.ds(pl.multiple_of(block * toks, 128), toks)
        lines = back_flat[:, tokens].astype(f32).T.astype(low)
        first_parts[tokens, :] = mm(lines, head_w[...], ((1,), (1,))).astype(low)
        first_fold.start(block // 2, block % 2)

    later.run(1)
    head_ring.relay(2)
    for m in range(micro):
        first_fold.send(m)
    later.run()
    for hop in range(2, hops + 1):
        if hop > 2:
            head_ring.relay(hop)
        out_ring.relay(hop)
        if hop == 2:
            down_merge.send()
    gain_one = None
    for m in range(micro):
        own = slice(m * rows, (m + 1) * rows)
        part, gain_now = norm_rows_back(x_ref[own, :].astype(f32), gain_row(gain_one_ref), first_fold.result(m))
        gain_one = gain_now if gain_one is None else gain_one + gain_now
        input_grad_ref[own, :] = (grad_residual[own, :] + part).astype(low)
    butterfly.start(jnp.concatenate([gain_one, gain_two], axis=0))
    gate_merge.send()
    butterfly.step(0)
    up_merge.send()
    butterfly.step(1)
    down_merge.finish()
    for stage in range(2, len(butterfly.partners) - 1):
        butterfly.step(stage)
    out_merge.send()
    gate_merge.finish()
    head_merge.send()
    up_merge.finish()
    gain_sums = butterfly.step(len(butterfly.partners) - 1)
    gain_one_g[...] = gain_sums[0]
    gain_two_g[...] = gain_sums[1]
    out_merge.finish()
    head_merge.finish()
    parts = [down_ring, gate_ring, up_ring, out_ring, head_ring, down_merge, gate_merge, up_merge, out_merge, head_merge]
    parts += [second_fold, output_fold, first_fold, spread, to_unit, from_unit, butterfly]
    for part in parts:
        part.drain()


def backward_call(micro, group, chips, heads, near, *far):
    own_rows, width = near[0].shape
    toks = own_rows // micro * 2
    all_rows = own_rows * 4
    pieces = micro * 2 * heads
    unit_rows, att_rows = (group + 2) * HEAD_SIZE, group * HEAD_SIZE
    shape = jax.ShapeDtypeStruct
    hidden = far[2].shape[1]
    depth = width // chips
    columns = [heads * unit_rows, heads * att_rows, hidden, hidden, hidden]
    stages = 2 + (chips - 1).bit_length()
    any_spec, vmem_spec = pl.BlockSpec(memory_space=pl.ANY), pl.BlockSpec(memory_space=pltpu.VMEM)
    outs = [shape((own_rows, width), low)] * 2 + [shape((depth // 2, 2 * c), f32) for c in columns] + [shape((width,), f32)] * 2
    scratch = [pltpu.VMEM(a.shape, a.dtype) for a in far]
    scratch += [pltpu.VMEM((all_rows // 2, width), low), pltpu.VMEM((own_rows, width), low), pltpu.VMEM((own_rows, width), low)] * 3
    scratch += [
        pltpu.VMEM((own_rows, width), f32),
        pltpu.VMEM((all_rows, width), low),
        pltpu.VMEM((all_rows, width), low),
        pltpu.VMEM((all_rows, width), low),
        pltpu.VMEM((pieces, att_rows, toks), low),
        pltpu.VMEM((pieces, att_rows, toks), low),
        pltpu.VMEM((unit_rows, DOCUMENT_LIMIT), low),
        pltpu.VMEM((att_rows, DOCUMENT_LIMIT), low),
        pltpu.VMEM((HEAD_SIZE, DOCUMENT_LIMIT), f32),
        pltpu.VMEM((HEAD_SIZE, DOCUMENT_LIMIT), f32),
        pltpu.VMEM((pieces, unit_rows, toks), low),
        pltpu.VMEM((pieces, unit_rows, toks), low),
        pltpu.VMEM((heads * att_rows, all_rows), low),
        pltpu.VMEM((heads * unit_rows, all_rows), low),
        pltpu.VMEM((width, heads * att_rows), low),
        pltpu.VMEM((HEAD_SIZE // 2, DOCUMENT_LIMIT), f32),
        pltpu.VMEM((HEAD_SIZE // 2, DOCUMENT_LIMIT), f32),
        pltpu.VMEM((DOCUMENT_LIMIT, 1), f32),
        pltpu.VMEM((1, DOCUMENT_LIMIT), f32),
        pltpu.VMEM((1, DOCUMENT_LIMIT), f32),
    ]
    scratch += [pltpu.VMEM((depth, c), low) for c in columns]
    scratch += [pltpu.VMEM((chips * depth, c), low) for c in columns]
    scratch += [pltpu.VMEM((depth // 2, c), low) for c in columns] * 2
    scratch += [pltpu.VMEM((stages, 2, width), f32)] * 2
    scratch += [pltpu.SemaphoreType.DMA((128,))] * 2 + [pltpu.SemaphoreType.DMA((len(far),))]
    return pl.pallas_call(
        functools.partial(backward_kernel, micro, group, chips),
        out_shape=tuple(outs),
        in_specs=[vmem_spec] * len(near) + [any_spec] * len(far),
        out_specs=tuple([vmem_spec] * len(outs)),
        scratch_shapes=scratch,
        compiler_params=pltpu.CompilerParams(collective_id=1, has_side_effects=True, vmem_limit_bytes=63 << 20),
    )(*near, *far)


def vmem_call(kernel, outs, scratch, flops, *operands):
    spec = pl.BlockSpec(memory_space=pltpu.VMEM)
    moved = sum(math.prod(a.shape) * a.dtype.itemsize for a in operands + tuple(outs))
    return pl.pallas_call(
        kernel,
        out_shape=tuple(outs),
        in_specs=[spec] * len(operands),
        out_specs=tuple([spec] * len(outs)),
        scratch_shapes=scratch,
        cost_estimate=pl.CostEstimate(flops=flops, bytes_accessed=moved, transcendentals=2 * DOCUMENT_LIMIT**2),
        compiler_params=pltpu.CompilerParams(vmem_limit_bytes=48 << 20),
    )(*operands)


def on_device(
    block_input,
    segments,
    positions,
    query_weight,
    key_matrix,
    value_matrix,
    out_weight,
    gate_weight,
    up_weight,
    down_weight,
    gain_first,
    gain_second,
    cotangent,
):
    chips, tp_count = lax.axis_size("chip"), lax.axis_size("tp")
    chip, core = lax.axis_index("chip"), lax.axis_index("core")
    cp_count, cp_index = chips * CORES, chip * CORES + core
    micro, tok_dev, width = block_input.shape
    dim = HEAD_SIZE
    block_rows = tok_dev * tp_count // 2
    query_heads, value_heads = query_weight.shape[1] // dim, key_matrix.shape[1] // dim
    group = query_heads // value_heads
    unit_rows = (group + 2) * dim
    head_cores = CORES if value_heads % CORES == 0 else 1
    heads = value_heads // head_cores
    toks = head_cores * block_rows
    pieces = DOCUMENT_LIMIT // toks
    assert pieces == micro * 2 * heads and cp_count % (pieces * head_cores) == 0

    out_t, down_t = out_weight.T, down_weight.T

    def halves(matrix):
        half = matrix.shape[1] // 2
        return matrix[:, :half], matrix[:, half:]

    def gather_head_weight(matrix):
        if head_cores == 2:
            return ring_gather(core_split(*halves(matrix)))
        return lax.all_gather(matrix, ("chip", "core"), axis=0, tiled=True)

    def scatter_head_weight(grads):
        if head_cores == 2:
            return jnp.concatenate(core_merge(ring_scatter(grads)), axis=1)
        return lax.psum_scatter(grads, ("chip", "core"), scatter_dimension=0, tiled=True).astype(f32)

    fused = tp_count == 2 and head_cores == CORES and pieces == chips and toks == 128
    if fused:
        cores = []
        for part in range(CORES):
            columns = lambda matrix: matrix[:, part * matrix.shape[1] // CORES : (part + 1) * matrix.shape[1] // CORES]
            cores += [columns(query_weight), columns(key_matrix), columns(value_matrix)]
        by_head = jnp.concatenate(cores, axis=1)
    else:
        by_head = jnp.concatenate(
            [
                query_weight.reshape(-1, value_heads, group * dim),
                key_matrix.reshape(-1, value_heads, dim),
                value_matrix.reshape(-1, value_heads, dim),
            ],
            axis=2,
        ).reshape(query_weight.shape[0], -1)
        head_full = gather_head_weight(by_head)
        out_full = gather_head_weight(out_t)
        gate_full = ring_gather(core_split(*halves(gate_weight)))
        up_full = ring_gather(core_split(*halves(up_weight)))
        down_full = ring_gather(core_split(*halves(down_t)))

    by_block = lambda line: line.reshape(micro, cp_count, 2, block_rows)
    group_cp = pieces * head_cores
    first_cp = cp_index // head_cores * head_cores
    if not fused:
        row_pos = lax.dynamic_slice_in_dim(by_block(positions), first_cp, head_cores, 1)
        row_pos = row_pos.transpose(0, 2, 1, 3).reshape(-1)
        unit_index = cp_index // head_cores % pieces
        unit_micro, unit_half = unit_index // (2 * heads), unit_index // heads % 2

        def unit_line(line):
            mine = lax.dynamic_slice(
                by_block(line),
                (unit_micro, cp_index // group_cp * group_cp, unit_half, 0),
                (1, group_cp, 1, block_rows),
            )
            return mine.reshape(1, DOCUMENT_LIMIT)

        unit_pos, unit_seg = unit_line(positions), unit_line(segments)
        first_code = unit_seg * DOCUMENT_LIMIT
        last_code = first_code + unit_pos
        code_column = last_code.reshape(DOCUMENT_LIMIT, 1)
        cosine, sine = angles_of(row_pos)
        unit_cosine, unit_sine = angles_of(unit_pos.reshape(-1))

    if head_cores == 2:
        exchange_axis = "chip"
        groups = [[g + i for i in range(pieces)] for g in range(0, chips, pieces)]
    else:
        exchange_axis = ("chip", "core")
        groups = [[g + i for i in range(pieces)] for g in range(0, cp_count, pieces)]
    groups = None if len(groups) == 1 else groups

    def exchange(values):
        return lax.all_to_all(values, exchange_axis, 0, 0, axis_index_groups=groups)

    def to_units(values):
        rows = values.shape[0] // heads
        return values.reshape(heads, rows, micro * 2, toks).transpose(2, 0, 1, 3).reshape(pieces, rows, toks)

    def from_units(values):
        rows = values.shape[1]
        return values.reshape(micro * 2, heads, rows, toks).transpose(1, 2, 0, 3).reshape(heads * rows, -1)

    gather_head_rows = functools.partial(gather_rows, micro_count=micro, cores=head_cores)
    scatter_head_rows = functools.partial(scatter_rows, micro_count=micro, cores=head_cores)
    gather_all_rows = functools.partial(gather_rows, micro_count=micro, cores=CORES)
    scatter_all_rows = functools.partial(scatter_rows, micro_count=micro, cores=CORES)

    own_input = block_input.reshape(-1, width).astype(f32)
    cot_own = cotangent.reshape(-1, width)
    square = DOCUMENT_LIMIT * DOCUMENT_LIMIT * dim * 2 * group
    own_rows = block_input.reshape(-1, width)
    if fused:
        facts = (gain_first, gain_second, positions, segments)
        head_full, out_full, down_full, first_t, second_t, cot_t, unit, att_pieces, hidden, gate_back, up_back, second_parts, unit_stat, residual = (
            forward_call(micro, group, chips, heads, own_rows, cot_own, by_head, out_t, gate_weight, up_weight, down_t, *facts)
        )
        output_rows, input_grad, head_grad, out_grad, gate_grad, up_grad, down_grad, *gain_sums = backward_call(
            micro, group, chips, heads,
            (own_rows, residual, cot_own, gain_first, gain_second, unit_stat, positions, segments),
            second_parts, cot_t, hidden, second_t, gate_back, up_back, unit, att_pieces, down_full, out_full, first_t, head_full,
        )
    else:
        first_rows = gather_head_rows((own_input * norm_scale(own_input) * gain_first).astype(low))
        projected = mm(head_full, first_rows, ((0,), (1,))).reshape(heads, unit_rows, -1)
        turned = projected[:, : (group + 1) * dim].reshape(heads, group + 1, 2, dim // 2, -1)
        front, back = turned[:, :, 0], turned[:, :, 1]
        turned = jnp.stack([front * cosine - back * sine, back * cosine + front * sine], axis=2)
        projected = jnp.concatenate(
            [turned.reshape(heads, (group + 1) * dim, -1).astype(low), projected[:, (group + 1) * dim :].astype(low)], axis=1
        )
        unit = exchange(to_units(projected.reshape(heads * unit_rows, -1)))
        unit_out, unit_stat = vmem_call(
            functools.partial(attend_kernel, group),
            (
                jax.ShapeDtypeStruct((pieces, group * dim, toks), low),
                jax.ShapeDtypeStruct((group, DOCUMENT_LIMIT), f32),
            ),
            [pltpu.VMEM((unit_rows, DOCUMENT_LIMIT), low)],
            2 * square,
            unit,
            code_column,
            last_code,
            first_code,
        )
        attended = from_units(exchange(unit_out))
        residual = own_input + scatter_head_rows(mm(attended, out_full, ((0,), (1,))).astype(low))

        second_rows = gather_all_rows((residual * norm_scale(residual) * gain_second).astype(low))
        cot_rows = gather_all_rows(cot_own)
        gate_value = mm(second_rows, gate_full, ((1,), (0,)))
        upward = mm(second_rows, up_full, ((1,), (0,)))
        sigma = jax.nn.sigmoid(gate_value)
        active = gate_value * sigma
        hidden = (active * upward).astype(low)
        grad_hidden = mm(cot_rows, down_full, ((1,), (0,)))
        gate_back = (grad_hidden * upward * (sigma * (1.0 + gate_value * (1.0 - sigma)))).astype(low)
        up_back = (grad_hidden * active).astype(low)
        second_parts = (mm(gate_back, gate_full, ((1,), (1,))) + mm(up_back, up_full, ((1,), (1,)))).astype(low)
        grad_second_rows = scatter_all_rows(second_parts)
        down_grad = jnp.concatenate(core_merge(ring_scatter(mm(cot_rows, hidden, ((0,), (0,))).astype(low))), axis=1)
        gate_grad = jnp.concatenate(core_merge(ring_scatter(mm(second_rows, gate_back, ((0,), (0,))).astype(low))), axis=1)
        up_grad = jnp.concatenate(core_merge(ring_scatter(mm(second_rows, up_back, ((0,), (0,))).astype(low))), axis=1)
        output_rows = residual + scatter_all_rows(mm(hidden, down_full, ((1,), (1,))).astype(low))

        residual_part, gain_two = norm_back(residual, gain_second, grad_second_rows)
        grad_residual = cot_own.astype(f32) + residual_part
        grad_rows = gather_head_rows(grad_residual.astype(low))
        grad_attended = mm(out_full, grad_rows, ((0,), (1,))).astype(low)
        unit_grad = exchange(to_units(grad_attended))
        (unit_back,) = vmem_call(
            functools.partial(attend_back_kernel, group),
            (jax.ShapeDtypeStruct((pieces, unit_rows, toks), low),),
            [
                pltpu.VMEM((unit_rows, DOCUMENT_LIMIT), low),
                pltpu.VMEM((group * dim, DOCUMENT_LIMIT), low),
                pltpu.VMEM((dim, DOCUMENT_LIMIT), f32),
                pltpu.VMEM((dim, DOCUMENT_LIMIT), f32),
            ],
            5 * square,
            unit,
            unit_grad,
            code_column,
            last_code,
            first_code,
            unit_stat,
            unit_cosine,
            unit_sine,
        )
        back_rows = from_units(exchange(unit_back))
        grad_first_rows = scatter_head_rows(mm(back_rows, head_full, ((0,), (1,))).astype(low))
        head_grad = scatter_head_weight(mm(first_rows, back_rows, ((0,), (1,))).astype(low))
        out_grad = scatter_head_weight(mm(grad_rows, attended, ((0,), (1,))).astype(low))
        input_part, gain_one = norm_back(own_input, gain_first, grad_first_rows)
        input_grad = (grad_residual + input_part).astype(low)
        gain_sums = all_sum(jnp.stack([gain_one, gain_two]))

    if fused:
        part_widths = [matrix.shape[1] // CORES for matrix in (query_weight, key_matrix, value_matrix)]
        starts = [0, part_widths[0], part_widths[0] + part_widths[1]]
        core_width = sum(part_widths)
        query_grad, key_grad, value_grad = (
            jnp.concatenate([head_grad[:, part * core_width + at : part * core_width + at + size] for part in range(CORES)], axis=1)
            for at, size in zip(starts, part_widths)
        )
    else:
        head_grad = head_grad.reshape(-1, value_heads, unit_rows)
        columns = query_weight.shape[0]
        query_grad = head_grad[:, :, : group * dim].reshape(columns, -1)
        key_grad = head_grad[:, :, group * dim : (group + 1) * dim].reshape(columns, -1)
        value_grad = head_grad[:, :, (group + 1) * dim :].reshape(columns, -1)
    return (
        output_rows.astype(low).reshape(block_input.shape),
        input_grad.reshape(block_input.shape),
        query_grad,
        key_grad,
        value_grad,
        out_grad.T,
        gate_grad,
        up_grad,
        down_grad.T,
        gain_sums[0],
        gain_sums[1],
    )


def solution(mesh):
    cp_count, tp_count = mesh.shape["cp"], mesh.shape["tp"]
    fine = Mesh(mesh.devices.reshape(cp_count // CORES, CORES, tp_count), ("chip", "core", "tp"))
    cp = ("chip", "core")
    rows = P(None, cp + ("tp",), None)
    wide, tall = P(cp, "tp"), P("tp", cp)
    return jax.shard_map(
        on_device,
        mesh=fine,
        in_specs=(rows, P(), P(), wide, wide, wide, tall, wide, wide, tall, P(), P(), rows),
        out_specs=(rows, rows, wide, wide, wide, tall, wide, wide, tall, P(), P()),
        check_vma=False,
    )
```

```python
import functools
import math

import jax
import jax.numpy as jnp
from jax import lax
from jax.experimental import pallas as pl
from jax.experimental.pallas import tpu as pltpu
from jax.sharding import Mesh
from jax.sharding import PartitionSpec as P

HEAD_SIZE = 96
DOCUMENT_LIMIT = 1024
CORES = 2

eps_norm = 1e-05
rope_base = 100000.0
masked_score = -1e30


f32 = jnp.float32
low = jnp.bfloat16


def mm(left, right, dims):
    return lax.dot_general(left, right, (dims, ((), ())), preferred_element_type=f32)


def pair_swap(values, axis):
    return lax.ppermute(values, axis, [(0, 1), (1, 0)])


def both(values, axis):
    other = pair_swap(values, axis)
    first = lax.axis_index(axis) == 0
    return jnp.stack([jnp.where(first, values, other), jnp.where(first, other, values)])


def split_pair(low_part, high_part, axis):
    first = lax.axis_index(axis) == 0
    return jnp.where(first, low_part, high_part), jnp.where(first, high_part, low_part)


def ring_of(count):
    order = list(range(0, count, 2)) + list(range(count - 1, 0, -2))
    place = [order.index(chip) for chip in range(count)]
    ahead = [(order[i], order[(i + 1) % count]) for i in range(count)]
    back = [(order[i], order[(i - 1) % count]) for i in range(count)]
    return order, place, ahead, back


def ring_gather(block):
    count = lax.axis_size("chip")
    order, place, ahead, back = ring_of(count)
    spot = jnp.array(place)[lax.axis_index("chip")]
    half_way, half_rows = count // 2, block.shape[0] // 2

    def put(whole, piece, step):
        owner = jnp.array(order)[(spot + step) % count]
        return lax.dynamic_update_index_in_dim(whole, piece, owner, 0)

    whole = put(jnp.zeros((count,) + block.shape, block.dtype), block, 0)
    up = down = block
    for step in range(1, half_way):
        up, down = lax.ppermute(up, "chip", ahead), lax.ppermute(down, "chip", back)
        whole = put(put(whole, up, count - step), down, step)
    up = lax.ppermute(up[:half_rows], "chip", ahead)
    down = lax.ppermute(down[half_rows:], "chip", back)
    whole = put(whole, jnp.concatenate([up, down], axis=0), half_way)
    return whole.reshape((count * block.shape[0],) + block.shape[1:])


def ring_scatter(terms):
    count = lax.axis_size("chip")
    order, place, ahead, back = ring_of(count)
    spot = jnp.array(place)[lax.axis_index("chip")]
    rows = terms.shape[0] // count
    half_way, half_rows = count // 2, rows // 2
    terms = terms.reshape((count, rows) + terms.shape[1:])

    def own(step):
        owner = jnp.array(order)[(spot + step) % count]
        return lax.dynamic_index_in_dim(terms, owner, 0, keepdims=False).astype(f32)

    far = own(half_way).astype(low)
    up = lax.ppermute(far[:half_rows], "chip", ahead)
    down = lax.ppermute(far[half_rows:], "chip", back)
    for step in range(half_way - 1, 0, -1):
        own_up, own_down = own(step), own(count - step)
        if step == half_way - 1:
            up = jnp.concatenate([own_up[:half_rows] + up.astype(f32), own_up[half_rows:]], axis=0)
            down = jnp.concatenate([own_down[:half_rows], own_down[half_rows:] + down.astype(f32)], axis=0)
        else:
            up, down = own_up + up.astype(f32), own_down + down.astype(f32)
        up = lax.ppermute(up.astype(low), "chip", ahead)
        down = lax.ppermute(down.astype(low), "chip", back)
    return own(0) + up.astype(f32) + down.astype(f32)


def core_split(low_part, high_part):
    kept, sent = split_pair(low_part, high_part, "core")
    other = pair_swap(sent, "core")
    first = lax.axis_index("core") == 0
    return jnp.concatenate([jnp.where(first, kept, other), jnp.where(first, other, kept)], axis=0)


def core_merge(rows):
    half = rows.shape[0] // 2
    kept, sent = split_pair(rows[:half], rows[half:], "core")
    other = pair_swap(sent.astype(low), "core").astype(f32)
    first = lax.axis_index("core") == 0
    return jnp.where(first, kept, other), jnp.where(first, other, kept)


def all_sum(values):
    for axis in ("tp", "core", "chip"):
        step = 1
        while step < lax.axis_size(axis):
            pairs = [(i, i ^ step) for i in range(lax.axis_size(axis))]
            values = values + lax.ppermute(values, axis, pairs)
            step *= 2
    return values


def gather_rows(rows, micro_count, cores):
    width = rows.shape[-1]
    tp_count = lax.axis_size("tp")
    joined = both(rows, "tp") if tp_count == 2 else lax.all_gather(rows, "tp", axis=0)
    joined = both(joined, "core") if cores == 2 else joined
    joined = joined.reshape((cores, 2, tp_count // 2, micro_count, -1, width))
    return joined.transpose((3, 1, 0, 2, 4, 5)).reshape((-1, width))


def scatter_rows(parts, micro_count, cores):
    width = parts.shape[-1]
    tp_count = lax.axis_size("tp")
    parts = parts.reshape((micro_count, 2, cores, tp_count // 2, -1, width)).transpose((2, 1, 3, 0, 4, 5))
    parts = parts.reshape((cores, tp_count, -1, width))
    if cores == 2:
        kept, sent = split_pair(parts[0], parts[1], "core")
        parts = (kept.astype(f32) + pair_swap(sent, "core").astype(f32)).astype(low)
    else:
        parts = parts[0]
    if tp_count == 2:
        kept, sent = split_pair(parts[0], parts[1], "tp")
        return kept.astype(f32) + pair_swap(sent, "tp").astype(f32)
    return lax.psum_scatter(parts, "tp", scatter_dimension=0, tiled=False).astype(f32)


def norm_scale(values):
    return lax.rsqrt(jnp.mean(values * values, axis=-1, keepdims=True) + eps_norm)


def norm_back(values, gain, grads):
    rho = norm_scale(values)
    scaled = grads * gain
    inner = jnp.mean(scaled * values, axis=-1, keepdims=True)
    return rho * scaled - values * (rho * rho * rho * inner), jnp.sum(grads * values * rho, axis=0)


def frequencies():
    return jnp.exp(jnp.arange(HEAD_SIZE // 2, dtype=f32) * (-2.0 * math.log(rope_base) / HEAD_SIZE))


def angles_of(spots):
    angles = frequencies()[:, None] * spots.astype(f32)[None, :]
    return jnp.cos(angles), jnp.sin(angles)


def unit_chunks(tokens):
    width = min(256, tokens)
    return [slice(start, start + width) for start in range(0, tokens, width)]


def lay_out(pieces_ref, flat):
    count, _, width = pieces_ref.shape
    for piece in range(count):
        flat[:, piece * width : (piece + 1) * width] = pieces_ref[piece]


def allowed_keys(code_column, last_row, first_row):
    return (code_column <= last_row) & (code_column >= first_row)


def attend_kernel(group, pieces_ref, code_ref, last_ref, first_ref, out_ref, stat_ref, flat):
    dim = HEAD_SIZE
    count, _, width = pieces_ref.shape
    tokens = count * width
    score_scale = dim ** (-0.5)
    lay_out(pieces_ref, flat)
    key_rows = flat[group * dim : (group + 1) * dim, :].astype(f32).T.astype(low)
    value_t = flat[(group + 1) * dim :, :]
    for cols in unit_chunks(tokens):
        keep = allowed_keys(code_ref[...], last_ref[:, cols], first_ref[:, cols])
        for head in range(group):
            query_t = flat[head * dim : (head + 1) * dim, cols]
            scores = mm(key_rows, query_t, ((1,), (0,))) * score_scale
            scores = jnp.where(keep, scores, masked_score)
            maximum = jnp.max(scores, axis=0, keepdims=True)
            weights = jnp.exp(scores - maximum)
            totals = jnp.sum(weights, axis=0, keepdims=True)
            probs = (weights * (1.0 / totals)).astype(low)
            stat_ref[head : head + 1, cols] = maximum + jnp.log(totals)
            result = mm(value_t, probs, ((1,), (0,))).astype(low)
            for piece in range(cols.start // width, cols.stop // width):
                start = piece * width - cols.start
                out_ref[piece, head * dim : (head + 1) * dim, :] = result[:, start : start + width]


def attend_back_kernel(
    group, pieces_ref, grads_ref, code_ref, last_ref, first_ref, stat_ref, cos_ref, sin_ref, out_ref, flat, grad_flat, key_sum, value_sum
):
    dim = HEAD_SIZE
    half = dim // 2
    count, _, width = pieces_ref.shape
    tokens = count * width
    score_scale = dim ** (-0.5)
    lay_out(pieces_ref, flat)
    lay_out(grads_ref, grad_flat)
    key_t = flat[group * dim : (group + 1) * dim, :]
    key_rows = key_t.astype(f32).T.astype(low)
    value_rows = flat[(group + 1) * dim :, :].astype(f32).T.astype(low)

    def store(values, base, cols):
        for piece in range(cols.start // width, cols.stop // width):
            start = piece * width - cols.start
            out_ref[piece, base : base + values.shape[0], :] = values[:, start : start + width]

    def unturn(values, base, cols):
        front, back = values[:half] * score_scale, values[half:] * score_scale
        cosine, sine = cos_ref[:, cols], sin_ref[:, cols]
        store((front * cosine + back * sine).astype(low), base, cols)
        store((back * cosine - front * sine).astype(low), base + half, cols)

    for index, cols in enumerate(unit_chunks(tokens)):
        keep = allowed_keys(code_ref[...], last_ref[:, cols], first_ref[:, cols])
        for head in range(group):
            rows = slice(head * dim, (head + 1) * dim)
            query_t, grad_t = flat[rows, cols], grad_flat[rows, cols]
            scores = mm(key_rows, query_t, ((1,), (0,))) * score_scale
            probs = jnp.where(keep, jnp.exp(scores - stat_ref[head : head + 1, cols]), 0.0)
            grad_probs = mm(value_rows, grad_t, ((1,), (0,)))
            delta = jnp.sum(probs * grad_probs, axis=0, keepdims=True)
            grad_scores = (probs * (grad_probs - delta)).astype(low)
            unturn(mm(key_t, grad_scores, ((1,), (0,))), head * dim, cols)
            key_part = mm(query_t, grad_scores, ((1,), (1,)))
            value_part = mm(grad_t, probs.astype(low), ((1,), (1,)))
            if index == 0 and head == 0:
                key_sum[...] = key_part
                value_sum[...] = value_part
            else:
                key_sum[...] += key_part
                value_sum[...] += value_part
    everything = slice(0, tokens)
    unturn(key_sum[...], group * dim, everything)
    store(value_sum[...].astype(low), (group + 1) * dim, everything)


MESH_ID = pl.DeviceIdType.MESH


class Sems:
    def __init__(self, send, recv):
        self.send, self.recv, self.used = send, recv, 0

    def take(self, count=1):
        base = self.used
        self.used += count
        return base


def remote(sems, index, source, target, there, arrive=None):
    return pltpu.make_async_remote_copy(
        src_ref=source,
        dst_ref=target,
        send_sem=sems.send.at[index],
        recv_sem=sems.recv.at[index if arrive is None else arrive],
        device_id=there,
        device_id_type=MESH_ID,
    )


def greet(chips, chip, core, tp):
    barrier = pltpu.get_barrier_semaphore()

    @pl.loop(1, chips)
    def _(step):
        pl.semaphore_signal(barrier, inc=1, device_id={"chip": (chip + step) % chips}, device_id_type=MESH_ID)

    pl.semaphore_signal(barrier, inc=1, device_id={"core": 1 - core}, device_id_type=MESH_ID)
    pl.semaphore_signal(barrier, inc=1, device_id={"tp": 1 - tp}, device_id_type=MESH_ID)
    pl.semaphore_wait(barrier, chips + 1)


def spot_of(chip, count):
    odd = chip % 2
    return (1 - odd) * (chip // 2) + odd * (count - 1 - chip // 2)


def chip_at(spot, count):
    spot = (spot + count) % count
    far = spot // (count // 2)
    return (1 - far) * 2 * spot + far * (2 * (count - 1 - spot) + 1)


class Ring:
    def __init__(self, sems, whole, rows, count, chip, saved, save_sem):
        self.sems, self.whole, self.rows, self.count = sems, whole, rows, count
        self.saved, self.save_sem = saved, save_sem
        self.spot = spot_of(chip, count)
        self.half = count // 2
        self.base = sems.take(2 * self.half)
        self.ways = (1, -1)

    def copy(self, side, hop, behind):
        way = self.ways[side]
        start = chip_at(self.spot - way * behind, self.count) * self.rows
        size = self.rows
        if hop == self.half:
            size = self.rows // 2
            start = start + side * size
        piece = self.whole.at[pl.ds(pl.multiple_of(start, 16), size), :]
        there = {"chip": chip_at(self.spot + way, self.count)}
        return remote(self.sems, self.base + side * self.half + hop - 1, piece, piece, there)

    def save(self, side, hop, behind):
        way = self.ways[side]
        start = chip_at(self.spot - way * behind, self.count) * self.rows
        size = self.rows
        if hop == self.half:
            size = self.rows // 2
            start = start + side * size
        if self.saved is None:
            return
        piece = pl.ds(pl.multiple_of(start, 16), size)
        pltpu.make_async_copy(self.whole.at[piece, :], self.saved.at[piece, :], self.save_sem).start()

    def start(self):
        for side in (0, 1):
            self.copy(side, 1, 0).start()
        self.save(0, 1, 0)

    def arrive(self):
        for side in (0, 1):
            self.copy(side, self.half, self.half).wait_recv()
            self.save(side, self.half, self.half)

    def relay(self, hop):
        for side in (0, 1):
            self.copy(side, hop - 1, hop - 1).wait_recv()
            self.copy(side, hop, hop - 1).start()
        for side in (0, 1):
            self.save(side, hop - 1, hop - 1)

    def saves_done(self):
        if self.saved is not None:
            pltpu.make_async_copy(self.whole, self.saved, self.save_sem).wait()

    def drain(self):
        for side in (0, 1):
            for hop in range(1, self.half + 1):
                self.copy(side, hop, hop - 1).wait_send()


class Spread:
    def __init__(self, sems, whole, micro, where):
        self.sems, self.whole, self.micro = sems, whole, micro
        _, self.core, self.tp = where
        self.rows = whole.shape[0] // (4 * micro)
        self.base = sems.take(3 * micro)

    def rows_of(self, m, half, core):
        return pl.ds(pl.multiple_of(((m * 2 + half) * 2 + core) * self.rows, 16), self.rows)

    def place(self, m, half, core):
        return self.whole.at[self.rows_of(m, half, core), :]

    def put(self, m, values):
        self.whole[self.rows_of(m, self.tp, self.core), :] = values

    def over_tp(self, m, half):
        piece = self.place(m, half, self.core)
        return remote(self.sems, self.base + m, piece, piece, {"tp": 1 - self.tp})

    def over_core(self, m, core):
        piece = self.place(m, self.tp, core)
        return remote(self.sems, self.base + self.micro + m, piece, piece, {"core": 1 - self.core})

    def passed_on(self, m, core):
        piece = self.place(m, 1 - self.tp, core)
        return remote(self.sems, self.base + 2 * self.micro + m, piece, piece, {"core": 1 - self.core})

    def start(self, m):
        self.over_tp(m, self.tp).start()
        self.over_core(m, self.core).start()

    def pass_on(self):
        for m in range(self.micro):
            self.over_tp(m, 1 - self.tp).wait_recv()
            self.passed_on(m, self.core).start()

    def finish(self):
        for m in range(self.micro):
            self.over_core(m, 1 - self.core).wait_recv()
            self.passed_on(m, 1 - self.core).wait_recv()

    def drain(self):
        for m in range(self.micro):
            self.over_tp(m, self.tp).wait_send()
            self.over_core(m, self.core).wait_send()
            self.passed_on(m, self.core).wait_send()


def turn_over(whole, turned):
    lanes = 256

    @pl.loop(0, whole.shape[1] // lanes)
    def _(part):
        columns = pl.ds(pl.multiple_of(part * lanes, 128), lanes)
        turned[columns, :] = whole[:, columns].astype(f32).T.astype(low)


def gain_row(gain_ref):
    return gain_ref[...].reshape(1, gain_ref.shape[0])


def half_blocks(front, back, which):
    lanes = front.shape[1]
    front, back = jnp.broadcast_to(front, (8, lanes)), jnp.broadcast_to(back, (8, lanes))
    front = jnp.where(which == 0, front, pltpu.roll(front, lanes // 2, 1))
    back = jnp.where(which == 0, pltpu.roll(back, lanes // 2, 1), back)
    return jnp.where(lax.broadcasted_iota(jnp.int32, (8, lanes), 1) < lanes // 2, front, back)[:1]


def angle_tables(spots, columns, cos_ref, sin_ref):
    place = lax.broadcasted_iota(jnp.int32, (HEAD_SIZE // 2, spots.shape[1]), 0).astype(f32)
    angles = jnp.exp(place * (-2.0 * math.log(rope_base) / HEAD_SIZE)) * spots.astype(f32)
    cos_ref[:, columns] = jnp.cos(angles)
    sin_ref[:, columns] = jnp.sin(angles)


def chip_line(ref, row, chip, which, toks):
    start = pl.multiple_of(chip * 2 * toks, 256)
    parts = []
    for at in (start, start + toks):
        lines = ref[:, pl.ds(at, toks)]
        line = lines[:1]
        for other in range(1, lines.shape[0]):
            line = jnp.where(row == other, lines[other : other + 1], line)
        parts.append(line)
    return half_blocks(*parts, which)


def unit_codes(seg_ref, pos_ref, code_ref, last_ref, start_ref, chips, chip, heads, tables=None):
    micro, half = chip // (2 * heads), chip // heads % 2
    toks = DOCUMENT_LIMIT // chips
    for source in range(chips):
        columns = slice(source * toks, (source + 1) * toks)
        spots = chip_line(pos_ref, micro, source, half, toks)
        first = (chip_line(seg_ref, micro, source, half, toks) * DOCUMENT_LIMIT).astype(f32)
        start_ref[:, columns] = first
        last_ref[:, columns] = first + spots.astype(f32)
        if tables is not None:
            angle_tables(spots, columns, *tables)
    code_ref[...] = jnp.broadcast_to(last_ref[...], (8, DOCUMENT_LIMIT)).T[:, :1]


class Fold:
    def __init__(self, sems, parts, from_core, to_tp, from_tp, micro, chip_core_tp):
        self.sems, self.parts, self.from_core, self.to_tp, self.from_tp = sems, parts, from_core, to_tp, from_tp
        self.micro = micro
        _, self.core, self.tp = chip_core_tp
        self.rows = from_tp.shape[0] // micro
        self.base = sems.take(3 * micro)

    def piece(self, m, half, core):
        start = ((m * 2 + half) * 2 + core) * self.rows
        return pl.ds(pl.multiple_of(start, 16), self.rows)

    def landing(self, m, half):
        return pl.ds(pl.multiple_of((m * 2 + half) * self.rows, 16), self.rows)

    def over_core(self, m, half):
        source = self.parts.at[self.piece(m, half, 1 - self.core), :]
        index = self.base + m * 2 + half
        return remote(self.sems, index, source, self.from_core.at[self.landing(m, half), :], {"core": 1 - self.core})

    def over_tp(self, m):
        rows = pl.ds(m * self.rows, self.rows)
        index = self.base + 2 * self.micro + m
        return remote(self.sems, index, self.to_tp.at[rows, :], self.from_tp.at[rows, :], {"tp": 1 - self.tp})

    def start(self, m, half):
        self.over_core(m, half).start()

    def summed(self, m, half):
        mine = self.parts[self.piece(m, half, self.core), :].astype(f32)
        return mine + self.from_core[self.landing(m, half), :].astype(f32)

    def send(self, m):
        for half in (0, 1):
            self.over_core(m, half).wait_recv()
        self.to_tp[m * self.rows : (m + 1) * self.rows, :] = self.summed(m, 1 - self.tp).astype(low)
        self.over_tp(m).start()

    def result(self, m):
        kept = self.summed(m, self.tp)
        self.over_tp(m).wait_recv()
        return kept + self.from_tp[m * self.rows : (m + 1) * self.rows, :].astype(f32)

    def drain(self):
        for m in range(self.micro):
            for half in (0, 1):
                self.over_core(m, half).wait_send()
            self.over_tp(m).wait_send()


class Exchange:
    def __init__(self, sems, outgoing, incoming, chips, chip):
        self.sems, self.outgoing, self.incoming, self.chips, self.chip = sems, outgoing, incoming, chips, chip
        self.base = sems.take(chips)

    def copy(self, to):
        return remote(
            self.sems, self.base + to, self.outgoing.at[to], self.incoming.at[self.chip], {"chip": to}, self.base + self.chip
        )

    def send(self, to):
        @pl.when(to != self.chip)
        def _():
            self.copy(to).start()

        @pl.when(to == self.chip)
        def _():
            self.incoming[to] = self.outgoing[to]

    def finish(self):
        @pl.loop(1, self.chips)
        def _(step):
            source = (self.chip + step) % self.chips
            remote(
                self.sems, self.base + source, self.outgoing.at[source], self.incoming.at[source], {"chip": source}
            ).wait_recv()

    def drain(self):
        @pl.loop(1, self.chips)
        def _(step):
            self.copy((self.chip + step) % self.chips).wait_send()


class Actions:
    def __init__(self, steps):
        self.steps = list(steps)

    def run(self, count=None):
        count = len(self.steps) if count is None else count
        for step in self.steps[:count]:
            step()
        self.steps = self.steps[count:]


def unit_sources(group, heads, head):
    queries = [(head * group + member) * HEAD_SIZE for member in range(group)]
    return queries + [(heads * group + head) * HEAD_SIZE, (heads * group + heads + head) * HEAD_SIZE]


def forward_kernel(
    micro, group, chips,
    x_ref, cot_ref, head_ref, out_ref, gate_ref, up_ref, down_ref, gain_one_ref, gain_two_ref, pos_ref, seg_ref,
    head_o, out_o, down_o, first_o, second_t_o, cot_t_o, unit_o, att_o, hidden_o, gate_back_o, up_back_o, second_o, stat_ref, residual_ref,
    head_w, out_w, gate_w, up_w, down_w, first_all, second_all, cot_all, first_t, second_t, cot_t, unit_send, unit_in, flat, att_send, att_in,
    parts, from_core, to_tp, from_tp, cos_ref, sin_ref, code_ref, last_ref, start_ref,
    gate_value, grad_hidden, hidden, gate_back, up_back, second_parts, send_sem, recv_sem, local_sem, save_sem,
):
    dim = HEAD_SIZE
    half = dim // 2
    chip, core, tp = lax.axis_index("chip"), lax.axis_index("core"), lax.axis_index("tp")
    where = (chip, core, tp)
    sems = Sems(send_sem, recv_sem)
    rows = x_ref.shape[0] // micro
    toks = 2 * rows
    unit_rows = (group + 2) * dim
    heads = head_w.shape[1] // unit_rows
    hops = chips // 2
    depth = head_ref.shape[0]
    greet(chips, chip, core, tp)

    weights = ((head_ref, head_w, head_o), (out_ref, out_w, out_o), (down_ref, down_w, down_o), (gate_ref, gate_w, None), (up_ref, up_w, None))
    rings, swaps, keeps = [], [], []
    for index, (shard, whole, saved) in enumerate(weights):
        columns = whole.shape[1]
        mine = whole.at[pl.ds(pl.multiple_of((chip * 2 + core) * depth, 16), depth), :]
        theirs = whole.at[pl.ds(pl.multiple_of((chip * 2 + 1 - core) * depth, 16), depth), :]
        at = sems.take()
        give = shard.at[:, pl.ds(pl.multiple_of((1 - core) * columns, 128), columns)]
        hold = shard.at[:, pl.ds(pl.multiple_of(core * columns, 128), columns)]
        swaps.append((remote(sems, at, give, mine, {"core": 1 - core}), remote(sems, at, give, theirs, {"core": 1 - core})))
        keeps.append(pltpu.make_async_copy(hold, mine, local_sem.at[index]))
        rings.append(Ring(sems, whole, 2 * depth, chips, chip, saved, save_sem.at[index]))
    first, second, cot = (Spread(sems, whole, micro, where) for whole in (first_all, second_all, cot_all))
    to_unit = Exchange(sems, unit_send, unit_in, chips, chip)
    from_unit = Exchange(sems, att_send, att_in, chips, chip)
    fold = Fold(sems, parts, from_core, to_tp, from_tp, micro, where)
    saves = []

    def save(source, target):
        saves.append(pltpu.make_async_copy(source, target, save_sem.at[5 + len(saves)]))
        saves[-1].start()

    for index in (0, 1):
        swaps[index][0].start()
        keeps[index].start()
    for m in range(micro):
        values = x_ref[m * rows : (m + 1) * rows, :].astype(f32)
        first.put(m, (values * norm_scale(values) * gain_row(gain_one_ref)).astype(low))
    for index in (2, 3, 4):
        swaps[index][0].start()
        keeps[index].start()
    for m in range(micro):
        cot.put(m, cot_ref[m * rows : (m + 1) * rows, :])
        first.start(m)
    head_ring, out_ring, down_ring, gate_ring, up_ring = rings
    for index in (0, 1):
        keeps[index].wait()
        swaps[index][1].wait_recv()
        rings[index].start()
    for m in range(micro):
        for side in (0, 1):
            columns = slice((m * 2 + side) * toks, (m * 2 + side + 1) * toks)
            angle_tables(chip_line(pos_ref, m, chip, side, toks), columns, cos_ref, sin_ref)
    first.pass_on()
    for hop in range(2, hops + 1):
        head_ring.relay(hop)
        out_ring.relay(hop)
    for index in (2, 3, 4):
        keeps[index].wait()
        swaps[index][1].wait_recv()
    down_ring.start()
    first.finish()
    head_ring.arrive()
    later = Actions(
        [ring.start for ring in (gate_ring, up_ring)]
        + [functools.partial(ring.relay, hop) for hop in range(2, hops + 1) for ring in (down_ring, gate_ring, up_ring)]
    )

    @pl.loop(0, micro * 2)
    def _(block):
        tokens = pl.ds(pl.multiple_of(block * toks, 128), toks)
        lines = mm(first_all[tokens, :], head_w[...], ((1,), (0,))).T
        cosine, sine = cos_ref[:, tokens], sin_ref[:, tokens]
        for head in range(heads):
            u = block * heads + head
            for turn, source in enumerate(unit_sources(group, heads, head)):
                front, back = lines[source : source + half], lines[source + half : source + dim]
                if turn < group + 1:
                    front, back = front * cosine - back * sine, back * cosine + front * sine
                unit_send[u, turn * dim : turn * dim + half, :] = front.astype(low)
                unit_send[u, turn * dim + half : (turn + 1) * dim, :] = back.astype(low)
            to_unit.send(u)

    later.run(1)
    for m in range(micro):
        cot.start(m)
    out_ring.arrive()
    unit_codes(seg_ref, pos_ref, code_ref, last_ref, start_ref, chips, chip, heads)
    later.run(2)
    cot.pass_on()
    to_unit.finish()

    score_scale = dim ** (-0.5)
    lay_out(unit_in, flat)
    save(unit_in, unit_o)
    key_rows = flat[group * dim : (group + 1) * dim, :].astype(f32).T.astype(low)
    lanes = 256

    @pl.loop(0, chips * toks // lanes)
    def _(number):
        cols = pl.ds(pl.multiple_of(number * lanes, 128), lanes)
        keep = allowed_keys(code_ref[...], last_ref[:, cols], start_ref[:, cols])
        for head in range(group):
            query_t = flat[head * dim : (head + 1) * dim, cols]
            scores = mm(key_rows, query_t, ((1,), (0,))) * score_scale
            scores = jnp.where(keep, scores, masked_score)
            maximum = jnp.max(scores, axis=0, keepdims=True)
            exponents = jnp.exp(scores - maximum)
            totals = jnp.sum(exponents, axis=0, keepdims=True)
            probs = (exponents * (1.0 / totals)).astype(low)
            stat_ref[head : head + 1, cols] = maximum + jnp.log(totals)
            result = mm(flat[(group + 1) * dim :, :], probs, ((1,), (0,))).astype(low)
            for piece in range(lanes // toks):
                here = result[:, piece * toks : (piece + 1) * toks]
                att_send[number * (lanes // toks) + piece, head * dim : (head + 1) * dim, :] = here
        for piece in range(lanes // toks):
            from_unit.send(number * (lanes // toks) + piece)

        @pl.when(number == 1)
        def _():
            later.run(1)

    later.run(1)
    cot.finish()
    turn_over(cot_all, cot_t)
    save(cot_t, cot_t_o)
    turn_over(first_all, first_t)
    save(first_t, first_o)
    from_unit.finish()
    save(att_in, att_o)

    @pl.loop(0, micro * 2)
    def _(block):
        lines = jnp.concatenate([att_in[block * heads + head] for head in range(heads)], axis=0)
        lines = lines.astype(f32).T.astype(low)
        sums = mm(lines, out_w[...], ((1,), (1,)))
        parts[pl.ds(pl.multiple_of(block * toks, 128), toks), :] = sums.astype(low)
        fold.start(block // 2, block % 2)

    for m in range(micro):
        fold.send(m)
    later.run(1)
    for m in range(micro):
        own = slice(m * rows, (m + 1) * rows)
        residual = x_ref[own, :].astype(f32) + fold.result(m)
        residual_ref[own, :] = residual
        second.put(m, (residual * norm_scale(residual) * gain_row(gain_two_ref)).astype(low))
        second.start(m)
    later.run(2)
    second.pass_on()
    second.finish()
    turn_over(second_all, second_t)
    save(second_t, second_t_o)
    later.run()

    lanes = 256
    hidden_blocks = gate_w.shape[1] // lanes

    def block_of(part):
        return pl.ds(pl.multiple_of(part * lanes, 128), lanes)

    down_ring.arrive()

    @pl.loop(0, hidden_blocks)
    def _(part):
        cols = block_of(part)
        grad_hidden[:, cols] = mm(cot_all[...], down_w[:, cols], ((1,), (0,)))

    gate_ring.arrive()

    @pl.loop(0, hidden_blocks)
    def _(part):
        cols = block_of(part)
        gate_value[:, cols] = mm(second_all[...], gate_w[:, cols], ((1,), (0,)))

    up_ring.arrive()

    @pl.loop(0, hidden_blocks)
    def _(part):
        cols = block_of(part)
        upward = mm(second_all[...], up_w[:, cols], ((1,), (0,)))
        value, grads = gate_value[:, cols], grad_hidden[:, cols]
        sigma = 1.0 / (1.0 + jnp.exp(-value))
        active = value * sigma
        hidden[:, cols] = (active * upward).astype(low)
        gate_back[:, cols] = (grads * upward * (sigma * (1.0 + value * (1.0 - sigma)))).astype(low)
        up_back[:, cols] = (grads * active).astype(low)

    save(hidden, hidden_o)
    save(gate_back, gate_back_o)
    save(up_back, up_back_o)

    @pl.loop(0, second_parts.shape[1] // lanes)
    def _(part):
        cols = block_of(part)
        sums = mm(gate_back[...], gate_w[cols, :], ((1,), (1,))) + mm(up_back[...], up_w[cols, :], ((1,), (1,)))
        second_parts[:, cols] = sums.astype(low)

    save(second_parts, second_o)
    for part in saves:
        part.wait()
    for ring in rings:
        ring.saves_done()
    for swap, _ in swaps:
        swap.wait_send()
    for part in rings + [first, second, cot, to_unit, from_unit, fold]:
        part.drain()


def forward_call(micro, group, chips, heads, *operands):
    x, _, head_s, out_s, gate_s, up_s, down_s = operands[:7]
    own_rows, width = x.shape
    toks = own_rows // micro * 2
    all_rows = own_rows * 4
    pieces = micro * 2 * heads
    unit_rows, att_rows = (group + 2) * HEAD_SIZE, group * HEAD_SIZE
    shape = jax.ShapeDtypeStruct
    columns = [s.shape[1] // CORES for s in (head_s, out_s, gate_s, up_s, down_s)]
    any_spec, vmem_spec = pl.BlockSpec(memory_space=pl.ANY), pl.BlockSpec(memory_space=pltpu.VMEM)
    hidden = columns[-1]
    any_outs = [shape((width, c), low) for c in (columns[0], columns[1], hidden)] + [shape((width, all_rows), low)] * 3
    any_outs += [shape((pieces, unit_rows, toks), low), shape((pieces, att_rows, toks), low)]
    any_outs += [shape((all_rows, hidden), low)] * 3 + [shape((all_rows, width), low)]
    vmem_outs = [shape((group, DOCUMENT_LIMIT), f32), shape((own_rows, width), f32)]
    scratch = [pltpu.VMEM((width, c), low) for c in columns]
    scratch += [pltpu.VMEM((all_rows, width), low)] * 3 + [pltpu.VMEM((width, all_rows), low)] * 3
    scratch += [
        pltpu.VMEM((pieces, unit_rows, toks), low),
        pltpu.VMEM((pieces, unit_rows, toks), low),
        pltpu.VMEM((unit_rows, DOCUMENT_LIMIT), low),
        pltpu.VMEM((pieces, att_rows, toks), low),
        pltpu.VMEM((pieces, att_rows, toks), low),
        pltpu.VMEM((all_rows, width), low),
        pltpu.VMEM((all_rows // 2, width), low),
        pltpu.VMEM((own_rows, width), low),
        pltpu.VMEM((own_rows, width), low),
        pltpu.VMEM((HEAD_SIZE // 2, all_rows), f32),
        pltpu.VMEM((HEAD_SIZE // 2, all_rows), f32),
        pltpu.VMEM((DOCUMENT_LIMIT, 1), f32),
        pltpu.VMEM((1, DOCUMENT_LIMIT), f32),
        pltpu.VMEM((1, DOCUMENT_LIMIT), f32),
        pltpu.VMEM((all_rows, hidden), f32),
        pltpu.VMEM((all_rows, hidden), f32),
        pltpu.VMEM((all_rows, hidden), low),
        pltpu.VMEM((all_rows, hidden), low),
        pltpu.VMEM((all_rows, hidden), low),
        pltpu.VMEM((all_rows, width), low),
        pltpu.SemaphoreType.DMA((96,)),
        pltpu.SemaphoreType.DMA((96,)),
        pltpu.SemaphoreType.DMA((5,)),
        pltpu.SemaphoreType.DMA((16,)),
    ]
    return pl.pallas_call(
        functools.partial(forward_kernel, micro, group, chips),
        out_shape=tuple(any_outs + vmem_outs),
        in_specs=[vmem_spec] * 2 + [any_spec] * 5 + [vmem_spec] * (len(operands) - 7),
        out_specs=tuple([any_spec] * len(any_outs) + [vmem_spec] * len(vmem_outs)),
        scratch_shapes=scratch,
        compiler_params=pltpu.CompilerParams(collective_id=0, has_side_effects=True, vmem_limit_bytes=60 << 20),
    )(*operands)


class RingSum:
    def __init__(self, sems, make, far, slots, count, chip, core):
        self.sems, self.make, self.far, self.slots, self.count, self.chip, self.core = sems, make, far, slots, count, chip, core
        self.rows = far.shape[0]
        self.spot = spot_of(chip, count)
        self.half = count // 2
        self.base = sems.take(2 * self.half)
        self.ways = (1, -1)

    def slot(self, side, hop):
        return (side * self.half + hop - 1) * self.rows

    def term(self, side, distance):
        return chip_at(self.spot + self.ways[side] * distance, self.count) * self.rows

    def copy(self, side, hop):
        there = {"chip": chip_at(self.spot + self.ways[side], self.count)}
        index = self.base + side * self.half + hop - 1
        if hop == 1:
            size = self.rows // 2
            source = self.far.at[side * size : (side + 1) * size, :]
            target = self.slots.at[pl.ds(self.slot(side, 1) + side * size, size), :]
        else:
            source = self.slots.at[pl.ds(self.slot(side, hop - 1), self.rows), :]
            target = self.slots.at[pl.ds(self.slot(side, hop), self.rows), :]
        return remote(self.sems, index, source, target, there)

    def start(self):
        self.far[...] = self.make((self.term(0, self.half),), self.rows).astype(low)
        for side in (0, 1):
            self.copy(side, 1).start()

    def relay(self, hop):
        size = self.rows // 2
        own = self.make([self.term(side, self.half - hop + 1) for side in (0, 1)], self.rows)
        for side in (0, 1):
            self.copy(side, hop - 1).wait_recv()
            at = self.slot(side, hop - 1)
            for part in (0, 1):
                here = pl.ds(at + part * size, size)
                mine = own[side * self.rows + part * size : side * self.rows + (part + 1) * size]
                if hop == 2 and part != side:
                    self.slots[here, :] = mine.astype(low)
                else:
                    self.slots[here, :] = (mine + self.slots[here, :].astype(f32)).astype(low)
            self.copy(side, hop).start()

    def result(self):
        size = self.rows // 2
        offsets = [self.core * size, (1 - self.core) * size]
        own = self.make([self.chip * self.rows + offset for offset in offsets], size)
        for side in (0, 1):
            self.copy(side, self.half).wait_recv()
        sums = []
        for index, offset in enumerate(offsets):
            total = own[index * size : (index + 1) * size]
            for side in (0, 1):
                here = pl.ds(pl.multiple_of(self.slot(side, self.half) + offset, 16), size)
                total = total + self.slots[here, :].astype(f32)
            sums.append(total)
        return sums

    def drain(self):
        for side in (0, 1):
            for hop in range(1, self.half + 1):
                self.copy(side, hop).wait_send()


def rows_from(ref, starts, size):
    blocks = [ref[pl.ds(pl.multiple_of(start, 16), size), :] for start in starts]
    return blocks[0] if len(blocks) == 1 else jnp.concatenate(blocks, axis=0)


class Merge:
    def __init__(self, sems, ring, leaving, landing, out, core):
        self.sems, self.ring, self.leaving, self.landing, self.out, self.core = sems, ring, leaving, landing, out, core
        self.index = sems.take()

    def copy(self):
        return remote(self.sems, self.index, self.leaving, self.landing, {"core": 1 - self.core})

    def send(self):
        kept, sent = self.ring.result()
        self.leaving[...] = sent.astype(low)
        self.copy().start()
        columns = self.leaving.shape[1]
        self.out[:, pl.ds(pl.multiple_of(self.core * columns, 128), columns)] = kept

    def finish(self):
        columns = self.leaving.shape[1]
        self.copy().wait_recv()
        self.out[:, pl.ds(pl.multiple_of((1 - self.core) * columns, 128), columns)] = self.landing[...].astype(f32)

    def drain(self):
        self.copy().wait_send()


class Butterfly:
    def __init__(self, sems, leaving, landing, chips, where):
        self.sems, self.leaving, self.landing = sems, leaving, landing
        chip, core, tp = where
        self.partners = [{"tp": 1 - tp}, {"core": 1 - core}]
        step = 1
        while step < chips:
            self.partners.append({"chip": chip + step - 2 * step * (chip // step % 2)})
            step *= 2
        self.base = sems.take(len(self.partners))

    def copy(self, stage):
        return remote(self.sems, self.base + stage, self.leaving.at[stage], self.landing.at[stage], self.partners[stage])

    def start(self, values):
        self.leaving[0] = values
        self.copy(0).start()

    def step(self, stage):
        self.copy(stage).wait_recv()
        values = self.leaving[stage] + self.landing[stage]
        if stage + 1 < len(self.partners):
            self.leaving[stage + 1] = values
            self.copy(stage + 1).start()
        return values

    def drain(self):
        for stage in range(len(self.partners)):
            self.copy(stage).wait_send()


def backward_kernel(
    micro, group, chips,
    x_ref, residual_ref, cot_ref, gain_one_ref, gain_two_ref, stat_ref, pos_ref, seg_ref,
    second_h, cot_t_h, hidden_h, second_t_h, gate_back_h, up_back_h, unit_h, att_h, down_h, out_h, first_t_h, head_h,
    output_ref, input_grad_ref, head_g, out_g, gate_g, up_g, down_g, gain_one_g, gain_two_g,
    second_parts, cot_t, hidden, second_t, gate_back, up_back, unit_ref, att_ref, down_w, out_w, first_t, head_w,
    core_a, to_tp_a, from_tp_a, core_b, to_tp_b, from_tp_b, core_c, to_tp_c, from_tp_c, grad_residual, grad_all, output_parts, first_parts,
    grad_send, grad_in, flat, grad_flat, key_sum, value_sum, back_send, back_in, att_flat, back_flat, out_terms,
    cos_ref, sin_ref, code_ref, last_ref, start_ref,
    head_far, out_far, down_far, gate_far, up_far, head_slots, out_slots, down_slots, gate_slots, up_slots,
    head_leave, out_leave, down_leave, gate_leave, up_leave, head_land, out_land, down_land, gate_land, up_land,
    gain_leave, gain_land, send_sem, recv_sem, local_sem,
):
    dim = HEAD_SIZE
    half = dim // 2
    chip, core, tp = lax.axis_index("chip"), lax.axis_index("core"), lax.axis_index("tp")
    where = (chip, core, tp)
    sems = Sems(send_sem, recv_sem)
    rows = x_ref.shape[0] // micro
    toks = 2 * rows
    unit_rows = (group + 2) * dim
    heads = head_w.shape[1] // unit_rows
    blocks = micro * 2
    hops = chips // 2
    sources = (second_h, cot_t_h, hidden_h, second_t_h, gate_back_h, up_back_h, unit_h, att_h, down_h, out_h, first_t_h, head_h)
    places = (second_parts, cot_t, hidden, second_t, gate_back, up_back, unit_ref, att_ref, down_w, out_w, first_t, head_w)
    loads = [pltpu.make_async_copy(a, b, local_sem.at[i]) for i, (a, b) in enumerate(zip(sources, places))]
    for load in loads:
        load.start()
    greet(chips, chip, core, tp)

    def ring_of_products(left, right, far, slots):
        make = lambda starts, size: mm(rows_from(left, starts, size), right[...], ((1,), (0,)))
        return RingSum(sems, make, far, slots, chips, chip, core)

    down_ring = ring_of_products(cot_t, hidden, down_far, down_slots)
    gate_ring = ring_of_products(second_t, gate_back, gate_far, gate_slots)
    up_ring = ring_of_products(second_t, up_back, up_far, up_slots)
    out_ring = RingSum(sems, lambda starts, size: rows_from(out_terms, starts, size).astype(f32), out_far, out_slots, chips, chip, core)
    head_ring = RingSum(
        sems, lambda starts, size: mm(rows_from(first_t, starts, size), back_flat[...], ((1,), (1,))), head_far, head_slots, chips, chip, core
    )
    down_merge, gate_merge, up_merge, out_merge, head_merge = (
        Merge(sems, down_ring, down_leave, down_land, down_g, core),
        Merge(sems, gate_ring, gate_leave, gate_land, gate_g, core),
        Merge(sems, up_ring, up_leave, up_land, up_g, core),
        Merge(sems, out_ring, out_leave, out_land, out_g, core),
        Merge(sems, head_ring, head_leave, head_land, head_g, core),
    )
    second_fold = Fold(sems, second_parts, core_a, to_tp_a, from_tp_a, micro, where)
    output_fold = Fold(sems, output_parts, core_b, to_tp_b, from_tp_b, micro, where)
    first_fold = Fold(sems, first_parts, core_c, to_tp_c, from_tp_c, micro, where)
    spread = Spread(sems, grad_all, micro, where)
    to_unit = Exchange(sems, grad_send, grad_in, chips, chip)
    from_unit = Exchange(sems, back_send, back_in, chips, chip)
    butterfly = Butterfly(sems, gain_leave, gain_land, chips, where)
    later = Actions([functools.partial(ring.relay, hop) for hop in range(2, hops + 1) for ring in (down_ring, gate_ring, up_ring)])

    loads[0].wait()
    for m in range(micro):
        for side in (0, 1):
            second_fold.start(m, side)
    for load in loads[1:3]:
        load.wait()
    down_ring.start()
    for m in range(micro):
        second_fold.send(m)
    for load in loads[3:6]:
        load.wait()
    gate_ring.start()
    up_ring.start()

    def norm_rows_back(values, gain, grads):
        rho = norm_scale(values)
        scaled = grads * gain
        inner = jnp.mean(scaled * values, axis=-1, keepdims=True)
        return rho * scaled - values * (rho * rho * rho * inner), jnp.sum(grads * values * rho, axis=0, keepdims=True)

    later.run(1)
    gain_two = None
    for m in range(micro):
        own = slice(m * rows, (m + 1) * rows)
        part, gain_now = norm_rows_back(residual_ref[own, :], gain_row(gain_two_ref), second_fold.result(m))
        gain_two = gain_now if gain_two is None else gain_two + gain_now
        grads = cot_ref[own, :].astype(f32) + part
        grad_residual[own, :] = grads
        spread.put(m, grads.astype(low))
        spread.start(m)
    for load in loads[6:8]:
        load.wait()
    lay_out(unit_ref, flat)
    for piece in range(blocks * heads):
        block, head = piece // heads, piece % heads
        att_flat[head * group * dim : (head + 1) * group * dim, block * toks : (block + 1) * toks] = att_ref[piece]
    key_t = flat[group * dim : (group + 1) * dim, :]
    key_rows = key_t.astype(f32).T.astype(low)
    value_rows = flat[(group + 1) * dim :, :].astype(f32).T.astype(low)
    unit_codes(seg_ref, pos_ref, code_ref, last_ref, start_ref, chips, chip, heads, (cos_ref, sin_ref))
    later.run(1)
    spread.pass_on()
    for load in loads[8:10]:
        load.wait()
    later.run(1)
    spread.finish()

    @pl.loop(0, blocks)
    def _(block):
        tokens = pl.ds(pl.multiple_of(block * toks, 128), toks)
        lines = mm(grad_all[tokens, :], out_w[...], ((1,), (0,))).T.astype(low)
        for head in range(heads):
            piece = block * heads + head
            grad_send[piece] = lines[head * group * dim : (head + 1) * group * dim]
            to_unit.send(piece)

    later.run(1)

    @pl.loop(0, blocks)
    def _(block):
        tokens = pl.ds(pl.multiple_of(block * toks, 128), toks)
        output_parts[tokens, :] = mm(hidden[tokens, :], down_w[...], ((1,), (1,))).astype(low)
        output_fold.start(block // 2, block % 2)

    lanes = 256

    @pl.loop(0, grad_all.shape[1] // lanes)
    def _(part):
        columns = pl.ds(pl.multiple_of(part * lanes, 128), lanes)
        out_terms[columns, :] = mm(att_flat[...], grad_all[:, columns], ((1,), (0,))).T.astype(low)

    out_ring.start()
    later.run(1)
    for m in range(micro):
        output_fold.send(m)
    to_unit.finish()
    lay_out(grad_in, grad_flat)

    score_scale = dim ** (-0.5)
    tokens_all = chips * toks
    key_sum[...] = jnp.zeros_like(key_sum)
    value_sum[...] = jnp.zeros_like(value_sum)

    def store(values, base, first_piece):
        for piece in range(values.shape[1] // toks):
            back_send[first_piece + piece, base : base + values.shape[0], :] = values[:, piece * toks : (piece + 1) * toks]

    def unturn(values, base, cols, first_piece):
        front, back = values[:half] * score_scale, values[half:] * score_scale
        cosine, sine = cos_ref[:, cols], sin_ref[:, cols]
        store((front * cosine + back * sine).astype(low), base, first_piece)
        store((back * cosine - front * sine).astype(low), base + half, first_piece)

    @pl.loop(0, tokens_all // lanes)
    def _(number):
        cols = pl.ds(pl.multiple_of(number * lanes, 128), lanes)
        keep = allowed_keys(code_ref[...], last_ref[:, cols], start_ref[:, cols])
        for head in range(group):
            lines = slice(head * dim, (head + 1) * dim)
            query_t, grad_t = flat[lines, cols], grad_flat[lines, cols]
            scores = mm(key_rows, query_t, ((1,), (0,))) * score_scale
            probs = jnp.where(keep, jnp.exp(scores - stat_ref[head : head + 1, cols]), 0.0)
            grad_probs = mm(value_rows, grad_t, ((1,), (0,)))
            delta = jnp.sum(probs * grad_probs, axis=0, keepdims=True)
            grad_scores = (probs * (grad_probs - delta)).astype(low)
            unturn(mm(key_t, grad_scores, ((1,), (0,))), head * dim, cols, number * (lanes // toks))
            key_sum[...] += mm(query_t, grad_scores, ((1,), (1,)))
            value_sum[...] += mm(grad_t, probs.astype(low), ((1,), (1,)))

        @pl.when(number == 1)
        def _():
            later.run(1)

    unturn(key_sum[...], group * dim, slice(0, tokens_all), 0)
    store(value_sum[...].astype(low), (group + 1) * dim, 0)

    @pl.loop(0, chips)
    def _(piece):
        from_unit.send(piece)

    later.run(1)
    for m in range(micro):
        own = slice(m * rows, (m + 1) * rows)
        output_ref[own, :] = (residual_ref[own, :] + output_fold.result(m)).astype(low)
    later.run(1)
    for load in loads[10:]:
        load.wait()
    from_unit.finish()

    for block in range(blocks):
        for head in range(heads):
            for turn, target in enumerate(unit_sources(group, heads, head)):
                piece = back_in[block * heads + head, turn * dim : (turn + 1) * dim, :]
                back_flat[target : target + dim, block * toks : (block + 1) * toks] = piece
    head_ring.start()

    @pl.loop(0, blocks)
    def _(block):
        tokens = pl.ds(pl.multiple_of(block * toks, 128), toks)
        lines = back_flat[:, tokens].astype(f32).T.astype(low)
        first_parts[tokens, :] = mm(lines, head_w[...], ((1,), (1,))).astype(low)
        first_fold.start(block // 2, block % 2)

    later.run(1)
    head_ring.relay(2)
    for m in range(micro):
        first_fold.send(m)
    later.run()
    out_ring.relay(2)
    down_merge.send()
    head_ring.relay(3)
    out_ring.relay(3)
    gain_one = None
    for m in range(micro):
        own = slice(m * rows, (m + 1) * rows)
        part, gain_now = norm_rows_back(x_ref[own, :].astype(f32), gain_row(gain_one_ref), first_fold.result(m))
        gain_one = gain_now if gain_one is None else gain_one + gain_now
        input_grad_ref[own, :] = (grad_residual[own, :] + part).astype(low)
    butterfly.start(jnp.concatenate([gain_one, gain_two], axis=0))
    head_ring.relay(4)
    out_ring.relay(4)
    butterfly.step(0)
    gate_merge.send()
    butterfly.step(1)
    up_merge.send()
    butterfly.step(2)
    down_merge.finish()
    gate_merge.finish()
    for stage in range(3, len(butterfly.partners) - 1):
        butterfly.step(stage)
    out_merge.send()
    head_merge.send()
    up_merge.finish()
    gain_sums = butterfly.step(len(butterfly.partners) - 1)
    gain_one_g[...] = gain_sums[0]
    gain_two_g[...] = gain_sums[1]
    out_merge.finish()
    head_merge.finish()
    parts = [down_ring, gate_ring, up_ring, out_ring, head_ring, down_merge, gate_merge, up_merge, out_merge, head_merge]
    parts += [second_fold, output_fold, first_fold, spread, to_unit, from_unit, butterfly]
    for part in parts:
        part.drain()


def backward_call(micro, group, chips, heads, near, *far):
    own_rows, width = near[0].shape
    toks = own_rows // micro * 2
    all_rows = own_rows * 4
    pieces = micro * 2 * heads
    unit_rows, att_rows = (group + 2) * HEAD_SIZE, group * HEAD_SIZE
    shape = jax.ShapeDtypeStruct
    hidden = far[2].shape[1]
    depth = width // chips
    columns = [heads * unit_rows, heads * att_rows, hidden, hidden, hidden]
    stages = 2 + (chips - 1).bit_length()
    any_spec, vmem_spec = pl.BlockSpec(memory_space=pl.ANY), pl.BlockSpec(memory_space=pltpu.VMEM)
    outs = [shape((own_rows, width), low)] * 2 + [shape((depth // 2, 2 * c), f32) for c in columns] + [shape((width,), f32)] * 2
    scratch = [pltpu.VMEM(a.shape, a.dtype) for a in far]
    scratch += [pltpu.VMEM((all_rows // 2, width), low), pltpu.VMEM((own_rows, width), low), pltpu.VMEM((own_rows, width), low)] * 3
    scratch += [
        pltpu.VMEM((own_rows, width), f32),
        pltpu.VMEM((all_rows, width), low),
        pltpu.VMEM((all_rows, width), low),
        pltpu.VMEM((all_rows, width), low),
        pltpu.VMEM((pieces, att_rows, toks), low),
        pltpu.VMEM((pieces, att_rows, toks), low),
        pltpu.VMEM((unit_rows, DOCUMENT_LIMIT), low),
        pltpu.VMEM((att_rows, DOCUMENT_LIMIT), low),
        pltpu.VMEM((HEAD_SIZE, DOCUMENT_LIMIT), f32),
        pltpu.VMEM((HEAD_SIZE, DOCUMENT_LIMIT), f32),
        pltpu.VMEM((pieces, unit_rows, toks), low),
        pltpu.VMEM((pieces, unit_rows, toks), low),
        pltpu.VMEM((heads * att_rows, all_rows), low),
        pltpu.VMEM((heads * unit_rows, all_rows), low),
        pltpu.VMEM((width, heads * att_rows), low),
        pltpu.VMEM((HEAD_SIZE // 2, DOCUMENT_LIMIT), f32),
        pltpu.VMEM((HEAD_SIZE // 2, DOCUMENT_LIMIT), f32),
        pltpu.VMEM((DOCUMENT_LIMIT, 1), f32),
        pltpu.VMEM((1, DOCUMENT_LIMIT), f32),
        pltpu.VMEM((1, DOCUMENT_LIMIT), f32),
    ]
    scratch += [pltpu.VMEM((depth, c), low) for c in columns]
    scratch += [pltpu.VMEM((chips * depth, c), low) for c in columns]
    scratch += [pltpu.VMEM((depth // 2, c), low) for c in columns] * 2
    scratch += [pltpu.VMEM((stages, 2, width), f32)] * 2
    scratch += [pltpu.SemaphoreType.DMA((128,))] * 2 + [pltpu.SemaphoreType.DMA((len(far),))]
    return pl.pallas_call(
        functools.partial(backward_kernel, micro, group, chips),
        out_shape=tuple(outs),
        in_specs=[vmem_spec] * len(near) + [any_spec] * len(far),
        out_specs=tuple([vmem_spec] * len(outs)),
        scratch_shapes=scratch,
        compiler_params=pltpu.CompilerParams(collective_id=1, has_side_effects=True, vmem_limit_bytes=63 << 20),
    )(*near, *far)


def vmem_call(kernel, outs, scratch, flops, *operands):
    spec = pl.BlockSpec(memory_space=pltpu.VMEM)
    moved = sum(math.prod(a.shape) * a.dtype.itemsize for a in operands + tuple(outs))
    return pl.pallas_call(
        kernel,
        out_shape=tuple(outs),
        in_specs=[spec] * len(operands),
        out_specs=tuple([spec] * len(outs)),
        scratch_shapes=scratch,
        cost_estimate=pl.CostEstimate(flops=flops, bytes_accessed=moved, transcendentals=2 * DOCUMENT_LIMIT**2),
        compiler_params=pltpu.CompilerParams(vmem_limit_bytes=48 << 20),
    )(*operands)


def on_device(
    block_input,
    segments,
    positions,
    query_weight,
    key_matrix,
    value_matrix,
    out_weight,
    gate_weight,
    up_weight,
    down_weight,
    gain_first,
    gain_second,
    cotangent,
):
    chips, tp_count = lax.axis_size("chip"), lax.axis_size("tp")
    chip, core = lax.axis_index("chip"), lax.axis_index("core")
    cp_count, cp_index = chips * CORES, chip * CORES + core
    micro, tok_dev, width = block_input.shape
    dim = HEAD_SIZE
    block_rows = tok_dev * tp_count // 2
    query_heads, value_heads = query_weight.shape[1] // dim, key_matrix.shape[1] // dim
    group = query_heads // value_heads
    unit_rows = (group + 2) * dim
    head_cores = CORES if value_heads % CORES == 0 else 1
    heads = value_heads // head_cores
    toks = head_cores * block_rows
    pieces = DOCUMENT_LIMIT // toks
    assert pieces == micro * 2 * heads and cp_count % (pieces * head_cores) == 0

    out_t, down_t = out_weight.T, down_weight.T

    def halves(matrix):
        half = matrix.shape[1] // 2
        return matrix[:, :half], matrix[:, half:]

    def gather_head_weight(matrix):
        if head_cores == 2:
            return ring_gather(core_split(*halves(matrix)))
        return lax.all_gather(matrix, ("chip", "core"), axis=0, tiled=True)

    def scatter_head_weight(grads):
        if head_cores == 2:
            return jnp.concatenate(core_merge(ring_scatter(grads)), axis=1)
        return lax.psum_scatter(grads, ("chip", "core"), scatter_dimension=0, tiled=True).astype(f32)

    fused = tp_count == 2 and head_cores == CORES and pieces == chips and toks == 128
    if fused:
        cores = []
        for part in range(CORES):
            columns = lambda matrix: matrix[:, part * matrix.shape[1] // CORES : (part + 1) * matrix.shape[1] // CORES]
            cores += [columns(query_weight), columns(key_matrix), columns(value_matrix)]
        by_head = jnp.concatenate(cores, axis=1)
    else:
        by_head = jnp.concatenate(
            [
                query_weight.reshape(-1, value_heads, group * dim),
                key_matrix.reshape(-1, value_heads, dim),
                value_matrix.reshape(-1, value_heads, dim),
            ],
            axis=2,
        ).reshape(query_weight.shape[0], -1)
        head_full = gather_head_weight(by_head)
        out_full = gather_head_weight(out_t)
        gate_full = ring_gather(core_split(*halves(gate_weight)))
        up_full = ring_gather(core_split(*halves(up_weight)))
        down_full = ring_gather(core_split(*halves(down_t)))

    by_block = lambda line: line.reshape(micro, cp_count, 2, block_rows)
    group_cp = pieces * head_cores
    first_cp = cp_index // head_cores * head_cores
    if not fused:
        row_pos = lax.dynamic_slice_in_dim(by_block(positions), first_cp, head_cores, 1)
        row_pos = row_pos.transpose(0, 2, 1, 3).reshape(-1)
        unit_index = cp_index // head_cores % pieces
        unit_micro, unit_half = unit_index // (2 * heads), unit_index // heads % 2

        def unit_line(line):
            mine = lax.dynamic_slice(
                by_block(line),
                (unit_micro, cp_index // group_cp * group_cp, unit_half, 0),
                (1, group_cp, 1, block_rows),
            )
            return mine.reshape(1, DOCUMENT_LIMIT)

        unit_pos, unit_seg = unit_line(positions), unit_line(segments)
        first_code = unit_seg * DOCUMENT_LIMIT
        last_code = first_code + unit_pos
        code_column = last_code.reshape(DOCUMENT_LIMIT, 1)
        cosine, sine = angles_of(row_pos)
        unit_cosine, unit_sine = angles_of(unit_pos.reshape(-1))

    if head_cores == 2:
        exchange_axis = "chip"
        groups = [[g + i for i in range(pieces)] for g in range(0, chips, pieces)]
    else:
        exchange_axis = ("chip", "core")
        groups = [[g + i for i in range(pieces)] for g in range(0, cp_count, pieces)]
    groups = None if len(groups) == 1 else groups

    def exchange(values):
        return lax.all_to_all(values, exchange_axis, 0, 0, axis_index_groups=groups)

    def to_units(values):
        rows = values.shape[0] // heads
        return values.reshape(heads, rows, micro * 2, toks).transpose(2, 0, 1, 3).reshape(pieces, rows, toks)

    def from_units(values):
        rows = values.shape[1]
        return values.reshape(micro * 2, heads, rows, toks).transpose(1, 2, 0, 3).reshape(heads * rows, -1)

    gather_head_rows = functools.partial(gather_rows, micro_count=micro, cores=head_cores)
    scatter_head_rows = functools.partial(scatter_rows, micro_count=micro, cores=head_cores)
    gather_all_rows = functools.partial(gather_rows, micro_count=micro, cores=CORES)
    scatter_all_rows = functools.partial(scatter_rows, micro_count=micro, cores=CORES)

    own_input = block_input.reshape(-1, width).astype(f32)
    cot_own = cotangent.reshape(-1, width)
    square = DOCUMENT_LIMIT * DOCUMENT_LIMIT * dim * 2 * group
    own_rows = block_input.reshape(-1, width)
    if fused:
        facts = (gain_first, gain_second, positions, segments)
        head_full, out_full, down_full, first_t, second_t, cot_t, unit, att_pieces, hidden, gate_back, up_back, second_parts, unit_stat, residual = (
            forward_call(micro, group, chips, heads, own_rows, cot_own, by_head, out_t, gate_weight, up_weight, down_t, *facts)
        )
        output_rows, input_grad, head_grad, out_grad, gate_grad, up_grad, down_grad, *gain_sums = backward_call(
            micro, group, chips, heads,
            (own_rows, residual, cot_own, gain_first, gain_second, unit_stat, positions, segments),
            second_parts, cot_t, hidden, second_t, gate_back, up_back, unit, att_pieces, down_full, out_full, first_t, head_full,
        )
    else:
        first_rows = gather_head_rows((own_input * norm_scale(own_input) * gain_first).astype(low))
        projected = mm(head_full, first_rows, ((0,), (1,))).reshape(heads, unit_rows, -1)
        turned = projected[:, : (group + 1) * dim].reshape(heads, group + 1, 2, dim // 2, -1)
        front, back = turned[:, :, 0], turned[:, :, 1]
        turned = jnp.stack([front * cosine - back * sine, back * cosine + front * sine], axis=2)
        projected = jnp.concatenate(
            [turned.reshape(heads, (group + 1) * dim, -1).astype(low), projected[:, (group + 1) * dim :].astype(low)], axis=1
        )
        unit = exchange(to_units(projected.reshape(heads * unit_rows, -1)))
        unit_out, unit_stat = vmem_call(
            functools.partial(attend_kernel, group),
            (
                jax.ShapeDtypeStruct((pieces, group * dim, toks), low),
                jax.ShapeDtypeStruct((group, DOCUMENT_LIMIT), f32),
            ),
            [pltpu.VMEM((unit_rows, DOCUMENT_LIMIT), low)],
            2 * square,
            unit,
            code_column,
            last_code,
            first_code,
        )
        attended = from_units(exchange(unit_out))
        residual = own_input + scatter_head_rows(mm(attended, out_full, ((0,), (1,))).astype(low))

        second_rows = gather_all_rows((residual * norm_scale(residual) * gain_second).astype(low))
        cot_rows = gather_all_rows(cot_own)
        gate_value = mm(second_rows, gate_full, ((1,), (0,)))
        upward = mm(second_rows, up_full, ((1,), (0,)))
        sigma = jax.nn.sigmoid(gate_value)
        active = gate_value * sigma
        hidden = (active * upward).astype(low)
        grad_hidden = mm(cot_rows, down_full, ((1,), (0,)))
        gate_back = (grad_hidden * upward * (sigma * (1.0 + gate_value * (1.0 - sigma)))).astype(low)
        up_back = (grad_hidden * active).astype(low)
        second_parts = (mm(gate_back, gate_full, ((1,), (1,))) + mm(up_back, up_full, ((1,), (1,)))).astype(low)
        grad_second_rows = scatter_all_rows(second_parts)
        down_grad = jnp.concatenate(core_merge(ring_scatter(mm(cot_rows, hidden, ((0,), (0,))).astype(low))), axis=1)
        gate_grad = jnp.concatenate(core_merge(ring_scatter(mm(second_rows, gate_back, ((0,), (0,))).astype(low))), axis=1)
        up_grad = jnp.concatenate(core_merge(ring_scatter(mm(second_rows, up_back, ((0,), (0,))).astype(low))), axis=1)
        output_rows = residual + scatter_all_rows(mm(hidden, down_full, ((1,), (1,))).astype(low))

        residual_part, gain_two = norm_back(residual, gain_second, grad_second_rows)
        grad_residual = cot_own.astype(f32) + residual_part
        grad_rows = gather_head_rows(grad_residual.astype(low))
        grad_attended = mm(out_full, grad_rows, ((0,), (1,))).astype(low)
        unit_grad = exchange(to_units(grad_attended))
        (unit_back,) = vmem_call(
            functools.partial(attend_back_kernel, group),
            (jax.ShapeDtypeStruct((pieces, unit_rows, toks), low),),
            [
                pltpu.VMEM((unit_rows, DOCUMENT_LIMIT), low),
                pltpu.VMEM((group * dim, DOCUMENT_LIMIT), low),
                pltpu.VMEM((dim, DOCUMENT_LIMIT), f32),
                pltpu.VMEM((dim, DOCUMENT_LIMIT), f32),
            ],
            5 * square,
            unit,
            unit_grad,
            code_column,
            last_code,
            first_code,
            unit_stat,
            unit_cosine,
            unit_sine,
        )
        back_rows = from_units(exchange(unit_back))
        grad_first_rows = scatter_head_rows(mm(back_rows, head_full, ((0,), (1,))).astype(low))
        head_grad = scatter_head_weight(mm(first_rows, back_rows, ((0,), (1,))).astype(low))
        out_grad = scatter_head_weight(mm(grad_rows, attended, ((0,), (1,))).astype(low))
        input_part, gain_one = norm_back(own_input, gain_first, grad_first_rows)
        input_grad = (grad_residual + input_part).astype(low)
        gain_sums = all_sum(jnp.stack([gain_one, gain_two]))

    if fused:
        part_widths = [matrix.shape[1] // CORES for matrix in (query_weight, key_matrix, value_matrix)]
        starts = [0, part_widths[0], part_widths[0] + part_widths[1]]
        core_width = sum(part_widths)
        query_grad, key_grad, value_grad = (
            jnp.concatenate([head_grad[:, part * core_width + at : part * core_width + at + size] for part in range(CORES)], axis=1)
            for at, size in zip(starts, part_widths)
        )
    else:
        head_grad = head_grad.reshape(-1, value_heads, unit_rows)
        columns = query_weight.shape[0]
        query_grad = head_grad[:, :, : group * dim].reshape(columns, -1)
        key_grad = head_grad[:, :, group * dim : (group + 1) * dim].reshape(columns, -1)
        value_grad = head_grad[:, :, (group + 1) * dim :].reshape(columns, -1)
    return (
        output_rows.astype(low).reshape(block_input.shape),
        input_grad.reshape(block_input.shape),
        query_grad,
        key_grad,
        value_grad,
        out_grad.T,
        gate_grad,
        up_grad,
        down_grad.T,
        gain_sums[0],
        gain_sums[1],
    )


def solution(mesh):
    cp_count, tp_count = mesh.shape["cp"], mesh.shape["tp"]
    fine = Mesh(mesh.devices.reshape(cp_count // CORES, CORES, tp_count), ("chip", "core", "tp"))
    cp = ("chip", "core")
    rows = P(None, cp + ("tp",), None)
    wide, tall = P(cp, "tp"), P("tp", cp)
    return jax.shard_map(
        on_device,
        mesh=fine,
        in_specs=(rows, P(), P(), wide, wide, wide, tall, wide, wide, tall, P(), P(), rows),
        out_specs=(rows, rows, wide, wide, wide, tall, wide, wide, tall, P(), P()),
        check_vma=False,
    )
```

```python
import functools
import math

import jax
import jax.numpy as jnp
from jax import lax
from jax.experimental import pallas as pl
from jax.experimental.pallas import tpu as pltpu
from jax.sharding import Mesh
from jax.sharding import PartitionSpec as P

HEAD_SIZE = 96
DOCUMENT_LIMIT = 1024
CORES = 2

eps_norm = 1e-05
rope_base = 100000.0
masked_score = -1e30


f32 = jnp.float32
low = jnp.bfloat16


def mm(left, right, dims):
    return lax.dot_general(left, right, (dims, ((), ())), preferred_element_type=f32)


def pair_swap(values, axis):
    return lax.ppermute(values, axis, [(0, 1), (1, 0)])


def both(values, axis):
    other = pair_swap(values, axis)
    first = lax.axis_index(axis) == 0
    return jnp.stack([jnp.where(first, values, other), jnp.where(first, other, values)])


def split_pair(low_part, high_part, axis):
    first = lax.axis_index(axis) == 0
    return jnp.where(first, low_part, high_part), jnp.where(first, high_part, low_part)


def ring_of(count):
    order = list(range(0, count, 2)) + list(range(count - 1, 0, -2))
    place = [order.index(chip) for chip in range(count)]
    ahead = [(order[i], order[(i + 1) % count]) for i in range(count)]
    back = [(order[i], order[(i - 1) % count]) for i in range(count)]
    return order, place, ahead, back


def ring_gather(block):
    count = lax.axis_size("chip")
    order, place, ahead, back = ring_of(count)
    spot = jnp.array(place)[lax.axis_index("chip")]
    half_way, half_rows = count // 2, block.shape[0] // 2

    def put(whole, piece, step):
        owner = jnp.array(order)[(spot + step) % count]
        return lax.dynamic_update_index_in_dim(whole, piece, owner, 0)

    whole = put(jnp.zeros((count,) + block.shape, block.dtype), block, 0)
    up = down = block
    for step in range(1, half_way):
        up, down = lax.ppermute(up, "chip", ahead), lax.ppermute(down, "chip", back)
        whole = put(put(whole, up, count - step), down, step)
    up = lax.ppermute(up[:half_rows], "chip", ahead)
    down = lax.ppermute(down[half_rows:], "chip", back)
    whole = put(whole, jnp.concatenate([up, down], axis=0), half_way)
    return whole.reshape((count * block.shape[0],) + block.shape[1:])


def ring_scatter(terms):
    count = lax.axis_size("chip")
    order, place, ahead, back = ring_of(count)
    spot = jnp.array(place)[lax.axis_index("chip")]
    rows = terms.shape[0] // count
    half_way, half_rows = count // 2, rows // 2
    terms = terms.reshape((count, rows) + terms.shape[1:])

    def own(step):
        owner = jnp.array(order)[(spot + step) % count]
        return lax.dynamic_index_in_dim(terms, owner, 0, keepdims=False).astype(f32)

    far = own(half_way).astype(low)
    up = lax.ppermute(far[:half_rows], "chip", ahead)
    down = lax.ppermute(far[half_rows:], "chip", back)
    for step in range(half_way - 1, 0, -1):
        own_up, own_down = own(step), own(count - step)
        if step == half_way - 1:
            up = jnp.concatenate([own_up[:half_rows] + up.astype(f32), own_up[half_rows:]], axis=0)
            down = jnp.concatenate([own_down[:half_rows], own_down[half_rows:] + down.astype(f32)], axis=0)
        else:
            up, down = own_up + up.astype(f32), own_down + down.astype(f32)
        up = lax.ppermute(up.astype(low), "chip", ahead)
        down = lax.ppermute(down.astype(low), "chip", back)
    return own(0) + up.astype(f32) + down.astype(f32)


def core_split(low_part, high_part):
    kept, sent = split_pair(low_part, high_part, "core")
    other = pair_swap(sent, "core")
    first = lax.axis_index("core") == 0
    return jnp.concatenate([jnp.where(first, kept, other), jnp.where(first, other, kept)], axis=0)


def core_merge(rows):
    half = rows.shape[0] // 2
    kept, sent = split_pair(rows[:half], rows[half:], "core")
    other = pair_swap(sent.astype(low), "core").astype(f32)
    first = lax.axis_index("core") == 0
    return jnp.where(first, kept, other), jnp.where(first, other, kept)


def all_sum(values):
    for axis in ("tp", "core", "chip"):
        step = 1
        while step < lax.axis_size(axis):
            pairs = [(i, i ^ step) for i in range(lax.axis_size(axis))]
            values = values + lax.ppermute(values, axis, pairs)
            step *= 2
    return values


def gather_rows(rows, micro_count, cores):
    width = rows.shape[-1]
    tp_count = lax.axis_size("tp")
    joined = both(rows, "tp") if tp_count == 2 else lax.all_gather(rows, "tp", axis=0)
    joined = both(joined, "core") if cores == 2 else joined
    joined = joined.reshape((cores, 2, tp_count // 2, micro_count, -1, width))
    return joined.transpose((3, 1, 0, 2, 4, 5)).reshape((-1, width))


def scatter_rows(parts, micro_count, cores):
    width = parts.shape[-1]
    tp_count = lax.axis_size("tp")
    parts = parts.reshape((micro_count, 2, cores, tp_count // 2, -1, width)).transpose((2, 1, 3, 0, 4, 5))
    parts = parts.reshape((cores, tp_count, -1, width))
    if cores == 2:
        kept, sent = split_pair(parts[0], parts[1], "core")
        parts = (kept.astype(f32) + pair_swap(sent, "core").astype(f32)).astype(low)
    else:
        parts = parts[0]
    if tp_count == 2:
        kept, sent = split_pair(parts[0], parts[1], "tp")
        return kept.astype(f32) + pair_swap(sent, "tp").astype(f32)
    return lax.psum_scatter(parts, "tp", scatter_dimension=0, tiled=False).astype(f32)


def norm_scale(values):
    return lax.rsqrt(jnp.mean(values * values, axis=-1, keepdims=True) + eps_norm)


def norm_back(values, gain, grads):
    rho = norm_scale(values)
    scaled = grads * gain
    inner = jnp.mean(scaled * values, axis=-1, keepdims=True)
    return rho * scaled - values * (rho * rho * rho * inner), jnp.sum(grads * values * rho, axis=0)


def frequencies():
    return jnp.exp(jnp.arange(HEAD_SIZE // 2, dtype=f32) * (-2.0 * math.log(rope_base) / HEAD_SIZE))


def angles_of(spots):
    angles = frequencies()[:, None] * spots.astype(f32)[None, :]
    return jnp.cos(angles), jnp.sin(angles)


def unit_chunks(tokens):
    width = min(256, tokens)
    return [slice(start, start + width) for start in range(0, tokens, width)]


def lay_out(pieces_ref, flat):
    count, _, width = pieces_ref.shape
    for piece in range(count):
        flat[:, piece * width : (piece + 1) * width] = pieces_ref[piece]


def allowed_keys(code_column, last_row, first_row):
    return (code_column <= last_row) & (code_column >= first_row)


def attend_kernel(group, pieces_ref, code_ref, last_ref, first_ref, out_ref, stat_ref, flat):
    dim = HEAD_SIZE
    count, _, width = pieces_ref.shape
    tokens = count * width
    score_scale = dim ** (-0.5)
    lay_out(pieces_ref, flat)
    key_rows = flat[group * dim : (group + 1) * dim, :].astype(f32).T.astype(low)
    value_t = flat[(group + 1) * dim :, :]
    for cols in unit_chunks(tokens):
        keep = allowed_keys(code_ref[...], last_ref[:, cols], first_ref[:, cols])
        for head in range(group):
            query_t = flat[head * dim : (head + 1) * dim, cols]
            scores = mm(key_rows, query_t, ((1,), (0,))) * score_scale
            scores = jnp.where(keep, scores, masked_score)
            maximum = jnp.max(scores, axis=0, keepdims=True)
            weights = jnp.exp(scores - maximum)
            totals = jnp.sum(weights, axis=0, keepdims=True)
            probs = (weights * (1.0 / totals)).astype(low)
            stat_ref[head : head + 1, cols] = maximum + jnp.log(totals)
            result = mm(value_t, probs, ((1,), (0,))).astype(low)
            for piece in range(cols.start // width, cols.stop // width):
                start = piece * width - cols.start
                out_ref[piece, head * dim : (head + 1) * dim, :] = result[:, start : start + width]


def attend_back_kernel(
    group, pieces_ref, grads_ref, code_ref, last_ref, first_ref, stat_ref, cos_ref, sin_ref, out_ref, flat, grad_flat, key_sum, value_sum
):
    dim = HEAD_SIZE
    half = dim // 2
    count, _, width = pieces_ref.shape
    tokens = count * width
    score_scale = dim ** (-0.5)
    lay_out(pieces_ref, flat)
    lay_out(grads_ref, grad_flat)
    key_t = flat[group * dim : (group + 1) * dim, :]
    key_rows = key_t.astype(f32).T.astype(low)
    value_rows = flat[(group + 1) * dim :, :].astype(f32).T.astype(low)

    def store(values, base, cols):
        for piece in range(cols.start // width, cols.stop // width):
            start = piece * width - cols.start
            out_ref[piece, base : base + values.shape[0], :] = values[:, start : start + width]

    def unturn(values, base, cols):
        front, back = values[:half] * score_scale, values[half:] * score_scale
        cosine, sine = cos_ref[:, cols], sin_ref[:, cols]
        store((front * cosine + back * sine).astype(low), base, cols)
        store((back * cosine - front * sine).astype(low), base + half, cols)

    for index, cols in enumerate(unit_chunks(tokens)):
        keep = allowed_keys(code_ref[...], last_ref[:, cols], first_ref[:, cols])
        for head in range(group):
            rows = slice(head * dim, (head + 1) * dim)
            query_t, grad_t = flat[rows, cols], grad_flat[rows, cols]
            scores = mm(key_rows, query_t, ((1,), (0,))) * score_scale
            probs = jnp.where(keep, jnp.exp(scores - stat_ref[head : head + 1, cols]), 0.0)
            grad_probs = mm(value_rows, grad_t, ((1,), (0,)))
            delta = jnp.sum(probs * grad_probs, axis=0, keepdims=True)
            grad_scores = (probs * (grad_probs - delta)).astype(low)
            unturn(mm(key_t, grad_scores, ((1,), (0,))), head * dim, cols)
            key_part = mm(query_t, grad_scores, ((1,), (1,)))
            value_part = mm(grad_t, probs.astype(low), ((1,), (1,)))
            if index == 0 and head == 0:
                key_sum[...] = key_part
                value_sum[...] = value_part
            else:
                key_sum[...] += key_part
                value_sum[...] += value_part
    everything = slice(0, tokens)
    unturn(key_sum[...], group * dim, everything)
    store(value_sum[...].astype(low), (group + 1) * dim, everything)


MESH_ID = pl.DeviceIdType.MESH


class Sems:
    def __init__(self, send, recv):
        self.send, self.recv, self.used = send, recv, 0

    def take(self, count=1):
        base = self.used
        self.used += count
        return base


def remote(sems, index, source, target, there, arrive=None):
    return pltpu.make_async_remote_copy(
        src_ref=source,
        dst_ref=target,
        send_sem=sems.send.at[index],
        recv_sem=sems.recv.at[index if arrive is None else arrive],
        device_id=there,
        device_id_type=MESH_ID,
    )


def greet(chips, chip, core, tp):
    barrier = pltpu.get_barrier_semaphore()

    @pl.loop(1, chips)
    def _(step):
        pl.semaphore_signal(barrier, inc=1, device_id={"chip": (chip + step) % chips}, device_id_type=MESH_ID)

    pl.semaphore_signal(barrier, inc=1, device_id={"core": 1 - core}, device_id_type=MESH_ID)
    pl.semaphore_signal(barrier, inc=1, device_id={"tp": 1 - tp}, device_id_type=MESH_ID)
    pl.semaphore_wait(barrier, chips + 1)


def spot_of(chip, count):
    odd = chip % 2
    return (1 - odd) * (chip // 2) + odd * (count - 1 - chip // 2)


def chip_at(spot, count):
    spot = (spot + count) % count
    far = spot // (count // 2)
    return (1 - far) * 2 * spot + far * (2 * (count - 1 - spot) + 1)


class Ring:
    def __init__(self, sems, whole, rows, count, chip, saved, save_sem):
        self.sems, self.whole, self.rows, self.count = sems, whole, rows, count
        self.saved, self.save_sem = saved, save_sem
        self.spot = spot_of(chip, count)
        self.half = count // 2
        self.base = sems.take(2 * self.half)
        self.ways = (1, -1)

    def copy(self, side, hop, behind):
        way = self.ways[side]
        start = chip_at(self.spot - way * behind, self.count) * self.rows
        size = self.rows
        if hop == self.half:
            size = self.rows // 2
            start = start + side * size
        piece = self.whole.at[pl.ds(pl.multiple_of(start, 16), size), :]
        there = {"chip": chip_at(self.spot + way, self.count)}
        return remote(self.sems, self.base + side * self.half + hop - 1, piece, piece, there)

    def save(self, side, hop, behind):
        way = self.ways[side]
        start = chip_at(self.spot - way * behind, self.count) * self.rows
        size = self.rows
        if hop == self.half:
            size = self.rows // 2
            start = start + side * size
        if self.saved is None:
            return
        piece = pl.ds(pl.multiple_of(start, 16), size)
        pltpu.make_async_copy(self.whole.at[piece, :], self.saved.at[piece, :], self.save_sem).start()

    def start(self):
        for side in (0, 1):
            self.copy(side, 1, 0).start()
        self.save(0, 1, 0)

    def arrive(self):
        for side in (0, 1):
            self.copy(side, self.half, self.half).wait_recv()
            self.save(side, self.half, self.half)

    def relay(self, hop):
        for side in (0, 1):
            self.copy(side, hop - 1, hop - 1).wait_recv()
            self.copy(side, hop, hop - 1).start()
        for side in (0, 1):
            self.save(side, hop - 1, hop - 1)

    def saves_done(self):
        if self.saved is not None:
            pltpu.make_async_copy(self.whole, self.saved, self.save_sem).wait()

    def drain(self):
        for side in (0, 1):
            for hop in range(1, self.half + 1):
                self.copy(side, hop, hop - 1).wait_send()


class Spread:
    def __init__(self, sems, whole, micro, where):
        self.sems, self.whole, self.micro = sems, whole, micro
        _, self.core, self.tp = where
        self.rows = whole.shape[0] // (4 * micro)
        self.base = sems.take(3 * micro)

    def rows_of(self, m, half, core):
        return pl.ds(pl.multiple_of(((m * 2 + half) * 2 + core) * self.rows, 16), self.rows)

    def place(self, m, half, core):
        return self.whole.at[self.rows_of(m, half, core), :]

    def put(self, m, values):
        self.whole[self.rows_of(m, self.tp, self.core), :] = values

    def over_tp(self, m, half):
        piece = self.place(m, half, self.core)
        return remote(self.sems, self.base + m, piece, piece, {"tp": 1 - self.tp})

    def over_core(self, m, core):
        piece = self.place(m, self.tp, core)
        return remote(self.sems, self.base + self.micro + m, piece, piece, {"core": 1 - self.core})

    def passed_on(self, m, core):
        piece = self.place(m, 1 - self.tp, core)
        return remote(self.sems, self.base + 2 * self.micro + m, piece, piece, {"core": 1 - self.core})

    def start(self, m):
        self.over_tp(m, self.tp).start()
        self.over_core(m, self.core).start()

    def pass_on(self):
        for m in range(self.micro):
            self.over_tp(m, 1 - self.tp).wait_recv()
            self.passed_on(m, self.core).start()

    def finish(self):
        for m in range(self.micro):
            self.over_core(m, 1 - self.core).wait_recv()
            self.passed_on(m, 1 - self.core).wait_recv()

    def drain(self):
        for m in range(self.micro):
            self.over_tp(m, self.tp).wait_send()
            self.over_core(m, self.core).wait_send()
            self.passed_on(m, self.core).wait_send()


def turn_over(whole, turned):
    lanes = 256

    @pl.loop(0, whole.shape[1] // lanes)
    def _(part):
        columns = pl.ds(pl.multiple_of(part * lanes, 128), lanes)
        turned[columns, :] = whole[:, columns].astype(f32).T.astype(low)


def gain_row(gain_ref):
    return gain_ref[...].reshape(1, gain_ref.shape[0])


def half_blocks(front, back, which):
    lanes = front.shape[1]
    front, back = jnp.broadcast_to(front, (8, lanes)), jnp.broadcast_to(back, (8, lanes))
    front = jnp.where(which == 0, front, pltpu.roll(front, lanes // 2, 1))
    back = jnp.where(which == 0, pltpu.roll(back, lanes // 2, 1), back)
    return jnp.where(lax.broadcasted_iota(jnp.int32, (8, lanes), 1) < lanes // 2, front, back)[:1]


def angle_tables(spots, columns, cos_ref, sin_ref):
    place = lax.broadcasted_iota(jnp.int32, (HEAD_SIZE // 2, spots.shape[1]), 0).astype(f32)
    angles = jnp.exp(place * (-2.0 * math.log(rope_base) / HEAD_SIZE)) * spots.astype(f32)
    cos_ref[:, columns] = jnp.cos(angles)
    sin_ref[:, columns] = jnp.sin(angles)


def chip_line(ref, row, chip, which, toks):
    start = pl.multiple_of(chip * 2 * toks, 256)
    parts = []
    for at in (start, start + toks):
        lines = ref[:, pl.ds(at, toks)]
        line = lines[:1]
        for other in range(1, lines.shape[0]):
            line = jnp.where(row == other, lines[other : other + 1], line)
        parts.append(line)
    return half_blocks(*parts, which)


def unit_codes(seg_ref, pos_ref, code_ref, last_ref, start_ref, chips, chip, heads, tables=None):
    micro, half = chip // (2 * heads), chip // heads % 2
    toks = DOCUMENT_LIMIT // chips
    for source in range(chips):
        columns = slice(source * toks, (source + 1) * toks)
        spots = chip_line(pos_ref, micro, source, half, toks)
        first = (chip_line(seg_ref, micro, source, half, toks) * DOCUMENT_LIMIT).astype(f32)
        start_ref[:, columns] = first
        last_ref[:, columns] = first + spots.astype(f32)
        if tables is not None:
            angle_tables(spots, columns, *tables)
    code_ref[...] = jnp.broadcast_to(last_ref[...], (8, DOCUMENT_LIMIT)).T[:, :1]


class Fold:
    def __init__(self, sems, parts, from_core, to_tp, from_tp, micro, chip_core_tp):
        self.sems, self.parts, self.from_core, self.to_tp, self.from_tp = sems, parts, from_core, to_tp, from_tp
        self.micro = micro
        _, self.core, self.tp = chip_core_tp
        self.rows = from_tp.shape[0] // micro
        self.base = sems.take(3 * micro)

    def piece(self, m, half, core):
        start = ((m * 2 + half) * 2 + core) * self.rows
        return pl.ds(pl.multiple_of(start, 16), self.rows)

    def landing(self, m, half):
        return pl.ds(pl.multiple_of((m * 2 + half) * self.rows, 16), self.rows)

    def over_core(self, m, half):
        source = self.parts.at[self.piece(m, half, 1 - self.core), :]
        index = self.base + m * 2 + half
        return remote(self.sems, index, source, self.from_core.at[self.landing(m, half), :], {"core": 1 - self.core})

    def over_tp(self, m):
        rows = pl.ds(m * self.rows, self.rows)
        index = self.base + 2 * self.micro + m
        return remote(self.sems, index, self.to_tp.at[rows, :], self.from_tp.at[rows, :], {"tp": 1 - self.tp})

    def start(self, m, half):
        self.over_core(m, half).start()

    def summed(self, m, half):
        mine = self.parts[self.piece(m, half, self.core), :].astype(f32)
        return mine + self.from_core[self.landing(m, half), :].astype(f32)

    def send(self, m):
        for half in (0, 1):
            self.over_core(m, half).wait_recv()
        self.to_tp[m * self.rows : (m + 1) * self.rows, :] = self.summed(m, 1 - self.tp).astype(low)
        self.over_tp(m).start()

    def result(self, m):
        kept = self.summed(m, self.tp)
        self.over_tp(m).wait_recv()
        return kept + self.from_tp[m * self.rows : (m + 1) * self.rows, :].astype(f32)

    def drain(self):
        for m in range(self.micro):
            for half in (0, 1):
                self.over_core(m, half).wait_send()
            self.over_tp(m).wait_send()


class Exchange:
    def __init__(self, sems, outgoing, incoming, chips, chip):
        self.sems, self.outgoing, self.incoming, self.chips, self.chip = sems, outgoing, incoming, chips, chip
        self.base = sems.take(chips)

    def copy(self, to):
        return remote(
            self.sems, self.base + to, self.outgoing.at[to], self.incoming.at[self.chip], {"chip": to}, self.base + self.chip
        )

    def send(self, to):
        @pl.when(to != self.chip)
        def _():
            self.copy(to).start()

        @pl.when(to == self.chip)
        def _():
            self.incoming[to] = self.outgoing[to]

    def finish(self):
        @pl.loop(1, self.chips)
        def _(step):
            source = (self.chip + step) % self.chips
            remote(
                self.sems, self.base + source, self.outgoing.at[source], self.incoming.at[source], {"chip": source}
            ).wait_recv()

    def drain(self):
        @pl.loop(1, self.chips)
        def _(step):
            self.copy((self.chip + step) % self.chips).wait_send()


class Actions:
    def __init__(self, steps):
        self.steps = list(steps)

    def run(self, count=None):
        count = len(self.steps) if count is None else count
        for step in self.steps[:count]:
            step()
        self.steps = self.steps[count:]


def unit_sources(group, heads, head):
    queries = [(head * group + member) * HEAD_SIZE for member in range(group)]
    return queries + [(heads * group + head) * HEAD_SIZE, (heads * group + heads + head) * HEAD_SIZE]


def forward_kernel(
    micro, group, chips,
    x_ref, cot_ref, head_ref, out_ref, gate_ref, up_ref, down_ref, gain_one_ref, gain_two_ref, pos_ref, seg_ref,
    head_o, out_o, down_o, first_o, second_t_o, cot_t_o, unit_o, att_o, hidden_o, gate_back_o, up_back_o, second_o, stat_ref, residual_ref,
    head_w, out_w, gate_w, up_w, down_w, first_all, second_all, cot_all, first_t, second_t, cot_t, unit_send, unit_in, flat, att_send, att_in,
    parts, from_core, to_tp, from_tp, cos_ref, sin_ref, code_ref, last_ref, start_ref,
    gate_value, grad_hidden, hidden, gate_back, up_back, second_parts, send_sem, recv_sem, local_sem, save_sem,
):
    dim = HEAD_SIZE
    half = dim // 2
    chip, core, tp = lax.axis_index("chip"), lax.axis_index("core"), lax.axis_index("tp")
    where = (chip, core, tp)
    sems = Sems(send_sem, recv_sem)
    rows = x_ref.shape[0] // micro
    toks = 2 * rows
    unit_rows = (group + 2) * dim
    heads = head_w.shape[1] // unit_rows
    hops = chips // 2
    depth = head_ref.shape[0]
    greet(chips, chip, core, tp)

    weights = ((head_ref, head_w, head_o), (out_ref, out_w, out_o), (down_ref, down_w, down_o), (gate_ref, gate_w, None), (up_ref, up_w, None))
    rings, swaps, keeps = [], [], []
    for index, (shard, whole, saved) in enumerate(weights):
        columns = whole.shape[1]
        mine = whole.at[pl.ds(pl.multiple_of((chip * 2 + core) * depth, 16), depth), :]
        theirs = whole.at[pl.ds(pl.multiple_of((chip * 2 + 1 - core) * depth, 16), depth), :]
        at = sems.take()
        give = shard.at[:, pl.ds(pl.multiple_of((1 - core) * columns, 128), columns)]
        hold = shard.at[:, pl.ds(pl.multiple_of(core * columns, 128), columns)]
        swaps.append((remote(sems, at, give, mine, {"core": 1 - core}), remote(sems, at, give, theirs, {"core": 1 - core})))
        keeps.append(pltpu.make_async_copy(hold, mine, local_sem.at[index]))
        rings.append(Ring(sems, whole, 2 * depth, chips, chip, saved, save_sem.at[index]))
    first, second, cot = (Spread(sems, whole, micro, where) for whole in (first_all, second_all, cot_all))
    to_unit = Exchange(sems, unit_send, unit_in, chips, chip)
    from_unit = Exchange(sems, att_send, att_in, chips, chip)
    fold = Fold(sems, parts, from_core, to_tp, from_tp, micro, where)
    saves = []

    def save(source, target):
        saves.append(pltpu.make_async_copy(source, target, save_sem.at[5 + len(saves)]))
        saves[-1].start()

    for index in (0, 1):
        swaps[index][0].start()
        keeps[index].start()
    for m in range(micro):
        values = x_ref[m * rows : (m + 1) * rows, :].astype(f32)
        first.put(m, (values * norm_scale(values) * gain_row(gain_one_ref)).astype(low))
    for index in (2, 3, 4):
        swaps[index][0].start()
        keeps[index].start()
    for m in range(micro):
        cot.put(m, cot_ref[m * rows : (m + 1) * rows, :])
        first.start(m)
    head_ring, out_ring, down_ring, gate_ring, up_ring = rings
    for index in (0, 1):
        keeps[index].wait()
        swaps[index][1].wait_recv()
        rings[index].start()
    for m in range(micro):
        for side in (0, 1):
            columns = slice((m * 2 + side) * toks, (m * 2 + side + 1) * toks)
            angle_tables(chip_line(pos_ref, m, chip, side, toks), columns, cos_ref, sin_ref)
    first.pass_on()
    for hop in range(2, hops + 1):
        head_ring.relay(hop)
        out_ring.relay(hop)
    for index in (2, 3, 4):
        keeps[index].wait()
        swaps[index][1].wait_recv()
    down_ring.start()
    first.finish()
    head_ring.arrive()
    later = Actions(
        [ring.start for ring in (gate_ring, up_ring)]
        + [functools.partial(ring.relay, hop) for hop in range(2, hops + 1) for ring in (down_ring, gate_ring, up_ring)]
    )

    @pl.loop(0, micro * 2)
    def _(block):
        tokens = pl.ds(pl.multiple_of(block * toks, 128), toks)
        lines = mm(first_all[tokens, :], head_w[...], ((1,), (0,))).T
        cosine, sine = cos_ref[:, tokens], sin_ref[:, tokens]
        for head in range(heads):
            u = block * heads + head
            for turn, source in enumerate(unit_sources(group, heads, head)):
                front, back = lines[source : source + half], lines[source + half : source + dim]
                if turn < group + 1:
                    front, back = front * cosine - back * sine, back * cosine + front * sine
                unit_send[u, turn * dim : turn * dim + half, :] = front.astype(low)
                unit_send[u, turn * dim + half : (turn + 1) * dim, :] = back.astype(low)
            to_unit.send(u)

    later.run(1)
    for m in range(micro):
        cot.start(m)
    out_ring.arrive()
    unit_codes(seg_ref, pos_ref, code_ref, last_ref, start_ref, chips, chip, heads)
    later.run(2)
    cot.pass_on()
    to_unit.finish()

    score_scale = dim ** (-0.5)
    lay_out(unit_in, flat)
    save(unit_in, unit_o)
    key_rows = flat[group * dim : (group + 1) * dim, :].astype(f32).T.astype(low)
    lanes = 256

    @pl.loop(0, chips * toks // lanes)
    def _(number):
        cols = pl.ds(pl.multiple_of(number * lanes, 128), lanes)
        keep = allowed_keys(code_ref[...], last_ref[:, cols], start_ref[:, cols])
        for head in range(group):
            query_t = flat[head * dim : (head + 1) * dim, cols]
            scores = mm(key_rows, query_t, ((1,), (0,))) * score_scale
            scores = jnp.where(keep, scores, masked_score)
            maximum = jnp.max(scores, axis=0, keepdims=True)
            exponents = jnp.exp(scores - maximum)
            totals = jnp.sum(exponents, axis=0, keepdims=True)
            probs = (exponents * (1.0 / totals)).astype(low)
            stat_ref[head : head + 1, cols] = maximum + jnp.log(totals)
            result = mm(flat[(group + 1) * dim :, :], probs, ((1,), (0,))).astype(low)
            for piece in range(lanes // toks):
                here = result[:, piece * toks : (piece + 1) * toks]
                att_send[number * (lanes // toks) + piece, head * dim : (head + 1) * dim, :] = here
        for piece in range(lanes // toks):
            from_unit.send(number * (lanes // toks) + piece)

        @pl.when(number == 1)
        def _():
            later.run(1)

    later.run(1)
    cot.finish()
    turn_over(cot_all, cot_t)
    save(cot_t, cot_t_o)
    turn_over(first_all, first_t)
    save(first_t, first_o)
    from_unit.finish()
    save(att_in, att_o)

    @pl.loop(0, micro * 2)
    def _(block):
        lines = jnp.concatenate([att_in[block * heads + head] for head in range(heads)], axis=0)
        lines = lines.astype(f32).T.astype(low)
        sums = mm(lines, out_w[...], ((1,), (1,)))
        parts[pl.ds(pl.multiple_of(block * toks, 128), toks), :] = sums.astype(low)
        fold.start(block // 2, block % 2)

    for m in range(micro):
        fold.send(m)
    later.run(1)
    for m in range(micro):
        own = slice(m * rows, (m + 1) * rows)
        residual = x_ref[own, :].astype(f32) + fold.result(m)
        residual_ref[own, :] = residual
        second.put(m, (residual * norm_scale(residual) * gain_row(gain_two_ref)).astype(low))
        second.start(m)
    later.run(2)
    second.pass_on()
    second.finish()
    later.run()

    lanes = 256
    hidden_blocks = gate_w.shape[1] // lanes

    def block_of(part):
        return pl.ds(pl.multiple_of(part * lanes, 128), lanes)

    down_ring.arrive()

    @pl.loop(0, hidden_blocks)
    def _(part):
        cols = block_of(part)
        grad_hidden[:, cols] = mm(cot_all[...], down_w[:, cols], ((1,), (0,)))

    gate_ring.arrive()

    @pl.loop(0, hidden_blocks)
    def _(part):
        cols = block_of(part)
        gate_value[:, cols] = mm(second_all[...], gate_w[:, cols], ((1,), (0,)))

    turn_over(second_all, second_t)
    save(second_t, second_t_o)
    up_ring.arrive()

    @pl.loop(0, hidden_blocks)
    def _(part):
        cols = block_of(part)
        upward = mm(second_all[...], up_w[:, cols], ((1,), (0,)))
        value, grads = gate_value[:, cols], grad_hidden[:, cols]
        sigma = 1.0 / (1.0 + jnp.exp(-value))
        active = value * sigma
        hidden[:, cols] = (active * upward).astype(low)
        gate_back[:, cols] = (grads * upward * (sigma * (1.0 + value * (1.0 - sigma)))).astype(low)
        up_back[:, cols] = (grads * active).astype(low)

    save(hidden, hidden_o)
    save(gate_back, gate_back_o)
    save(up_back, up_back_o)

    @pl.loop(0, second_parts.shape[1] // lanes)
    def _(part):
        cols = block_of(part)
        sums = mm(gate_back[...], gate_w[cols, :], ((1,), (1,))) + mm(up_back[...], up_w[cols, :], ((1,), (1,)))
        second_parts[:, cols] = sums.astype(low)

    save(second_parts, second_o)
    for part in saves:
        part.wait()
    for ring in rings:
        ring.saves_done()
    for swap, _ in swaps:
        swap.wait_send()
    for part in rings + [first, second, cot, to_unit, from_unit, fold]:
        part.drain()


def forward_call(micro, group, chips, heads, *operands):
    x, _, head_s, out_s, gate_s, up_s, down_s = operands[:7]
    own_rows, width = x.shape
    toks = own_rows // micro * 2
    all_rows = own_rows * 4
    pieces = micro * 2 * heads
    unit_rows, att_rows = (group + 2) * HEAD_SIZE, group * HEAD_SIZE
    shape = jax.ShapeDtypeStruct
    columns = [s.shape[1] // CORES for s in (head_s, out_s, gate_s, up_s, down_s)]
    any_spec, vmem_spec = pl.BlockSpec(memory_space=pl.ANY), pl.BlockSpec(memory_space=pltpu.VMEM)
    hidden = columns[-1]
    any_outs = [shape((width, c), low) for c in (columns[0], columns[1], hidden)] + [shape((width, all_rows), low)] * 3
    any_outs += [shape((pieces, unit_rows, toks), low), shape((pieces, att_rows, toks), low)]
    any_outs += [shape((all_rows, hidden), low)] * 3 + [shape((all_rows, width), low)]
    vmem_outs = [shape((group, DOCUMENT_LIMIT), f32), shape((own_rows, width), f32)]
    scratch = [pltpu.VMEM((width, c), low) for c in columns]
    scratch += [pltpu.VMEM((all_rows, width), low)] * 3 + [pltpu.VMEM((width, all_rows), low)] * 3
    scratch += [
        pltpu.VMEM((pieces, unit_rows, toks), low),
        pltpu.VMEM((pieces, unit_rows, toks), low),
        pltpu.VMEM((unit_rows, DOCUMENT_LIMIT), low),
        pltpu.VMEM((pieces, att_rows, toks), low),
        pltpu.VMEM((pieces, att_rows, toks), low),
        pltpu.VMEM((all_rows, width), low),
        pltpu.VMEM((all_rows // 2, width), low),
        pltpu.VMEM((own_rows, width), low),
        pltpu.VMEM((own_rows, width), low),
        pltpu.VMEM((HEAD_SIZE // 2, all_rows), f32),
        pltpu.VMEM((HEAD_SIZE // 2, all_rows), f32),
        pltpu.VMEM((DOCUMENT_LIMIT, 1), f32),
        pltpu.VMEM((1, DOCUMENT_LIMIT), f32),
        pltpu.VMEM((1, DOCUMENT_LIMIT), f32),
        pltpu.VMEM((all_rows, hidden), f32),
        pltpu.VMEM((all_rows, hidden), f32),
        pltpu.VMEM((all_rows, hidden), low),
        pltpu.VMEM((all_rows, hidden), low),
        pltpu.VMEM((all_rows, hidden), low),
        pltpu.VMEM((all_rows, width), low),
        pltpu.SemaphoreType.DMA((96,)),
        pltpu.SemaphoreType.DMA((96,)),
        pltpu.SemaphoreType.DMA((5,)),
        pltpu.SemaphoreType.DMA((16,)),
    ]
    return pl.pallas_call(
        functools.partial(forward_kernel, micro, group, chips),
        out_shape=tuple(any_outs + vmem_outs),
        in_specs=[vmem_spec] * 2 + [any_spec] * 5 + [vmem_spec] * (len(operands) - 7),
        out_specs=tuple([any_spec] * len(any_outs) + [vmem_spec] * len(vmem_outs)),
        scratch_shapes=scratch,
        compiler_params=pltpu.CompilerParams(collective_id=0, has_side_effects=True, vmem_limit_bytes=60 << 20),
    )(*operands)


class RingSum:
    def __init__(self, sems, make, far, slots, count, chip, core):
        self.sems, self.make, self.far, self.slots, self.count, self.chip, self.core = sems, make, far, slots, count, chip, core
        self.rows = far.shape[0]
        self.spot = spot_of(chip, count)
        self.half = count // 2
        self.base = sems.take(2 * self.half)
        self.ways = (1, -1)

    def slot(self, side, hop):
        return (side * self.half + hop - 1) * self.rows

    def term(self, side, distance):
        return chip_at(self.spot + self.ways[side] * distance, self.count) * self.rows

    def copy(self, side, hop):
        there = {"chip": chip_at(self.spot + self.ways[side], self.count)}
        index = self.base + side * self.half + hop - 1
        if hop == 1:
            size = self.rows // 2
            source = self.far.at[side * size : (side + 1) * size, :]
            target = self.slots.at[pl.ds(self.slot(side, 1) + side * size, size), :]
        else:
            source = self.slots.at[pl.ds(self.slot(side, hop - 1), self.rows), :]
            target = self.slots.at[pl.ds(self.slot(side, hop), self.rows), :]
        return remote(self.sems, index, source, target, there)

    def start(self):
        self.far[...] = self.make((self.term(0, self.half),), self.rows).astype(low)
        for side in (0, 1):
            self.copy(side, 1).start()

    def relay(self, hop):
        size = self.rows // 2
        own = self.make([self.term(side, self.half - hop + 1) for side in (0, 1)], self.rows)
        for side in (0, 1):
            self.copy(side, hop - 1).wait_recv()
            at = self.slot(side, hop - 1)
            for part in (0, 1):
                here = pl.ds(at + part * size, size)
                mine = own[side * self.rows + part * size : side * self.rows + (part + 1) * size]
                if hop == 2 and part != side:
                    self.slots[here, :] = mine.astype(low)
                else:
                    self.slots[here, :] = (mine + self.slots[here, :].astype(f32)).astype(low)
            self.copy(side, hop).start()

    def result(self):
        size = self.rows // 2
        offsets = [self.core * size, (1 - self.core) * size]
        own = self.make([self.chip * self.rows + offset for offset in offsets], size)
        for side in (0, 1):
            self.copy(side, self.half).wait_recv()
        sums = []
        for index, offset in enumerate(offsets):
            total = own[index * size : (index + 1) * size]
            for side in (0, 1):
                here = pl.ds(pl.multiple_of(self.slot(side, self.half) + offset, 16), size)
                total = total + self.slots[here, :].astype(f32)
            sums.append(total)
        return sums

    def drain(self):
        for side in (0, 1):
            for hop in range(1, self.half + 1):
                self.copy(side, hop).wait_send()


def rows_from(ref, starts, size):
    blocks = [ref[pl.ds(pl.multiple_of(start, 16), size), :] for start in starts]
    return blocks[0] if len(blocks) == 1 else jnp.concatenate(blocks, axis=0)


class Merge:
    def __init__(self, sems, ring, leaving, landing, out, core, result, result_sem):
        self.sems, self.ring, self.leaving, self.landing, self.out, self.core = sems, ring, leaving, landing, out, core
        self.result = pltpu.make_async_copy(out, result, result_sem)
        self.index = sems.take()

    def copy(self):
        return remote(self.sems, self.index, self.leaving, self.landing, {"core": 1 - self.core})

    def send(self):
        kept, sent = self.ring.result()
        self.leaving[...] = sent.astype(low)
        self.copy().start()
        columns = self.leaving.shape[1]
        self.out[:, pl.ds(pl.multiple_of(self.core * columns, 128), columns)] = kept

    def finish(self):
        columns = self.leaving.shape[1]
        self.copy().wait_recv()
        self.out[:, pl.ds(pl.multiple_of((1 - self.core) * columns, 128), columns)] = self.landing[...].astype(f32)
        self.result.start()

    def drain(self):
        self.copy().wait_send()
        self.result.wait()


class Butterfly:
    def __init__(self, sems, leaving, landing, chips, where):
        self.sems, self.leaving, self.landing = sems, leaving, landing
        chip, core, tp = where
        self.partners = [{"tp": 1 - tp}, {"core": 1 - core}]
        step = 1
        while step < chips:
            self.partners.append({"chip": chip + step - 2 * step * (chip // step % 2)})
            step *= 2
        self.base = sems.take(len(self.partners))

    def copy(self, stage):
        return remote(self.sems, self.base + stage, self.leaving.at[stage], self.landing.at[stage], self.partners[stage])

    def start(self, values):
        self.leaving[0] = values
        self.copy(0).start()

    def step(self, stage):
        self.copy(stage).wait_recv()
        values = self.leaving[stage] + self.landing[stage]
        if stage + 1 < len(self.partners):
            self.leaving[stage + 1] = values
            self.copy(stage + 1).start()
        return values

    def drain(self):
        for stage in range(len(self.partners)):
            self.copy(stage).wait_send()


def backward_kernel(
    micro, group, chips,
    x_ref, residual_ref, cot_ref, gain_one_ref, gain_two_ref, stat_ref, pos_ref, seg_ref,
    second_h, cot_t_h, hidden_h, second_t_h, gate_back_h, up_back_h, unit_h, att_h, down_h, out_h, first_t_h, head_h,
    output_ref, input_grad_ref, head_x, out_x, gate_x, up_x, down_x, gain_one_g, gain_two_g,
    second_parts, cot_t, hidden, second_t, gate_back, up_back, unit_ref, att_ref, down_w, out_w, first_t, head_w,
    core_a, to_tp_a, from_tp_a, core_b, to_tp_b, from_tp_b, core_c, to_tp_c, from_tp_c, grad_residual, grad_all, output_parts, first_parts,
    grad_send, grad_in, flat, grad_flat, key_sum, value_sum, back_send, back_in, att_flat, back_flat, out_terms,
    cos_ref, sin_ref, code_ref, last_ref, start_ref,
    head_far, out_far, down_far, gate_far, up_far, head_slots, out_slots, down_slots, gate_slots, up_slots,
    head_leave, out_leave, down_leave, gate_leave, up_leave, head_land, out_land, down_land, gate_land, up_land,
    gain_leave, gain_land, head_g, out_g, gate_g, up_g, down_g, send_sem, recv_sem, local_sem, leave_sem,
):
    dim = HEAD_SIZE
    half = dim // 2
    chip, core, tp = lax.axis_index("chip"), lax.axis_index("core"), lax.axis_index("tp")
    where = (chip, core, tp)
    sems = Sems(send_sem, recv_sem)
    rows = x_ref.shape[0] // micro
    toks = 2 * rows
    unit_rows = (group + 2) * dim
    heads = head_w.shape[1] // unit_rows
    blocks = micro * 2
    hops = chips // 2
    sources = (second_h, cot_t_h, hidden_h, second_t_h, gate_back_h, up_back_h, unit_h, att_h, down_h, out_h, first_t_h, head_h)
    places = (second_parts, cot_t, hidden, second_t, gate_back, up_back, unit_ref, att_ref, down_w, out_w, first_t, head_w)
    loads = [pltpu.make_async_copy(a, b, local_sem.at[i]) for i, (a, b) in enumerate(zip(sources, places))]
    for load in loads:
        load.start()
    greet(chips, chip, core, tp)

    def ring_of_products(left, right, far, slots):
        make = lambda starts, size: mm(rows_from(left, starts, size), right[...], ((1,), (0,)))
        return RingSum(sems, make, far, slots, chips, chip, core)

    down_ring = ring_of_products(cot_t, hidden, down_far, down_slots)
    gate_ring = ring_of_products(second_t, gate_back, gate_far, gate_slots)
    up_ring = ring_of_products(second_t, up_back, up_far, up_slots)
    out_ring = RingSum(sems, lambda starts, size: rows_from(out_terms, starts, size).astype(f32), out_far, out_slots, chips, chip, core)
    head_ring = RingSum(
        sems, lambda starts, size: mm(rows_from(first_t, starts, size), back_flat[...], ((1,), (1,))), head_far, head_slots, chips, chip, core
    )
    down_merge, gate_merge, up_merge, out_merge, head_merge = (
        Merge(sems, down_ring, down_leave, down_land, down_g, core, down_x, leave_sem.at[0]),
        Merge(sems, gate_ring, gate_leave, gate_land, gate_g, core, gate_x, leave_sem.at[1]),
        Merge(sems, up_ring, up_leave, up_land, up_g, core, up_x, leave_sem.at[2]),
        Merge(sems, out_ring, out_leave, out_land, out_g, core, out_x, leave_sem.at[3]),
        Merge(sems, head_ring, head_leave, head_land, head_g, core, head_x, leave_sem.at[4]),
    )
    second_fold = Fold(sems, second_parts, core_a, to_tp_a, from_tp_a, micro, where)
    output_fold = Fold(sems, output_parts, core_b, to_tp_b, from_tp_b, micro, where)
    first_fold = Fold(sems, first_parts, core_c, to_tp_c, from_tp_c, micro, where)
    spread = Spread(sems, grad_all, micro, where)
    to_unit = Exchange(sems, grad_send, grad_in, chips, chip)
    from_unit = Exchange(sems, back_send, back_in, chips, chip)
    butterfly = Butterfly(sems, gain_leave, gain_land, chips, where)
    later = Actions([functools.partial(ring.relay, hop) for hop in range(2, hops + 1) for ring in (down_ring, gate_ring, up_ring)])

    loads[0].wait()
    for m in range(micro):
        for side in (0, 1):
            second_fold.start(m, side)
    for load in loads[1:3]:
        load.wait()
    down_ring.start()
    for m in range(micro):
        second_fold.send(m)
    for load in loads[3:6]:
        load.wait()
    gate_ring.start()
    up_ring.start()

    def norm_rows_back(values, gain, grads):
        rho = norm_scale(values)
        scaled = grads * gain
        inner = jnp.mean(scaled * values, axis=-1, keepdims=True)
        return rho * scaled - values * (rho * rho * rho * inner), jnp.sum(grads * values * rho, axis=0, keepdims=True)

    later.run(1)
    gain_two = None
    for m in range(micro):
        own = slice(m * rows, (m + 1) * rows)
        part, gain_now = norm_rows_back(residual_ref[own, :], gain_row(gain_two_ref), second_fold.result(m))
        gain_two = gain_now if gain_two is None else gain_two + gain_now
        grads = cot_ref[own, :].astype(f32) + part
        grad_residual[own, :] = grads
        spread.put(m, grads.astype(low))
        spread.start(m)
    for load in loads[6:8]:
        load.wait()
    lay_out(unit_ref, flat)
    for piece in range(blocks * heads):
        block, head = piece // heads, piece % heads
        att_flat[head * group * dim : (head + 1) * group * dim, block * toks : (block + 1) * toks] = att_ref[piece]
    key_t = flat[group * dim : (group + 1) * dim, :]
    key_rows = key_t.astype(f32).T.astype(low)
    value_rows = flat[(group + 1) * dim :, :].astype(f32).T.astype(low)
    unit_codes(seg_ref, pos_ref, code_ref, last_ref, start_ref, chips, chip, heads, (cos_ref, sin_ref))
    later.run(1)
    spread.pass_on()
    for load in loads[8:10]:
        load.wait()
    later.run(1)
    spread.finish()

    @pl.loop(0, blocks)
    def _(block):
        tokens = pl.ds(pl.multiple_of(block * toks, 128), toks)
        lines = mm(grad_all[tokens, :], out_w[...], ((1,), (0,))).T.astype(low)
        for head in range(heads):
            piece = block * heads + head
            grad_send[piece] = lines[head * group * dim : (head + 1) * group * dim]
            to_unit.send(piece)

    later.run(1)

    @pl.loop(0, blocks)
    def _(block):
        tokens = pl.ds(pl.multiple_of(block * toks, 128), toks)
        output_parts[tokens, :] = mm(hidden[tokens, :], down_w[...], ((1,), (1,))).astype(low)
        output_fold.start(block // 2, block % 2)

    lanes = 256

    @pl.loop(0, grad_all.shape[1] // lanes)
    def _(part):
        columns = pl.ds(pl.multiple_of(part * lanes, 128), lanes)
        out_terms[columns, :] = mm(att_flat[...], grad_all[:, columns], ((1,), (0,))).T.astype(low)

    out_ring.start()
    later.run(1)
    for m in range(micro):
        output_fold.send(m)
    to_unit.finish()
    lay_out(grad_in, grad_flat)

    score_scale = dim ** (-0.5)
    tokens_all = chips * toks
    key_sum[...] = jnp.zeros_like(key_sum)
    value_sum[...] = jnp.zeros_like(value_sum)

    def store(values, base, first_piece):
        for piece in range(values.shape[1] // toks):
            back_send[first_piece + piece, base : base + values.shape[0], :] = values[:, piece * toks : (piece + 1) * toks]

    def unturn(values, base, cols, first_piece):
        front, back = values[:half] * score_scale, values[half:] * score_scale
        cosine, sine = cos_ref[:, cols], sin_ref[:, cols]
        store((front * cosine + back * sine).astype(low), base, first_piece)
        store((back * cosine - front * sine).astype(low), base + half, first_piece)

    @pl.loop(0, tokens_all // lanes)
    def _(number):
        cols = pl.ds(pl.multiple_of(number * lanes, 128), lanes)
        keep = allowed_keys(code_ref[...], last_ref[:, cols], start_ref[:, cols])
        for head in range(group):
            lines = slice(head * dim, (head + 1) * dim)
            query_t, grad_t = flat[lines, cols], grad_flat[lines, cols]
            scores = mm(key_rows, query_t, ((1,), (0,))) * score_scale
            probs = jnp.where(keep, jnp.exp(scores - stat_ref[head : head + 1, cols]), 0.0)
            grad_probs = mm(value_rows, grad_t, ((1,), (0,)))
            delta = jnp.sum(probs * grad_probs, axis=0, keepdims=True)
            grad_scores = (probs * (grad_probs - delta)).astype(low)
            unturn(mm(key_t, grad_scores, ((1,), (0,))), head * dim, cols, number * (lanes // toks))
            key_sum[...] += mm(query_t, grad_scores, ((1,), (1,)))
            value_sum[...] += mm(grad_t, probs.astype(low), ((1,), (1,)))

        @pl.when(number == 1)
        def _():
            later.run(1)

    unturn(key_sum[...], group * dim, slice(0, tokens_all), 0)
    store(value_sum[...].astype(low), (group + 1) * dim, 0)

    @pl.loop(0, chips)
    def _(piece):
        from_unit.send(piece)

    later.run(1)
    for m in range(micro):
        own = slice(m * rows, (m + 1) * rows)
        output_ref[own, :] = (residual_ref[own, :] + output_fold.result(m)).astype(low)
    later.run(1)
    for load in loads[10:]:
        load.wait()
    from_unit.finish()

    for block in range(blocks):
        for head in range(heads):
            for turn, target in enumerate(unit_sources(group, heads, head)):
                piece = back_in[block * heads + head, turn * dim : (turn + 1) * dim, :]
                back_flat[target : target + dim, block * toks : (block + 1) * toks] = piece
    head_ring.start()

    @pl.loop(0, blocks)
    def _(block):
        tokens = pl.ds(pl.multiple_of(block * toks, 128), toks)
        lines = back_flat[:, tokens].astype(f32).T.astype(low)
        first_parts[tokens, :] = mm(lines, head_w[...], ((1,), (1,))).astype(low)
        first_fold.start(block // 2, block % 2)

    later.run(1)
    head_ring.relay(2)
    for m in range(micro):
        first_fold.send(m)
    later.run()
    out_ring.relay(2)
    down_merge.send()
    head_ring.relay(3)
    out_ring.relay(3)
    gain_one = None
    for m in range(micro):
        own = slice(m * rows, (m + 1) * rows)
        part, gain_now = norm_rows_back(x_ref[own, :].astype(f32), gain_row(gain_one_ref), first_fold.result(m))
        gain_one = gain_now if gain_one is None else gain_one + gain_now
        input_grad_ref[own, :] = (grad_residual[own, :] + part).astype(low)
    butterfly.start(jnp.concatenate([gain_one, gain_two], axis=0))
    head_ring.relay(4)
    out_ring.relay(4)
    butterfly.step(0)
    gate_merge.send()
    butterfly.step(1)
    up_merge.send()
    butterfly.step(2)
    down_merge.finish()
    gate_merge.finish()
    for stage in range(3, len(butterfly.partners) - 1):
        butterfly.step(stage)
    out_merge.send()
    head_merge.send()
    up_merge.finish()
    gain_sums = butterfly.step(len(butterfly.partners) - 1)
    gain_one_g[...] = gain_sums[0]
    gain_two_g[...] = gain_sums[1]
    out_merge.finish()
    head_merge.finish()
    parts = [down_ring, gate_ring, up_ring, out_ring, head_ring, down_merge, gate_merge, up_merge, out_merge, head_merge]
    parts += [second_fold, output_fold, first_fold, spread, to_unit, from_unit, butterfly]
    for part in parts:
        part.drain()


def backward_call(micro, group, chips, heads, near, *far):
    own_rows, width = near[0].shape
    toks = own_rows // micro * 2
    all_rows = own_rows * 4
    pieces = micro * 2 * heads
    unit_rows, att_rows = (group + 2) * HEAD_SIZE, group * HEAD_SIZE
    shape = jax.ShapeDtypeStruct
    hidden = far[2].shape[1]
    depth = width // chips
    columns = [heads * unit_rows, heads * att_rows, hidden, hidden, hidden]
    stages = 2 + (chips - 1).bit_length()
    any_spec, vmem_spec = pl.BlockSpec(memory_space=pl.ANY), pl.BlockSpec(memory_space=pltpu.VMEM)
    outs = [shape((own_rows, width), low)] * 2 + [shape((depth // 2, 2 * c), f32) for c in columns] + [shape((width,), f32)] * 2
    scratch = [pltpu.VMEM(a.shape, a.dtype) for a in far]
    scratch += [pltpu.VMEM((all_rows // 2, width), low), pltpu.VMEM((own_rows, width), low), pltpu.VMEM((own_rows, width), low)] * 3
    scratch += [
        pltpu.VMEM((own_rows, width), f32),
        pltpu.VMEM((all_rows, width), low),
        pltpu.VMEM((all_rows, width), low),
        pltpu.VMEM((all_rows, width), low),
        pltpu.VMEM((pieces, att_rows, toks), low),
        pltpu.VMEM((pieces, att_rows, toks), low),
        pltpu.VMEM((unit_rows, DOCUMENT_LIMIT), low),
        pltpu.VMEM((att_rows, DOCUMENT_LIMIT), low),
        pltpu.VMEM((HEAD_SIZE, DOCUMENT_LIMIT), f32),
        pltpu.VMEM((HEAD_SIZE, DOCUMENT_LIMIT), f32),
        pltpu.VMEM((pieces, unit_rows, toks), low),
        pltpu.VMEM((pieces, unit_rows, toks), low),
        pltpu.VMEM((heads * att_rows, all_rows), low),
        pltpu.VMEM((heads * unit_rows, all_rows), low),
        pltpu.VMEM((width, heads * att_rows), low),
        pltpu.VMEM((HEAD_SIZE // 2, DOCUMENT_LIMIT), f32),
        pltpu.VMEM((HEAD_SIZE // 2, DOCUMENT_LIMIT), f32),
        pltpu.VMEM((DOCUMENT_LIMIT, 1), f32),
        pltpu.VMEM((1, DOCUMENT_LIMIT), f32),
        pltpu.VMEM((1, DOCUMENT_LIMIT), f32),
    ]
    scratch += [pltpu.VMEM((depth, c), low) for c in columns]
    scratch += [pltpu.VMEM((chips * depth, c), low) for c in columns]
    scratch += [pltpu.VMEM((depth // 2, c), low) for c in columns] * 2
    scratch += [pltpu.VMEM((stages, 2, width), f32)] * 2
    scratch += [pltpu.VMEM((depth // 2, 2 * c), f32) for c in columns]
    scratch += [pltpu.SemaphoreType.DMA((128,))] * 2 + [pltpu.SemaphoreType.DMA((len(far),)), pltpu.SemaphoreType.DMA((len(columns),))]
    return pl.pallas_call(
        functools.partial(backward_kernel, micro, group, chips),
        out_shape=tuple(outs),
        in_specs=[vmem_spec] * len(near) + [any_spec] * len(far),
        out_specs=tuple([vmem_spec] * 2 + [any_spec] * len(columns) + [vmem_spec] * 2),
        scratch_shapes=scratch,
        compiler_params=pltpu.CompilerParams(collective_id=1, has_side_effects=True, vmem_limit_bytes=63 << 20),
    )(*near, *far)


def vmem_call(kernel, outs, scratch, flops, *operands):
    spec = pl.BlockSpec(memory_space=pltpu.VMEM)
    moved = sum(math.prod(a.shape) * a.dtype.itemsize for a in operands + tuple(outs))
    return pl.pallas_call(
        kernel,
        out_shape=tuple(outs),
        in_specs=[spec] * len(operands),
        out_specs=tuple([spec] * len(outs)),
        scratch_shapes=scratch,
        cost_estimate=pl.CostEstimate(flops=flops, bytes_accessed=moved, transcendentals=2 * DOCUMENT_LIMIT**2),
        compiler_params=pltpu.CompilerParams(vmem_limit_bytes=48 << 20),
    )(*operands)


def on_device(
    block_input,
    segments,
    positions,
    query_weight,
    key_matrix,
    value_matrix,
    out_weight,
    gate_weight,
    up_weight,
    down_weight,
    gain_first,
    gain_second,
    cotangent,
):
    chips, tp_count = lax.axis_size("chip"), lax.axis_size("tp")
    chip, core = lax.axis_index("chip"), lax.axis_index("core")
    cp_count, cp_index = chips * CORES, chip * CORES + core
    micro, tok_dev, width = block_input.shape
    dim = HEAD_SIZE
    block_rows = tok_dev * tp_count // 2
    query_heads, value_heads = query_weight.shape[1] // dim, key_matrix.shape[1] // dim
    group = query_heads // value_heads
    unit_rows = (group + 2) * dim
    head_cores = CORES if value_heads % CORES == 0 else 1
    heads = value_heads // head_cores
    toks = head_cores * block_rows
    pieces = DOCUMENT_LIMIT // toks
    assert pieces == micro * 2 * heads and cp_count % (pieces * head_cores) == 0

    out_t, down_t = out_weight.T, down_weight.T

    def halves(matrix):
        half = matrix.shape[1] // 2
        return matrix[:, :half], matrix[:, half:]

    def gather_head_weight(matrix):
        if head_cores == 2:
            return ring_gather(core_split(*halves(matrix)))
        return lax.all_gather(matrix, ("chip", "core"), axis=0, tiled=True)

    def scatter_head_weight(grads):
        if head_cores == 2:
            return jnp.concatenate(core_merge(ring_scatter(grads)), axis=1)
        return lax.psum_scatter(grads, ("chip", "core"), scatter_dimension=0, tiled=True).astype(f32)

    fused = tp_count == 2 and head_cores == CORES and pieces == chips and toks == 128
    if fused:
        cores = []
        for part in range(CORES):
            columns = lambda matrix: matrix[:, part * matrix.shape[1] // CORES : (part + 1) * matrix.shape[1] // CORES]
            cores += [columns(query_weight), columns(key_matrix), columns(value_matrix)]
        by_head = jnp.concatenate(cores, axis=1)
    else:
        by_head = jnp.concatenate(
            [
                query_weight.reshape(-1, value_heads, group * dim),
                key_matrix.reshape(-1, value_heads, dim),
                value_matrix.reshape(-1, value_heads, dim),
            ],
            axis=2,
        ).reshape(query_weight.shape[0], -1)
        head_full = gather_head_weight(by_head)
        out_full = gather_head_weight(out_t)
        gate_full = ring_gather(core_split(*halves(gate_weight)))
        up_full = ring_gather(core_split(*halves(up_weight)))
        down_full = ring_gather(core_split(*halves(down_t)))

    by_block = lambda line: line.reshape(micro, cp_count, 2, block_rows)
    group_cp = pieces * head_cores
    first_cp = cp_index // head_cores * head_cores
    if not fused:
        row_pos = lax.dynamic_slice_in_dim(by_block(positions), first_cp, head_cores, 1)
        row_pos = row_pos.transpose(0, 2, 1, 3).reshape(-1)
        unit_index = cp_index // head_cores % pieces
        unit_micro, unit_half = unit_index // (2 * heads), unit_index // heads % 2

        def unit_line(line):
            mine = lax.dynamic_slice(
                by_block(line),
                (unit_micro, cp_index // group_cp * group_cp, unit_half, 0),
                (1, group_cp, 1, block_rows),
            )
            return mine.reshape(1, DOCUMENT_LIMIT)

        unit_pos, unit_seg = unit_line(positions), unit_line(segments)
        first_code = unit_seg * DOCUMENT_LIMIT
        last_code = first_code + unit_pos
        code_column = last_code.reshape(DOCUMENT_LIMIT, 1)
        cosine, sine = angles_of(row_pos)
        unit_cosine, unit_sine = angles_of(unit_pos.reshape(-1))

    if head_cores == 2:
        exchange_axis = "chip"
        groups = [[g + i for i in range(pieces)] for g in range(0, chips, pieces)]
    else:
        exchange_axis = ("chip", "core")
        groups = [[g + i for i in range(pieces)] for g in range(0, cp_count, pieces)]
    groups = None if len(groups) == 1 else groups

    def exchange(values):
        return lax.all_to_all(values, exchange_axis, 0, 0, axis_index_groups=groups)

    def to_units(values):
        rows = values.shape[0] // heads
        return values.reshape(heads, rows, micro * 2, toks).transpose(2, 0, 1, 3).reshape(pieces, rows, toks)

    def from_units(values):
        rows = values.shape[1]
        return values.reshape(micro * 2, heads, rows, toks).transpose(1, 2, 0, 3).reshape(heads * rows, -1)

    gather_head_rows = functools.partial(gather_rows, micro_count=micro, cores=head_cores)
    scatter_head_rows = functools.partial(scatter_rows, micro_count=micro, cores=head_cores)
    gather_all_rows = functools.partial(gather_rows, micro_count=micro, cores=CORES)
    scatter_all_rows = functools.partial(scatter_rows, micro_count=micro, cores=CORES)

    own_input = block_input.reshape(-1, width).astype(f32)
    cot_own = cotangent.reshape(-1, width)
    square = DOCUMENT_LIMIT * DOCUMENT_LIMIT * dim * 2 * group
    own_rows = block_input.reshape(-1, width)
    if fused:
        facts = (gain_first, gain_second, positions, segments)
        head_full, out_full, down_full, first_t, second_t, cot_t, unit, att_pieces, hidden, gate_back, up_back, second_parts, unit_stat, residual = (
            forward_call(micro, group, chips, heads, own_rows, cot_own, by_head, out_t, gate_weight, up_weight, down_t, *facts)
        )
        output_rows, input_grad, head_grad, out_grad, gate_grad, up_grad, down_grad, *gain_sums = backward_call(
            micro, group, chips, heads,
            (own_rows, residual, cot_own, gain_first, gain_second, unit_stat, positions, segments),
            second_parts, cot_t, hidden, second_t, gate_back, up_back, unit, att_pieces, down_full, out_full, first_t, head_full,
        )
    else:
        first_rows = gather_head_rows((own_input * norm_scale(own_input) * gain_first).astype(low))
        projected = mm(head_full, first_rows, ((0,), (1,))).reshape(heads, unit_rows, -1)
        turned = projected[:, : (group + 1) * dim].reshape(heads, group + 1, 2, dim // 2, -1)
        front, back = turned[:, :, 0], turned[:, :, 1]
        turned = jnp.stack([front * cosine - back * sine, back * cosine + front * sine], axis=2)
        projected = jnp.concatenate(
            [turned.reshape(heads, (group + 1) * dim, -1).astype(low), projected[:, (group + 1) * dim :].astype(low)], axis=1
        )
        unit = exchange(to_units(projected.reshape(heads * unit_rows, -1)))
        unit_out, unit_stat = vmem_call(
            functools.partial(attend_kernel, group),
            (
                jax.ShapeDtypeStruct((pieces, group * dim, toks), low),
                jax.ShapeDtypeStruct((group, DOCUMENT_LIMIT), f32),
            ),
            [pltpu.VMEM((unit_rows, DOCUMENT_LIMIT), low)],
            2 * square,
            unit,
            code_column,
            last_code,
            first_code,
        )
        attended = from_units(exchange(unit_out))
        residual = own_input + scatter_head_rows(mm(attended, out_full, ((0,), (1,))).astype(low))

        second_rows = gather_all_rows((residual * norm_scale(residual) * gain_second).astype(low))
        cot_rows = gather_all_rows(cot_own)
        gate_value = mm(second_rows, gate_full, ((1,), (0,)))
        upward = mm(second_rows, up_full, ((1,), (0,)))
        sigma = jax.nn.sigmoid(gate_value)
        active = gate_value * sigma
        hidden = (active * upward).astype(low)
        grad_hidden = mm(cot_rows, down_full, ((1,), (0,)))
        gate_back = (grad_hidden * upward * (sigma * (1.0 + gate_value * (1.0 - sigma)))).astype(low)
        up_back = (grad_hidden * active).astype(low)
        second_parts = (mm(gate_back, gate_full, ((1,), (1,))) + mm(up_back, up_full, ((1,), (1,)))).astype(low)
        grad_second_rows = scatter_all_rows(second_parts)
        down_grad = jnp.concatenate(core_merge(ring_scatter(mm(cot_rows, hidden, ((0,), (0,))).astype(low))), axis=1)
        gate_grad = jnp.concatenate(core_merge(ring_scatter(mm(second_rows, gate_back, ((0,), (0,))).astype(low))), axis=1)
        up_grad = jnp.concatenate(core_merge(ring_scatter(mm(second_rows, up_back, ((0,), (0,))).astype(low))), axis=1)
        output_rows = residual + scatter_all_rows(mm(hidden, down_full, ((1,), (1,))).astype(low))

        residual_part, gain_two = norm_back(residual, gain_second, grad_second_rows)
        grad_residual = cot_own.astype(f32) + residual_part
        grad_rows = gather_head_rows(grad_residual.astype(low))
        grad_attended = mm(out_full, grad_rows, ((0,), (1,))).astype(low)
        unit_grad = exchange(to_units(grad_attended))
        (unit_back,) = vmem_call(
            functools.partial(attend_back_kernel, group),
            (jax.ShapeDtypeStruct((pieces, unit_rows, toks), low),),
            [
                pltpu.VMEM((unit_rows, DOCUMENT_LIMIT), low),
                pltpu.VMEM((group * dim, DOCUMENT_LIMIT), low),
                pltpu.VMEM((dim, DOCUMENT_LIMIT), f32),
                pltpu.VMEM((dim, DOCUMENT_LIMIT), f32),
            ],
            5 * square,
            unit,
            unit_grad,
            code_column,
            last_code,
            first_code,
            unit_stat,
            unit_cosine,
            unit_sine,
        )
        back_rows = from_units(exchange(unit_back))
        grad_first_rows = scatter_head_rows(mm(back_rows, head_full, ((0,), (1,))).astype(low))
        head_grad = scatter_head_weight(mm(first_rows, back_rows, ((0,), (1,))).astype(low))
        out_grad = scatter_head_weight(mm(grad_rows, attended, ((0,), (1,))).astype(low))
        input_part, gain_one = norm_back(own_input, gain_first, grad_first_rows)
        input_grad = (grad_residual + input_part).astype(low)
        gain_sums = all_sum(jnp.stack([gain_one, gain_two]))

    if fused:
        part_widths = [matrix.shape[1] // CORES for matrix in (query_weight, key_matrix, value_matrix)]
        starts = [0, part_widths[0], part_widths[0] + part_widths[1]]
        core_width = sum(part_widths)
        query_grad, key_grad, value_grad = (
            jnp.concatenate([head_grad[:, part * core_width + at : part * core_width + at + size] for part in range(CORES)], axis=1)
            for at, size in zip(starts, part_widths)
        )
    else:
        head_grad = head_grad.reshape(-1, value_heads, unit_rows)
        columns = query_weight.shape[0]
        query_grad = head_grad[:, :, : group * dim].reshape(columns, -1)
        key_grad = head_grad[:, :, group * dim : (group + 1) * dim].reshape(columns, -1)
        value_grad = head_grad[:, :, (group + 1) * dim :].reshape(columns, -1)
    return (
        output_rows.astype(low).reshape(block_input.shape),
        input_grad.reshape(block_input.shape),
        query_grad,
        key_grad,
        value_grad,
        out_grad.T,
        gate_grad,
        up_grad,
        down_grad.T,
        gain_sums[0],
        gain_sums[1],
    )


def solution(mesh):
    cp_count, tp_count = mesh.shape["cp"], mesh.shape["tp"]
    fine = Mesh(mesh.devices.reshape(cp_count // CORES, CORES, tp_count), ("chip", "core", "tp"))
    cp = ("chip", "core")
    rows = P(None, cp + ("tp",), None)
    wide, tall = P(cp, "tp"), P("tp", cp)
    return jax.shard_map(
        on_device,
        mesh=fine,
        in_specs=(rows, P(), P(), wide, wide, wide, tall, wide, wide, tall, P(), P(), rows),
        out_specs=(rows, rows, wide, wide, wide, tall, wide, wide, tall, P(), P()),
        check_vma=False,
    )
```
